32 devices in a mesh: ep: 8 (over z, y), tp: 4 (over x, core).
Axes of the slice: x: 2, y: 2, z: 4, core: 2. Of those that a mesh axis runs over, the one named last changes fastest.
Arguments:
- layer_input: bfloat16 [8192, 2048], P(('ep', 'tp')), may hold values from -6 to 6
- routes: int32 [8192, 8], P(('ep', 'tp')), may hold values from 0 to 31, all different within a row; in each aligned block of 256 rows (0 to 255, 256 to 511, ...) at most 96 rows name the same one
- doc_lengths: int32 [8, 4], P('ep'), may hold values from 1 to 512, 1024 in all within a row
- norm1_gain: bfloat16 [2048], replicated, may hold values from 0.25 to 1.75
- w_qkv: bfloat16 [2048, 3, 2048], P(None, None, 'tp'), may hold values from -0.125 to 0.125
- q_gain: bfloat16 [128], replicated, may hold values from 0.25 to 1.75
- k_gain: bfloat16 [128], replicated, may hold values from 0.25 to 1.75
- w_out: bfloat16 [2048, 2048], P('tp'), may hold values from -0.5 to 0.5
- norm2_gain: bfloat16 [2048], replicated, may hold values from 0.25 to 1.75
- w_router: bfloat16 [2048, 32], replicated, may hold values from -0.125 to 0.125
- expert_gate_up: bfloat16 [32, 2048, 2, 1024], P('ep', None, None, 'tp'), may hold values from -0.125 to 0.125
- expert_down: bfloat16 [32, 1024, 2048], P('ep', 'tp'), may hold values from -0.375 to 0.375
- d_out: bfloat16 [8192, 2048], P(('ep', 'tp')), may hold values from -6 to 6
Outputs:
- output: bfloat16 [8192, 2048], P(('ep', 'tp'))
- grad_input: float32 [8192, 2048], P(('ep', 'tp'))
- grad_norm1: float32 [2048], replicated
- grad_w_qkv: float32 [2048, 3, 2048], P('ep', None, 'tp')
- grad_q_gain: float32 [128], replicated
- grad_k_gain: float32 [128], replicated
- grad_w_out: float32 [2048, 2048], P('tp', 'ep')
- grad_norm2: float32 [2048], replicated
- grad_router: float32 [2048, 32], replicated
- grad_gate_up: float32 [32, 2048, 2, 1024], P('ep', None, None, 'tp')
- grad_down: float32 [32, 1024, 2048], P('ep', 'tp')
The draws below stay inside these ranges and needn't reach their ends.
Inputs may be any that keep to these rules, and one draw needn't show every extreme that they name: `routes`: among the rows of one device (aligned blocks of 256 tokens), no expert is chosen by more than 96 tokens; some expert is chosen by exactly 96 of them. A token's 8 experts differ. `doc_lengths`: A sequence's 4 lengths sum to 1024; the longest is 512.
All inputs are finite; a program needn't handle non-finite values.
Results may differ from the reference program's by a relative error of at most 0.024.
Values may be sent and summed in bfloat16 or wider, within the bound.
A program may use at most 576 MiB of HBM per device.

```python
import math
import jax
import jax.numpy as jnp
import numpy as np
from jax import lax

D = 2048
HEADS = 16
HEAD_DIM = 128
FF = 1024
TOPK = 8
SEQ = 1024
DOCS = 4
EXPERTS = 32
TOKENS = 8192
ROWS = 256
CAP = 96
QBLOCK = 512
N_EP = 8


def block_scale(stream_key, dims, pieces, least, top_value):
    def one(axis_at, parts):
        draws = jax.random.uniform(jax.random.fold_in(jax.random.fold_in(stream_key, 6), axis_at), (parts,), jnp.float32, least / len(pieces), top_value / len(pieces))
        return jnp.repeat(jnp.exp(draws), dims[axis_at] // parts).reshape((-1,) + (1,) * (len(dims) - axis_at - 1))

    level = one(*pieces[0])
    for cut in pieces[1:]:
        level = level * one(*cut)
    return level


def profile(number_of, total, bound, slope):
    loads = [(1 << 20) // math.isqrt(grade ** slope) + 1 for grade in range(2, number_of + 1)]
    rest, given = total - bound - (number_of - 1), [1] * (number_of - 1)
    while rest > 0:
        candidates = [i for i in range(number_of - 1) if given[i] < bound]
        mass, budget = sum([loads[i] for i in candidates]), rest
        for i in candidates:
            extra = min(bound - given[i], max(1, budget * loads[i] // mass), rest)
            given[i] = given[i] + extra
            rest = rest - extra
    return np.array([bound] + given)


def uneven_parts(rng, number_of, total, reach, slope):
    if number_of == 2:
        one = jax.random.randint(rng, (), max(1, total - reach), min(reach, total - 1) + 1)
        return jnp.stack([one, total - one])
    sizes = jnp.asarray(profile(number_of, total, reach, slope), jnp.int32)
    couples = (number_of - 1) // 2
    donor, receiver = sizes[1:1 + 2 * couples:2], sizes[2:2 + 2 * couples:2]
    slack = jnp.minimum(donor - 1, reach - receiver)
    shifted = jax.random.randint(jax.random.fold_in(rng, 1), (couples,), 0, 1 << 20) % (slack + 1)
    sizes = sizes.at[1:1 + 2 * couples:2].set(donor - shifted).at[2:2 + 2 * couples:2].set(receiver + shifted)
    return sizes[jax.random.permutation(jax.random.fold_in(rng, 2), number_of)]


def assign_block(rng, own, number, rows, count, top, reach, lean):
    order = jax.random.permutation(rng, count)
    crowded, usual = shares(count, rows * top, reach, lean, True), shares(count, rows * top, reach, lean, False)
    places = jnp.arange(count)

    def named(tallies, rotation):
        used = int((tallies > 0).sum())
        fixed = max(1, used // 4)
        shifted = fixed + (places - fixed + rotation * (used - fixed)) % max(1, count - fixed)
        return jnp.zeros((count,), jnp.int32).at[order[jnp.where(places < fixed, places, shifted)]].set(jnp.asarray(tallies, jnp.int32))

    tallies = jnp.where(number % 4 == 0, named(crowded, number // 4), named(usual, number - number // 4 - 1))
    mixed = jax.random.permutation(jax.random.fold_in(own, 3), count)
    source_of, receiver = mixed[0:count // 2 * 2:2], mixed[1:count // 2 * 2:2]
    room = jnp.minimum(tallies[source_of] - 1, reach - tallies[receiver]) // 2
    room = jnp.where((source_of == order[0]) | (receiver == order[0]) | (tallies[receiver] == 0), 0, jnp.maximum(room, 0))
    shifted = jax.random.randint(jax.random.fold_in(own, 4), (count // 2,), 0, 1 << 20) % (room + 1)
    tallies = tallies.at[source_of].add(-shifted).at[receiver].add(shifted)
    items = jnp.searchsorted(jnp.cumsum(tallies), jnp.arange(rows * top), side="right").astype(jnp.int32)
    table = items.reshape(top, rows).T
    table = table[jax.random.permutation(jax.random.fold_in(own, 1), rows)]
    rotation = jax.random.randint(jax.random.fold_in(own, 2), (rows, 1), 0, top)
    return jnp.take_along_axis(table, (jnp.arange(top)[None, :] + rotation) % top, axis=1)


def shares(count, total, reach, slope, full):
    weights = [(1 << 20) // math.isqrt(rank ** slope) + 1 for rank in range(1, count + 1)]
    largest = reach if full else min(reach, max(-(-total // count), total * weights[0] // sum(weights)))
    least = 1 if total - largest >= count - 1 else 0
    given, rest = [largest] + [least] * (count - 1), total - largest - least * (count - 1)
    while rest > 0:
        movable = [i for i in range(1, count) if given[i] < largest] or [i for i in range(1, count) if given[i] < reach]
        pool, remaining = sum([weights[i] for i in movable]), rest
        for i in movable:
            extra = min(reach - given[i], max(1, remaining * weights[i] // pool), rest)
            given[i] = given[i] + extra
            rest = rest - extra
    return np.array(given)


def scatter_about(key, extent, width, bound, split=(), kind=jnp.bfloat16):
    values = width * jax.random.normal(key, extent, jnp.float32)
    if split:
        values = values * block_scale(key, extent, split, -0.22, 0.18)
    return jnp.clip(values, -bound, bound).astype(kind)


def setup_inputs(seed: int = 0) -> dict:
    key_list = jax.random.split(jax.random.key(seed), 14)
    layer_input = scatter_about(key_list[0], (TOKENS, D), 1.0, 6.0, ((0, 32),))
    routes_keys = jax.random.split(jax.random.fold_in(key_list[1], 1), TOKENS // ROWS)
    routes_turns = jax.random.permutation(jax.random.fold_in(key_list[1], 3), TOKENS // ROWS)
    routes = jax.vmap(lambda own, number: assign_block(jax.random.fold_in(key_list[1], 2), own, number, ROWS, EXPERTS, TOPK, CAP, 2))(routes_keys, routes_turns).reshape((TOKENS, TOPK))
    doc_lengths = jax.vmap(lambda own: uneven_parts(own, DOCS, SEQ, SEQ // 2, 2))(jax.random.split(key_list[2], N_EP)).reshape((N_EP, DOCS)).astype(jnp.int32)
    norm1_gain = jnp.clip(1.0 + 0.15 * jax.random.normal(key_list[3], (D,), jnp.float32), 0.25, 1.75).astype(jnp.bfloat16)
    w_qkv = scatter_about(key_list[4], (D, 3, HEADS * HEAD_DIM), D ** -0.5, 0.125, ((2, 4),))
    q_gain = jnp.clip(1.0 + 0.15 * jax.random.normal(key_list[5], (HEAD_DIM,), jnp.float32), 0.25, 1.75).astype(jnp.bfloat16)
    k_gain = jnp.clip(1.0 + 0.15 * jax.random.normal(key_list[6], (HEAD_DIM,), jnp.float32), 0.25, 1.75).astype(jnp.bfloat16)
    w_out = scatter_about(key_list[7], (HEADS * HEAD_DIM, D), (HEADS * HEAD_DIM // 16) ** -0.5, 0.5, ((0, 4),))
    norm2_gain = jnp.clip(1.0 + 0.15 * jax.random.normal(key_list[8], (D,), jnp.float32), 0.25, 1.75).astype(jnp.bfloat16)
    w_router = scatter_about(key_list[9], (D, EXPERTS), D ** -0.5, 0.125)
    expert_gate_up = scatter_about(key_list[10], (EXPERTS, D, 2, FF), D ** -0.5, 0.125, ((0, 8), (3, 4)))
    expert_down = scatter_about(key_list[11], (EXPERTS, FF, D), (FF // 4) ** -0.5, 0.375, ((0, 8), (1, 4)))
    d_out = scatter_about(key_list[12], (TOKENS, D), 1.0, 6.0, ((0, 32),))
    return {"layer_input": layer_input, "routes": routes, "doc_lengths": doc_lengths, "norm1_gain": norm1_gain, "w_qkv": w_qkv, "q_gain": q_gain, "k_gain": k_gain, "w_out": w_out, "norm2_gain": norm2_gain, "w_router": w_router, "expert_gate_up": expert_gate_up, "expert_down": expert_down, "d_out": d_out}


HIGH = lax.Precision.HIGHEST
EPS_NORM = 1e-05
EPS_HEAD = 1e-06
ROPE_BASE = 10000.0
MASKED = -1e+30

@jax.custom_vjp
def low(v):
    return lax.optimization_barrier(v.astype(jnp.bfloat16)).astype(jnp.float32)

@jax.custom_vjp
def low_back(v):
    return v

def low_keep(v):
    return (low(v), None)

def low_pass(kept, grad):
    return (grad,)

def back_keep(v):
    return (v, None)

def back_low(kept, grad):
    return (low(grad),)
low.defvjp(low_keep, low_pass)
low_back.defvjp(back_keep, back_low)

def rms_scale(value, gain, eps):
    return value * lax.rsqrt(lax.optimization_barrier(jnp.mean(value * value, axis=-1, keepdims=True)) + eps) * gain

def rotate(value, cosine, sine):
    half = value.shape[-1] // 2
    first = value[..., :half]
    second = value[..., half:]
    return jnp.concatenate([first * cosine - second * sine, second * cosine + first * sine], axis=-1)

def positions(lengths, seq_len):
    ends = jnp.cumsum(lengths).astype(jnp.int32)
    starts = ends - lengths
    index = jnp.arange(seq_len, dtype=jnp.int32)
    doc_ids = lax.optimization_barrier(jnp.sum((index[:, None] >= ends[None, :]).astype(jnp.int32), axis=1))
    member = doc_ids[:, None] == jnp.arange(lengths.shape[0], dtype=jnp.int32)[None, :]
    offset = lax.optimization_barrier(jnp.sum(jnp.where(member, starts[None, :], 0), axis=1))
    return (doc_ids, index - offset)

def rope_tables(position, head_dim):
    half = head_dim // 2
    freq = ROPE_BASE ** (-(2.0 * jnp.arange(half, dtype=jnp.float32)) / head_dim)
    angle = position.astype(jnp.float32)[:, None] * freq[None, :]
    return (jnp.cos(angle), jnp.sin(angle))

def attention(h_seq, w_qkv, q_gain, k_gain, w_out, lengths):
    seq_len = h_seq.shape[0]
    projected = jnp.einsum('sd,dcf->csf', h_seq, w_qkv, precision=HIGH)
    q_raw = low_back(projected[0]).reshape(seq_len, HEADS, HEAD_DIM)
    k_raw = low_back(projected[1]).reshape(seq_len, HEADS, HEAD_DIM)
    v_raw = low_back(projected[2]).reshape(seq_len, HEADS, HEAD_DIM)
    doc_ids, position = positions(lengths, seq_len)
    cosine, sine = rope_tables(position, HEAD_DIM)
    cosine = cosine[:, None, :]
    sine = sine[:, None, :]
    queries = low(rotate(rms_scale(q_raw, q_gain, EPS_HEAD), cosine, sine))
    keys = low(rotate(rms_scale(k_raw, k_gain, EPS_HEAD), cosine, sine))
    values = low(v_raw)
    scale = HEAD_DIM ** (-0.5)
    blocks = seq_len // QBLOCK

    def one_block(item):
        q_block, doc_block = item
        scores = jnp.einsum('qhd,khd->hqk', q_block, keys, precision=HIGH) * scale
        scores = low_back(scores)
        scores = jnp.where((doc_block[:, None] == doc_ids[None, :])[None], scores, MASKED)
        weights = jax.nn.softmax(scores, axis=-1)
        return jnp.einsum('hqk,khd->qhd', low(weights), values, precision=HIGH)
    mixed = lax.map(jax.checkpoint(one_block), (queries.reshape(blocks, QBLOCK, HEADS, HEAD_DIM), doc_ids.reshape(blocks, QBLOCK)))
    mixed = mixed.reshape(seq_len, HEADS * HEAD_DIM)
    mixed = low(low_back(mixed))
    return jnp.dot(mixed, w_out, precision=HIGH)

def experts(h_two, route_ids, probs, gate_up, down):
    tokens = h_two.shape[0]
    flat = route_ids.reshape(-1)
    count_all = flat.shape[0]
    table = (flat[:, None] == jnp.arange(EXPERTS, dtype=jnp.int32)[None, :]).astype(jnp.int32)
    counts = lax.optimization_barrier(jnp.sum(table, axis=0))
    offsets = jnp.cumsum(counts) - counts
    rank = lax.optimization_barrier(jnp.sum((jnp.cumsum(table, axis=0) - table) * table, axis=1))
    order = jnp.argsort(flat, stable=True).astype(jnp.int32)
    window = tokens // ROWS * CAP
    slots = jnp.arange(window, dtype=jnp.int32)

    def one_expert(item):
        w_pair, w_down, start, count = item
        source = order[jnp.minimum(start + slots, count_all - 1)]
        rows_in = low_back(h_two[source // TOPK])
        pair = low_back(jnp.einsum('wd,dcf->wcf', rows_in, w_pair, precision=HIGH))
        hidden = low(jax.nn.silu(pair[:, 0]) * pair[:, 1])
        result = jnp.dot(hidden, w_down, precision=HIGH)
        valid = (slots < count).astype(jnp.float32)[:, None]
        return low_back(low(result)) * valid
    table_out = lax.map(jax.checkpoint(one_expert), (gate_up, down, offsets, counts))
    picked = table_out[flat, rank].reshape(tokens, TOPK, D)
    return lax.optimization_barrier(jnp.sum(probs[:, :, None] * picked, axis=1))

def layer(input_group, route_group, length_group, params):
    gain_one, w_qkv, q_gain, k_gain, w_out, gain_two, w_router, gate_up, down = params
    group = length_group.shape[0]
    h_one = low(rms_scale(input_group, gain_one, EPS_NORM))
    attn = jnp.concatenate([attention(h_one[i * SEQ:(i + 1) * SEQ], w_qkv, q_gain, k_gain, w_out, length_group[i]) for i in range(group)], axis=0)
    middle = input_group + low_back(attn)
    h_two = low(rms_scale(middle, gain_two, EPS_NORM))
    logits = jnp.dot(h_two, w_router, precision=HIGH)
    chosen = jnp.take_along_axis(logits, route_group, axis=1)
    probs = jax.nn.softmax(chosen, axis=-1)
    return middle + experts(h_two, route_group, probs, gate_up, down)

def reference(layer_input, routes, doc_lengths, norm1_gain, w_qkv, q_gain, k_gain, w_out, norm2_gain, w_router, expert_gate_up, expert_down, d_out):
    params = tuple((value.astype(jnp.float32) for value in (norm1_gain, w_qkv, q_gain, k_gain, w_out, norm2_gain, w_router, expert_gate_up, expert_down)))
    group = max(1, min(N_EP, 4096 // SEQ))
    steps_count = N_EP // group
    input_groups = layer_input.astype(jnp.float32).reshape(steps_count, group * SEQ, D)
    route_groups = routes.reshape(steps_count, group * SEQ, TOPK)
    length_groups = doc_lengths.reshape(steps_count, group, DOCS)

    def whole(input_all, weights):

        def step(carry, item):
            input_group, route_group, length_group = item
            return (carry, jax.checkpoint(layer)(input_group, route_group, length_group, weights))
        _, outputs = lax.scan(step, jnp.zeros((), jnp.float32), (input_all, route_groups, length_groups))
        return outputs
    result, back = jax.vjp(whole, input_groups, params)
    grad_in, grads = back(d_out.astype(jnp.float32).reshape(input_groups.shape))
    output = result.reshape(TOKENS, D).astype(jnp.bfloat16)
    grad_input = grad_in.reshape(TOKENS, D)
    return (output, grad_input, grads[0], grads[1], grads[2], grads[3], grads[4], grads[5], grads[6], grads[7], grads[8])
```

```python
import jax
import jax.numpy as jnp
from jax import lax
from jax.sharding import Mesh
from jax.sharding import PartitionSpec as P

HIGH = lax.Precision.HIGHEST
EPS_NORM = 1e-05
EPS_HEAD = 1e-06
ROPE_BASE = 10000.0
MASKED = -1e30
F32 = jnp.float32
BF16 = jnp.bfloat16
PLANE = ("ep", "x")
GROUP = ("x", "core")
ALL = ("ep", "x", "core")


def norm_rows(value, gain):
    inverse = lax.rsqrt(jnp.mean(value * value, axis=-1, keepdims=True) + EPS_NORM)
    return value * inverse * gain


def norm_back(value, gain, grad):
    inverse = lax.rsqrt(jnp.mean(value * value, axis=-1, keepdims=True) + EPS_NORM)
    normed = value * inverse
    lifted = grad * gain
    inner = jnp.mean(lifted * normed, axis=-1, keepdims=True)
    return (lifted - normed * inner) * inverse, jnp.sum(grad * normed, axis=0)


def rms_scale(value, gain, eps):
    return value * lax.rsqrt(jnp.mean(value * value, axis=-1, keepdims=True) + eps) * gain


def rotate(value, cosine, sine):
    half = value.shape[-1] // 2
    first = value[..., :half]
    second = value[..., half:]
    return jnp.concatenate(
        [first * cosine - second * sine, second * cosine + first * sine], axis=-1
    )


def positions(lengths, seq_len):
    ends = jnp.cumsum(lengths)
    starts = ends - lengths
    index = jnp.arange(seq_len, dtype=jnp.int32)
    doc_ids = jnp.sum((index[:, None] >= ends[None, :]).astype(jnp.int32), axis=1)
    member = doc_ids[:, None] == jnp.arange(lengths.shape[0], dtype=jnp.int32)[None, :]
    offset = jnp.sum(jnp.where(member, starts[None, :], 0), axis=1)
    return (doc_ids, index - offset)


def rope_tables(position, head_dim):
    half = head_dim // 2
    freq = ROPE_BASE ** (-(2.0 * jnp.arange(half, dtype=F32)) / head_dim)
    angle = position.astype(F32)[:, None] * freq[None, :]
    return (jnp.cos(angle), jnp.sin(angle))


def einsum(spec, left, right):
    return jnp.einsum(spec, left, right, preferred_element_type=F32)


def swap_cores(value):
    return lax.ppermute(value, "core", [(0, 1), (1, 0)])


def gather(value, axes):
    return lax.all_gather(value, axes, axis=0, tiled=True)


def scatter(value, axes, dim=0):
    return lax.psum_scatter(value, axes, scatter_dimension=dim, tiled=True)


def masked_softmax(logits, mask):
    kept = jnp.where(mask, logits, MASKED)
    lifted = jnp.where(mask, jnp.exp(kept - jnp.max(kept, axis=-1, keepdims=True)), 0.0)
    return lifted / jnp.sum(lifted, axis=-1, keepdims=True)


def route_mask(routes, experts_all):
    ids = jnp.arange(experts_all, dtype=jnp.int32)
    return jnp.any(routes[:, :, None] == ids[None, None, :], axis=1)


def per_device(
    layer_input,
    routes,
    doc_lengths,
    norm1_gain,
    w_qkv,
    q_gain,
    k_gain,
    w_out,
    norm2_gain,
    w_router,
    expert_gate_up,
    expert_down,
    d_out,
):
    rows, width = layer_input.shape
    x_count = lax.axis_size("x")
    ep_count = lax.axis_size("ep")
    seq_len = rows * x_count * 2
    blocks = ep_count * x_count
    topk = routes.shape[1]
    experts_all = w_router.shape[1]
    local = expert_gate_up.shape[0]
    hidden_local = expert_down.shape[1]
    head_dim = q_gain.shape[0]
    qkv_local = w_qkv.shape[2]
    heads = qkv_local // head_dim
    capacity = min(3 * rows * topk // (2 * experts_all), rows)
    q_rows = min(512, seq_len)
    q_count = seq_len // q_rows
    scale = head_dim ** (-0.5)
    my_ep = lax.axis_index("ep")

    gain_one = norm1_gain.astype(F32)
    gain_two = norm2_gain.astype(F32)
    inputs = layer_input.astype(F32)
    grad_out = d_out.astype(F32)
    input_seq = gather(layer_input, GROUP)
    h_seq = norm_rows(input_seq.astype(F32), gain_one).astype(BF16)
    w_flat = w_qkv.reshape(width, 3 * qkv_local)
    projected = jnp.dot(h_seq, w_flat, preferred_element_type=F32).reshape(
        seq_len, 3, heads, head_dim
    )
    q_raw = projected[:, 0]
    k_raw = projected[:, 1]
    v_raw = projected[:, 2]
    doc_ids, position = positions(doc_lengths[0], seq_len)
    cosine, sine = rope_tables(position, head_dim)
    cosine = cosine[:, None, :]
    sine = sine[:, None, :]

    def shape_heads(value, gain):
        return rotate(rms_scale(value, gain, EPS_HEAD), cosine, sine)

    q_rot, q_back = jax.vjp(shape_heads, q_raw, q_gain.astype(F32))
    k_rot, k_back = jax.vjp(shape_heads, k_raw, k_gain.astype(F32))
    queries = q_rot.astype(BF16)
    keys = k_rot.astype(BF16)
    values = v_raw.astype(BF16)
    q_blocks = queries.reshape(q_count, q_rows, heads, head_dim)
    doc_blocks = doc_ids.reshape(q_count, q_rows)

    def scores_of(q_block, doc_block):
        plain = einsum("qhd,khd->hqk", q_block, keys) * scale
        return jnp.where((doc_block[:, None] == doc_ids[None, :])[None], plain, MASKED)

    def attend(item):
        q_block, doc_block = item
        scores = scores_of(q_block, doc_block)
        peak = jnp.max(scores, axis=-1, keepdims=True)
        lifted = jnp.exp(scores - peak)
        total = jnp.sum(lifted, axis=-1, keepdims=True)
        weights = (lifted / total).astype(BF16)
        return (einsum("hqk,khd->qhd", weights, values), peak, total)

    mixed, peaks, totals = lax.map(attend, (q_blocks, doc_blocks))
    attn_vals = mixed.reshape(seq_len, qkv_local).astype(BF16)
    attn_out = scatter(jnp.dot(attn_vals, w_out, preferred_element_type=F32).astype(BF16), GROUP)
    middle = inputs + attn_out.astype(F32)
    h_two = norm_rows(middle, gain_two).astype(BF16)

    g_plane = gather(d_out, PLANE).reshape(blocks, rows, width)
    routes_plane = gather(routes, PLANE)
    h_flat = gather(h_two, PLANE)
    h_plane = h_flat.reshape(blocks, rows, width)
    gate_own = expert_gate_up[:, :, 0]
    up_own = expert_gate_up[:, :, 1]
    pair_other = swap_cores(expert_gate_up.reshape(local, width, 2 * hidden_local))
    down_other = swap_cores(expert_down)
    pair_own = expert_gate_up.reshape(local, width, 2 * hidden_local)

    mask_plane = route_mask(routes_plane, experts_all)
    logits_plane = jnp.dot(h_flat, w_router, preferred_element_type=F32)
    probs_plane = masked_softmax(logits_plane, mask_plane)
    first = my_ep * local
    mask_here = lax.dynamic_slice_in_dim(mask_plane, first, local, axis=1)
    probs_here = lax.dynamic_slice_in_dim(probs_plane, first, local, axis=1)
    mask_here = mask_here.reshape(blocks, rows, local).transpose(0, 2, 1)
    probs_here = probs_here.reshape(blocks, rows, local).transpose(0, 2, 1)
    before = jnp.triu(jnp.ones((rows, rows), BF16), 1)
    rank = einsum("bet,tu->beu", mask_here.astype(BF16), before).astype(jnp.int32)
    slots = jnp.arange(capacity, dtype=jnp.int32)[None, None, :, None]
    picks = mask_here[:, :, None, :] & (rank[:, :, None, :] == slots)
    pick = picks.astype(BF16)
    prob_rows = jnp.sum(jnp.where(picks, probs_here[:, :, None, :], 0.0), axis=-1)
    prob_rows = prob_rows.transpose(1, 0, 2)[..., None]

    g_rows = einsum("bect,btd->ebcd", pick, g_plane).astype(BF16)
    h_rows = einsum("bect,btd->ebcd", pick, h_plane).astype(BF16)

    def expert_half(pair, down):
        gate = einsum("ebcd,edf->ebcf", h_rows, pair[:, :, :hidden_local])
        up = einsum("ebcd,edf->ebcf", h_rows, pair[:, :, hidden_local:])
        back = einsum("ebcd,efd->ebcf", g_rows, down)
        sigma = jax.nn.sigmoid(gate)
        silu = gate * sigma
        hidden = (silu * up).astype(BF16).astype(F32)
        dots = jnp.sum(hidden * back, axis=-1)
        weighted = (hidden * prob_rows).astype(BF16)
        grad_hidden = back * prob_rows
        grad_gate = (grad_hidden * up * (sigma + silu * (1.0 - sigma))).astype(BF16)
        grad_up = (grad_hidden * silu).astype(BF16)
        return dots, weighted, jnp.concatenate([grad_gate, grad_up], axis=-1)

    dots_own, weighted_own, ggu_own = expert_half(pair_own, expert_down)
    dots_other, weighted_other, ggu_other = expert_half(pair_other, down_other)
    back_rows = (
        einsum("ebcf,edf->ebcd", ggu_own, pair_own)
        + einsum("ebcf,edf->ebcd", ggu_other, pair_other)
    ).astype(BF16)
    out_rows = (
        einsum("ebcf,efd->ebcd", weighted_own, expert_down)
        + einsum("ebcf,efd->ebcd", weighted_other, down_other)
    ).astype(BF16)
    dot_rows = (dots_own + dots_other).transpose(1, 0, 2)
    dots_token = jnp.sum(jnp.where(picks, dot_rows[..., None], 0.0), axis=2)
    dots_token = dots_token.transpose(0, 2, 1).reshape(blocks * rows, local)
    dots_high = dots_token.astype(BF16)
    dots_low = (dots_token - dots_high.astype(F32)).astype(BF16)
    my_x = lax.axis_index("x")
    placed = jnp.zeros((blocks * rows, x_count, 2, experts_all), BF16)
    placed = lax.dynamic_update_slice(
        placed,
        jnp.stack([dots_high, dots_low], axis=1)[:, None],
        (0, my_x, 0, first),
    ).reshape(blocks * rows, x_count * 2 * experts_all)
    back_part = einsum("bect,ebcd->btd", pick, back_rows).astype(BF16)
    back_sum = scatter(
        jnp.concatenate([back_part.reshape(blocks * rows, width), placed], axis=1), PLANE
    )
    out_part = einsum("bect,ebcd->btd", pick, out_rows).astype(BF16)
    mixture = scatter(out_part.reshape(blocks * rows, width), PLANE).astype(F32)
    output = (middle + mixture).astype(BF16)

    grad_pair_own = einsum("ebcd,ebcf->edf", h_rows, ggu_own)
    grad_pair_other = einsum("ebcd,ebcf->edf", h_rows, ggu_other)
    grad_down_own = einsum("ebcf,ebcd->efd", weighted_own, g_rows)
    grad_down_other = einsum("ebcf,ebcd->efd", weighted_other, g_rows)
    grad_pair = grad_pair_own + swap_cores(grad_pair_other.astype(BF16)).astype(F32)
    grad_down = grad_down_own + swap_cores(grad_down_other.astype(BF16)).astype(F32)
    grad_gate_up = grad_pair.reshape(local, width, 2, hidden_local)

    grad_probs = jnp.sum(
        back_sum[:, width:].astype(F32).reshape(rows, x_count * 2, experts_all), axis=1
    )
    mask_own = route_mask(routes, experts_all)
    probs_own = masked_softmax(jnp.dot(h_two, w_router, preferred_element_type=F32), mask_own)
    inner = jnp.sum(probs_own * grad_probs, axis=-1, keepdims=True)
    grad_logits = probs_own * (grad_probs - inner)
    grad_router = jnp.dot(h_two.astype(F32).T, grad_logits, precision=HIGH)
    grad_h_two = back_sum[:, :width].astype(F32) + jnp.dot(
        grad_logits, w_router.astype(F32).T, precision=HIGH
    )
    grad_mid_norm, grad_gain_two = norm_back(middle, gain_two, grad_h_two)
    grad_mid = grad_out + grad_mid_norm

    ga_seq = gather(grad_mid.astype(BF16), GROUP)
    grad_wout = lax.dot_general(
        attn_vals, ga_seq, (((0,), (0,)), ((), ())), preferred_element_type=F32
    )
    grad_vals = lax.dot_general(
        ga_seq, w_out, (((1,), (1,)), ((), ())), preferred_element_type=F32
    )
    grad_mixed = grad_vals.astype(BF16).reshape(q_count, q_rows, heads, head_dim)

    def attend_back(carry, item):
        grad_keys, grad_values = carry
        q_block, doc_block, peak, total, grad_block = item
        scores = scores_of(q_block, doc_block)
        probs_full = jnp.exp(scores - peak) / total
        weights = probs_full.astype(BF16)
        grad_weights = einsum("qhd,khd->hqk", grad_block, values)
        delta = jnp.sum(grad_weights * probs_full, axis=-1, keepdims=True)
        grad_scores = (probs_full * (grad_weights - delta)).astype(BF16)
        grad_q = einsum("hqk,khd->qhd", grad_scores, keys) * scale
        grad_keys = grad_keys + einsum("hqk,qhd->khd", grad_scores, q_block) * scale
        grad_values = grad_values + einsum("hqk,qhd->khd", weights, grad_block)
        return ((grad_keys, grad_values), grad_q)

    head_zeros = jnp.zeros((seq_len, heads, head_dim), F32)
    (grad_keys, grad_values), grad_queries = lax.scan(
        attend_back, (head_zeros, head_zeros), (q_blocks, doc_blocks, peaks, totals, grad_mixed)
    )
    grad_queries = grad_queries.reshape(seq_len, heads, head_dim)
    grad_q_raw, grad_q_gain = q_back(grad_queries)
    grad_k_raw, grad_k_gain = k_back(grad_keys)
    grad_proj = (
        jnp.stack([grad_q_raw, grad_k_raw, grad_values], axis=1)
        .reshape(seq_len, 3 * qkv_local)
        .astype(BF16)
    )
    grad_wqkv = lax.dot_general(
        h_seq, grad_proj, (((0,), (0,)), ((), ())), preferred_element_type=F32
    )
    grad_h_one = scatter(
        lax.dot_general(
            grad_proj, w_flat, (((1,), (1,)), ((), ())), preferred_element_type=F32
        ).astype(BF16),
        GROUP,
    ).astype(F32)
    grad_in_norm, grad_gain_one = norm_back(inputs, gain_one, grad_h_one)
    grad_input = grad_mid + grad_in_norm
    dense_qkv = scatter(grad_wqkv.astype(BF16), "ep").astype(F32)
    dense_out = scatter(grad_wout.astype(BF16), "ep", 1).astype(F32)
    summed = lax.psum((grad_gain_one, grad_gain_two, grad_q_gain, grad_k_gain, grad_router), ALL)
    return (
        output,
        grad_input,
        summed[0],
        dense_qkv.reshape(dense_qkv.shape[0], 3, qkv_local),
        summed[2],
        summed[3],
        dense_out,
        summed[1],
        summed[4],
        grad_gate_up,
        grad_down,
    )


def solution(mesh):
    ep_count, tp_count = mesh.shape["ep"], mesh.shape["tp"]
    fine = Mesh(mesh.devices.reshape(ep_count, tp_count // 2, 2), ALL)
    in_specs = (
        P(ALL, None),
        P(ALL, None),
        P("ep", None),
        P(),
        P(None, None, GROUP),
        P(),
        P(),
        P(GROUP, None),
        P(),
        P(),
        P("ep", None, None, GROUP),
        P("ep", GROUP, None),
        P(ALL, None),
    )
    out_specs = (
        P(ALL, None),
        P(ALL, None),
        P(),
        P("ep", None, GROUP),
        P(),
        P(),
        P(GROUP, "ep"),
        P(),
        P(),
        P("ep", None, None, GROUP),
        P("ep", GROUP, None),
    )
    return jax.shard_map(
        per_device, mesh=fine, in_specs=in_specs, out_specs=out_specs, check_vma=False
    )
```

```python
import functools
import math

import jax
import jax.numpy as jnp
from jax import lax
from jax.experimental import pallas as pl
from jax.experimental.pallas import tpu as pltpu
from jax.sharding import Mesh
from jax.sharding import PartitionSpec as P

HIGH = lax.Precision.HIGHEST
EPS_NORM = 1e-05
EPS_HEAD = 1e-06
ROPE_BASE = 10000.0
MASKED = -1e30
F32 = jnp.float32
BF16 = jnp.bfloat16
PLANE = ("ep", "x")
GROUP = ("x", "core")
ALL = ("ep", "x", "core")

MESH = pl.DeviceIdType.MESH
VMEM_BYTES = 60 * 1024 * 1024


def remote(source, target, send, recv, where):
    return pltpu.make_async_remote_copy(
        src_ref=source,
        dst_ref=target,
        send_sem=send,
        recv_sem=recv,
        device_id=where,
        device_id_type=MESH,
    )


def greet(where):
    pl.semaphore_signal(
        pltpu.get_barrier_semaphore(), inc=1, device_id=where, device_id_type=MESH
    )


def add_into(target, terms, step=32):
    def body(index, carry):
        at = pl.ds(pl.multiple_of(index * step, step), step)
        total = terms[0][at, :].astype(F32)
        for term in terms[1:]:
            total = total + term[at, :].astype(F32)
        target[at, :] = total.astype(target.dtype)
        return carry

    lax.fori_loop(0, target.shape[0] // step, body, 0)


def peer_of(axes, counts, index):
    where = {}
    for axis, count in reversed(list(zip(axes, counts))):
        where[axis] = lax.rem(index, count)
        index = index // count
    return where


def spread_kernel(axes, counts, own_slices, v_ref, out_ref, local_sem, send, recv):
    total = math.prod(counts)
    me = 0
    for axis, count in zip(axes, counts):
        me = me * count + lax.axis_index(axis)

    def hello(step, carry):
        greet(peer_of(axes, counts, lax.rem(me + step, total)))
        return carry

    lax.fori_loop(1, total, hello, 0)
    pl.semaphore_wait(pltpu.get_barrier_semaphore(), total - 1)

    def copy(step):
        peer = lax.rem(me + step, total)
        source = v_ref.at[peer] if own_slices else v_ref
        return remote(
            source, out_ref.at[me], send.at[step], recv.at[step], peer_of(axes, counts, peer)
        )

    mine = pltpu.make_async_copy(
        v_ref.at[me] if own_slices else v_ref, out_ref.at[me], local_sem
    )
    mine.start()

    def begin(step, carry):
        copy(step).start()
        return carry

    def finish(step, carry):
        copy(step).wait()
        return carry

    lax.fori_loop(1, total, begin, 0)
    mine.wait()
    lax.fori_loop(1, total, finish, 0)


def spread(value, axes, collective_id, own_slices=False):
    counts = tuple(lax.axis_size(axis) for axis in axes)
    total = math.prod(counts)
    shape = value.shape[1:] if own_slices else value.shape
    return pl.pallas_call(
        functools.partial(spread_kernel, axes, counts, own_slices),
        out_shape=jax.ShapeDtypeStruct((total,) + shape, value.dtype),
        in_specs=[pl.BlockSpec(memory_space=pltpu.VMEM)],
        out_specs=pl.BlockSpec(memory_space=pltpu.VMEM),
        scratch_shapes=[
            pltpu.SemaphoreType.DMA,
            pltpu.SemaphoreType.DMA((total,)),
            pltpu.SemaphoreType.DMA((total,)),
        ],
        compiler_params=pltpu.CompilerParams(
            collective_id=collective_id, has_side_effects=True
        ),
        name="spread",
    )(value)


def visiting_order(count):
    order, low, high = [], 0, count - 1
    while low <= high:
        order.append(high)
        high -= 1
        if low <= high:
            order.append(low)
            low += 1
    return order


def reduce_kernel(
    depth, half, p_ref, out_ref, own, one, two, right, left,
    own_sem, s1, r1, s2, r2, sr, rr, sl, rl,
):
    ep = lax.axis_index("ep")
    x = lax.axis_index("x")
    z = ep // 2
    y = lax.rem(ep, 2)
    first = ({"x": 1 - x}, {"ep": z * 2 + 1 - y})
    second = (first[1], first[0])
    up, down = {"ep": ep + 2}, {"ep": ep - 2}
    barrier = pltpu.get_barrier_semaphore()
    greet(first[0])
    greet(first[1])
    pl.when(z < depth - 1)(lambda: greet(up))
    pl.when(z > 0)(lambda: greet(down))
    peers = 2 + (z > 0).astype(jnp.int32) + (z < depth - 1).astype(jnp.int32)
    pl.semaphore_wait(barrier, peers)

    order = visiting_order(depth)
    cols = (pl.ds(0, half), pl.ds(half, half))
    mine = (y, x)

    def block(part, level, step, theirs):
        near = (x, y)[part]
        near = 1 - near if theirs else near
        far = 1 - mine[part] if step == 0 else mine[part]
        at = (far, near) if part == 0 else (near, far)
        return p_ref.at[level, at[0], at[1], :, cols[part]]

    def send_one(part, level, step):
        return remote(
            block(part, level, step, True),
            one.at[part, level, step],
            s1.at[part, level, step],
            r1.at[part, level, step],
            first[part],
        )

    def send_two(part, level):
        return remote(
            one.at[part, level, 0],
            two.at[part, level],
            s2.at[part, level],
            r2.at[part, level],
            second[part],
        )

    def load(part, level, step):
        return pltpu.make_async_copy(
            block(part, level, step, False),
            own.at[part, level, step],
            own_sem.at[part, level, step],
        )

    def go_right(part, level):
        ref = right.at[part, level]
        return remote(ref, ref, sr.at[part, level], rr.at[part, level], up)

    def go_left(part, level):
        ref = left.at[part, level]
        return remote(ref, ref, sl.at[part, level], rl.at[part, level], down)

    for level in order:
        for part in (0, 1):
            send_one(part, level, 0).start()
    for step in (0, 1):
        for level in order:
            for part in (0, 1):
                load(part, level, step).start()
    for level in order:
        for part in (0, 1):
            load(part, level, 0).wait()
            send_one(part, level, 0).wait()
            arrived = one.at[part, level, 0]
            add_into(arrived, [arrived, own.at[part, level, 0]])
            send_two(part, level).start()
            send_one(part, level, 1).start()

    def begin(level):
        for part in (0, 1):
            if level > 0:

                @pl.when(z == 0)
                def _():
                    add_into(right.at[part, level], [two.at[part, level]])
                    go_right(part, level).start()

            if level < depth - 1:

                @pl.when(z == depth - 1)
                def _():
                    add_into(left.at[part, level], [two.at[part, level]])
                    go_left(part, level).start()

    def forward(level):
        for part in (0, 1):

            @pl.when((z > 0) & (z < level))
            def _():
                go_right(part, level).wait_recv()
                ref = right.at[part, level]
                add_into(ref, [ref, two.at[part, level]])
                go_right(part, level).start()

            @pl.when((z < depth - 1) & (z > level))
            def _():
                go_left(part, level).wait_recv()
                ref = left.at[part, level]
                add_into(ref, [ref, two.at[part, level]])
                go_left(part, level).start()

    for turn, level in enumerate(order):
        for part in (0, 1):
            load(part, level, 1).wait()
            send_one(part, level, 1).wait()
            kept = own.at[part, level, 1]
            add_into(kept, [one.at[part, level, 1], kept])
            send_two(part, level).wait()
            add_into(two.at[part, level], [two.at[part, level], kept])
        begin(level)
        if turn > 0:
            forward(order[turn - 1])
    forward(order[-1])
    for level in range(depth):

        @pl.when(z == level)
        def _():
            for part in (0, 1):
                terms = [two.at[part, level]]
                if level > 0:
                    go_right(part, level).wait_recv()
                    terms.append(right.at[part, level])
                if level < depth - 1:
                    go_left(part, level).wait_recv()
                    terms.append(left.at[part, level])
                add_into(out_ref.at[:, cols[part]], terms)

        for part in (0, 1):
            pl.when(z < level)(lambda: go_right(part, level).wait_send())
            pl.when(z > level)(lambda: go_left(part, level).wait_send())


def plane_reduce(parts, collective_id):
    blocks, rows, columns = parts.shape
    ep_count, x_count = lax.axis_size("ep"), lax.axis_size("x")
    if x_count != 2 or ep_count % 2 or blocks * rows * columns > 2**24:
        flat = parts.reshape(blocks * rows, columns)
        return lax.psum_scatter(flat, PLANE, scatter_dimension=0, tiled=True).astype(F32)
    depth, half = ep_count // 2, columns // 2

    def buffer(*lead):
        return pltpu.VMEM(lead + (rows, half), parts.dtype)

    def sems(*lead):
        return pltpu.SemaphoreType.DMA(lead)

    return pl.pallas_call(
        functools.partial(reduce_kernel, depth, half),
        out_shape=jax.ShapeDtypeStruct((rows, columns), F32),
        in_specs=[pl.BlockSpec(memory_space=pl.ANY)],
        out_specs=pl.BlockSpec(memory_space=pltpu.VMEM),
        scratch_shapes=[
            buffer(2, depth, 2), buffer(2, depth, 2),
            buffer(2, depth), buffer(2, depth), buffer(2, depth),
            sems(2, depth, 2), sems(2, depth, 2), sems(2, depth, 2),
            sems(2, depth), sems(2, depth), sems(2, depth),
            sems(2, depth), sems(2, depth), sems(2, depth),
        ],
        compiler_params=pltpu.CompilerParams(
            collective_id=collective_id, has_side_effects=True, vmem_limit_bytes=VMEM_BYTES
        ),
        name="plane_reduce",
    )(parts.reshape(depth, 2, 2, rows, columns))


def norm_rows(value, gain):
    inverse = lax.rsqrt(jnp.mean(value * value, axis=-1, keepdims=True) + EPS_NORM)
    return value * inverse * gain


def norm_back(value, gain, grad):
    inverse = lax.rsqrt(jnp.mean(value * value, axis=-1, keepdims=True) + EPS_NORM)
    normed = value * inverse
    lifted = grad * gain
    inner = jnp.mean(lifted * normed, axis=-1, keepdims=True)
    return (lifted - normed * inner) * inverse, jnp.sum(grad * normed, axis=0)


def rms_scale(value, gain, eps):
    return value * lax.rsqrt(jnp.mean(value * value, axis=-1, keepdims=True) + eps) * gain


def rotate(value, cosine, sine):
    half = value.shape[-1] // 2
    first = value[..., :half]
    second = value[..., half:]
    return jnp.concatenate(
        [first * cosine - second * sine, second * cosine + first * sine], axis=-1
    )


def positions(lengths, seq_len):
    ends = jnp.cumsum(lengths)
    starts = ends - lengths
    index = jnp.arange(seq_len, dtype=jnp.int32)
    doc_ids = jnp.sum((index[:, None] >= ends[None, :]).astype(jnp.int32), axis=1)
    member = doc_ids[:, None] == jnp.arange(lengths.shape[0], dtype=jnp.int32)[None, :]
    offset = jnp.sum(jnp.where(member, starts[None, :], 0), axis=1)
    return (doc_ids, index - offset)


def rope_tables(position, head_dim):
    half = head_dim // 2
    freq = ROPE_BASE ** (-(2.0 * jnp.arange(half, dtype=F32)) / head_dim)
    angle = position.astype(F32)[:, None] * freq[None, :]
    return (jnp.cos(angle), jnp.sin(angle))


def einsum(spec, left, right):
    return jnp.einsum(spec, left, right, preferred_element_type=F32)


def swap_cores(value):
    return lax.ppermute(value, "core", [(0, 1), (1, 0)])


def gather(value, axes):
    return lax.all_gather(value, axes, axis=0, tiled=True)


def scatter(value, axes, dim=0):
    return lax.psum_scatter(value, axes, scatter_dimension=dim, tiled=True)


def masked_softmax(logits, mask):
    kept = jnp.where(mask, logits, MASKED)
    lifted = jnp.where(mask, jnp.exp(kept - jnp.max(kept, axis=-1, keepdims=True)), 0.0)
    return lifted / jnp.sum(lifted, axis=-1, keepdims=True)


def route_mask(routes, experts_all):
    ids = jnp.arange(experts_all, dtype=jnp.int32)
    return jnp.any(routes[:, :, None] == ids[None, None, :], axis=1)


def per_device(
    layer_input,
    routes,
    doc_lengths,
    norm1_gain,
    w_qkv,
    q_gain,
    k_gain,
    w_out,
    norm2_gain,
    w_router,
    expert_gate_up,
    expert_down,
    d_out,
):
    rows, width = layer_input.shape
    x_count = lax.axis_size("x")
    ep_count = lax.axis_size("ep")
    seq_len = rows * x_count * 2
    blocks = ep_count * x_count
    topk = routes.shape[1]
    experts_all = w_router.shape[1]
    local = expert_gate_up.shape[0]
    hidden_local = expert_down.shape[1]
    head_dim = q_gain.shape[0]
    qkv_local = w_qkv.shape[2]
    heads = qkv_local // head_dim
    capacity = min(3 * rows * topk // (2 * experts_all), rows)
    q_rows = min(512, seq_len)
    q_count = seq_len // q_rows
    scale = head_dim ** (-0.5)
    my_ep = lax.axis_index("ep")

    gain_one = norm1_gain.astype(F32)
    gain_two = norm2_gain.astype(F32)
    inputs = layer_input.astype(F32)
    grad_out = d_out.astype(F32)
    input_seq = gather(layer_input, GROUP)
    h_seq = norm_rows(input_seq.astype(F32), gain_one).astype(BF16)
    w_parts = w_qkv.transpose(1, 0, 2)
    q_raw, k_raw, v_raw = (
        jnp.dot(h_seq, w_parts[part], preferred_element_type=F32).reshape(
            seq_len, heads, head_dim
        )
        for part in range(3)
    )
    doc_ids, position = positions(doc_lengths[0], seq_len)
    cosine, sine = rope_tables(position, head_dim)
    cosine = cosine[:, None, :]
    sine = sine[:, None, :]

    def shape_heads(value, gain):
        return rotate(rms_scale(value, gain, EPS_HEAD), cosine, sine)

    q_rot, q_back = jax.vjp(shape_heads, q_raw, q_gain.astype(F32))
    k_rot, k_back = jax.vjp(shape_heads, k_raw, k_gain.astype(F32))
    queries = q_rot.astype(BF16)
    keys = k_rot.astype(BF16)
    values = v_raw.astype(BF16)
    q_blocks = queries.reshape(q_count, q_rows, heads, head_dim)
    doc_blocks = doc_ids.reshape(q_count, q_rows)

    def scores_of(q_block, doc_block):
        plain = einsum("qhd,khd->hqk", q_block, keys) * scale
        return jnp.where((doc_block[:, None] == doc_ids[None, :])[None], plain, MASKED)

    def attend(item):
        q_block, doc_block = item
        scores = scores_of(q_block, doc_block)
        peak = jnp.max(scores, axis=-1, keepdims=True)
        lifted = jnp.exp(scores - peak)
        total = jnp.sum(lifted, axis=-1, keepdims=True)
        weights = (lifted / total).astype(BF16)
        return (einsum("hqk,khd->qhd", weights, values), peak, total)

    mixed, peaks, totals = lax.map(attend, (q_blocks, doc_blocks))
    attn_vals = mixed.reshape(seq_len, qkv_local).astype(BF16)
    attn_out = scatter(jnp.dot(attn_vals, w_out, preferred_element_type=F32).astype(BF16), GROUP)
    middle = inputs + attn_out.astype(F32)
    h_two = norm_rows(middle, gain_two).astype(BF16)

    g_plane = gather(d_out, PLANE).reshape(blocks, rows, width)
    routes_plane = spread(routes.T, PLANE, 1).transpose(0, 2, 1).reshape(blocks * rows, topk)
    h_flat = gather(h_two, PLANE)
    h_plane = h_flat.reshape(blocks, rows, width)
    gate_own = expert_gate_up[:, :, 0]
    up_own = expert_gate_up[:, :, 1]
    pair_other = swap_cores(expert_gate_up.reshape(local, width, 2 * hidden_local))
    down_other = swap_cores(expert_down)
    pair_own = expert_gate_up.reshape(local, width, 2 * hidden_local)

    mask_plane = route_mask(routes_plane, experts_all)
    logits_plane = jnp.dot(h_flat, w_router, preferred_element_type=F32)
    probs_plane = masked_softmax(logits_plane, mask_plane)
    first = my_ep * local
    mask_here = lax.dynamic_slice_in_dim(mask_plane, first, local, axis=1)
    probs_here = lax.dynamic_slice_in_dim(probs_plane, first, local, axis=1)
    mask_here = mask_here.reshape(blocks, rows, local).transpose(0, 2, 1)
    probs_here = probs_here.reshape(blocks, rows, local).transpose(0, 2, 1)
    before = jnp.triu(jnp.ones((rows, rows), BF16), 1)
    rank = einsum("bet,tu->beu", mask_here.astype(BF16), before).astype(jnp.int32)
    slots = jnp.arange(capacity, dtype=jnp.int32)[None, None, :, None]
    picks = mask_here[:, :, None, :] & (rank[:, :, None, :] == slots)
    pick = picks.astype(BF16)
    prob_rows = jnp.sum(jnp.where(picks, probs_here[:, :, None, :], 0.0), axis=-1)
    prob_rows = prob_rows.transpose(1, 0, 2)[..., None]

    g_rows = einsum("bect,btd->ebcd", pick, g_plane).astype(BF16)
    h_rows = einsum("bect,btd->ebcd", pick, h_plane).astype(BF16)

    def expert_half(pair, down):
        gate = einsum("ebcd,edf->ebcf", h_rows, pair[:, :, :hidden_local])
        up = einsum("ebcd,edf->ebcf", h_rows, pair[:, :, hidden_local:])
        back = einsum("ebcd,efd->ebcf", g_rows, down)
        sigma = jax.nn.sigmoid(gate)
        silu = gate * sigma
        hidden = (silu * up).astype(BF16).astype(F32)
        dots = jnp.sum(hidden * back, axis=-1)
        weighted = (hidden * prob_rows).astype(BF16)
        grad_hidden = back * prob_rows
        grad_gate = (grad_hidden * up * (sigma + silu * (1.0 - sigma))).astype(BF16)
        grad_up = (grad_hidden * silu).astype(BF16)
        return dots, weighted, jnp.concatenate([grad_gate, grad_up], axis=-1)

    dots_own, weighted_own, ggu_own = expert_half(pair_own, expert_down)
    dots_other, weighted_other, ggu_other = expert_half(pair_other, down_other)
    back_rows = (
        einsum("ebcf,edf->ebcd", ggu_own, pair_own)
        + einsum("ebcf,edf->ebcd", ggu_other, pair_other)
    ).astype(BF16)
    out_rows = (
        einsum("ebcf,efd->ebcd", weighted_own, expert_down)
        + einsum("ebcf,efd->ebcd", weighted_other, down_other)
    ).astype(BF16)
    dot_rows = (dots_own + dots_other).transpose(1, 0, 2)
    dots_token = jnp.sum(jnp.where(picks, dot_rows[..., None], 0.0), axis=2)
    grad_probs = spread(dots_token, PLANE, 2, True)
    grad_probs = jnp.sum(grad_probs.reshape(ep_count, x_count, local, rows), axis=1)
    grad_probs = grad_probs.reshape(experts_all, rows).T
    back_part = einsum("bect,ebcd->btd", pick, back_rows).astype(BF16)
    back_sum = plane_reduce(back_part, 3)
    out_part = einsum("bect,ebcd->btd", pick, out_rows).astype(BF16)

    grad_pair_own = einsum("ebcd,ebcf->edf", h_rows, ggu_own)
    grad_pair_other = einsum("ebcd,ebcf->edf", h_rows, ggu_other)
    grad_down_own = einsum("ebcf,ebcd->efd", weighted_own, g_rows)
    grad_down_other = einsum("ebcf,ebcd->efd", weighted_other, g_rows)
    grad_pair = grad_pair_own + swap_cores(grad_pair_other.astype(BF16)).astype(F32)
    grad_down = grad_down_own + swap_cores(grad_down_other.astype(BF16)).astype(F32)
    grad_gate_up = grad_pair.reshape(local, width, 2, hidden_local)

    mask_own = route_mask(routes, experts_all)
    probs_own = masked_softmax(jnp.dot(h_two, w_router, preferred_element_type=F32), mask_own)
    inner = jnp.sum(probs_own * grad_probs, axis=-1, keepdims=True)
    grad_logits = probs_own * (grad_probs - inner)
    grad_router = jnp.dot(h_two.astype(F32).T, grad_logits, precision=HIGH)
    grad_h_two = back_sum + jnp.dot(
        grad_logits, w_router.astype(F32).T, precision=HIGH
    )
    grad_mid_norm, grad_gain_two = norm_back(middle, gain_two, grad_h_two)
    grad_mid = grad_out + grad_mid_norm

    ga_seq = gather(grad_mid.astype(BF16), GROUP)
    grad_wout = lax.dot_general(
        attn_vals, ga_seq, (((0,), (0,)), ((), ())), preferred_element_type=F32
    )
    grad_vals = lax.dot_general(
        ga_seq, w_out, (((1,), (1,)), ((), ())), preferred_element_type=F32
    )
    grad_mixed = grad_vals.astype(BF16).reshape(q_count, q_rows, heads, head_dim)

    def attend_back(carry, item):
        grad_keys, grad_values = carry
        q_block, doc_block, peak, total, grad_block = item
        scores = scores_of(q_block, doc_block)
        probs_full = jnp.exp(scores - peak) / total
        weights = probs_full.astype(BF16)
        grad_weights = einsum("qhd,khd->hqk", grad_block, values)
        delta = jnp.sum(grad_weights * probs_full, axis=-1, keepdims=True)
        grad_scores = (probs_full * (grad_weights - delta)).astype(BF16)
        grad_q = einsum("hqk,khd->qhd", grad_scores, keys) * scale
        grad_keys = grad_keys + einsum("hqk,qhd->khd", grad_scores, q_block) * scale
        grad_values = grad_values + einsum("hqk,qhd->khd", weights, grad_block)
        return ((grad_keys, grad_values), grad_q)

    head_zeros = jnp.zeros((seq_len, heads, head_dim), F32)
    (grad_keys, grad_values), grad_queries = lax.scan(
        attend_back, (head_zeros, head_zeros), (q_blocks, doc_blocks, peaks, totals, grad_mixed)
    )
    grad_queries = grad_queries.reshape(seq_len, heads, head_dim)
    grad_q_raw, grad_q_gain = q_back(grad_queries)
    grad_k_raw, grad_k_gain = k_back(grad_keys)
    grad_proj = [
        grad.reshape(seq_len, qkv_local).astype(BF16)
        for grad in (grad_q_raw, grad_k_raw, grad_values)
    ]
    grad_h_part = sum(
        lax.dot_general(grad, w, (((1,), (1,)), ((), ())), preferred_element_type=F32)
        for grad, w in zip(grad_proj, w_parts)
    )
    grad_h_one = scatter(grad_h_part.astype(BF16), GROUP).astype(F32)
    grad_wqkv = jnp.stack(
        [
            lax.dot_general(
                h_seq, grad, (((0,), (0,)), ((), ())), preferred_element_type=F32
            ).astype(BF16)
            for grad in grad_proj
        ],
    )
    grad_in_norm, grad_gain_one = norm_back(inputs, gain_one, grad_h_one)
    grad_input = grad_mid + grad_in_norm
    dense_qkv = scatter(grad_wqkv, "ep", 1).astype(F32)
    dense_out = scatter(grad_wout.astype(BF16), "ep", 1).astype(F32)
    out_part, grad_proj = lax.optimization_barrier((out_part, grad_proj))
    output = (middle + plane_reduce(out_part, 4)).astype(BF16)
    grad_router = lax.psum(grad_router, ALL)
    small = jnp.concatenate([grad_gain_one, grad_gain_two, grad_q_gain, grad_k_gain])
    small = jnp.sum(spread(small.reshape(-1, 128), ALL, 5), axis=0).reshape(-1)
    gains = jnp.split(small, (width, 2 * width, 2 * width + head_dim))
    return (
        output,
        grad_input,
        gains[0],
        dense_qkv.transpose(1, 0, 2),
        gains[2],
        gains[3],
        dense_out,
        gains[1],
        grad_router,
        grad_gate_up,
        grad_down,
    )


def solution(mesh):
    ep_count, tp_count = mesh.shape["ep"], mesh.shape["tp"]
    fine = Mesh(mesh.devices.reshape(ep_count, tp_count // 2, 2), ALL)
    in_specs = (
        P(ALL, None),
        P(ALL, None),
        P("ep", None),
        P(),
        P(None, None, GROUP),
        P(),
        P(),
        P(GROUP, None),
        P(),
        P(),
        P("ep", None, None, GROUP),
        P("ep", GROUP, None),
        P(ALL, None),
    )
    out_specs = (
        P(ALL, None),
        P(ALL, None),
        P(),
        P("ep", None, GROUP),
        P(),
        P(),
        P(GROUP, "ep"),
        P(),
        P(),
        P("ep", None, None, GROUP),
        P("ep", GROUP, None),
    )
    return jax.shard_map(
        per_device, mesh=fine, in_specs=in_specs, out_specs=out_specs, check_vma=False
    )
```

```python
import functools
import math

import jax
import jax.numpy as jnp
from jax import lax
from jax.experimental import pallas as pl
from jax.experimental.pallas import tpu as pltpu
from jax.sharding import Mesh
from jax.sharding import PartitionSpec as P


HIGH = lax.Precision.HIGHEST
EPS_NORM = 1e-05
EPS_HEAD = 1e-06
ROPE_BASE = 10000.0
MASKED = -1e30
F32 = jnp.float32
BF16 = jnp.bfloat16
PLANE = ("ep", "x")
GROUP = ("x", "core")
ALL = ("ep", "x", "core")

MESH = pl.DeviceIdType.MESH
VMEM_BYTES = 60 * 1024 * 1024


def remote(source, target, send, recv, where):
    return pltpu.make_async_remote_copy(
        src_ref=source,
        dst_ref=target,
        send_sem=send,
        recv_sem=recv,
        device_id=where,
        device_id_type=MESH,
    )


def greet(where):
    pl.semaphore_signal(
        pltpu.get_barrier_semaphore(), inc=1, device_id=where, device_id_type=MESH
    )


def add_into(target, terms, step=32):
    def body(index, carry):
        at = pl.ds(pl.multiple_of(index * step, step), step)
        total = terms[0][at, :].astype(F32)
        for term in terms[1:]:
            total = total + term[at, :].astype(F32)
        target[at, :] = total.astype(target.dtype)
        return carry

    lax.fori_loop(0, target.shape[0] // step, body, 0)


def peer_of(axes, counts, index):
    where = {}
    for axis, count in reversed(list(zip(axes, counts))):
        where[axis] = lax.rem(index, count)
        index = index // count
    return where


def spread_kernel(axes, counts, own_slices, v_ref, out_ref, local_sem, send, recv):
    total = math.prod(counts)
    me = 0
    for axis, count in zip(axes, counts):
        me = me * count + lax.axis_index(axis)

    def hello(step, carry):
        greet(peer_of(axes, counts, lax.rem(me + step, total)))
        return carry

    lax.fori_loop(1, total, hello, 0)
    pl.semaphore_wait(pltpu.get_barrier_semaphore(), total - 1)

    def copy(step):
        peer = lax.rem(me + step, total)
        source = v_ref.at[peer] if own_slices else v_ref
        return remote(
            source, out_ref.at[me], send.at[step], recv.at[step], peer_of(axes, counts, peer)
        )

    mine = pltpu.make_async_copy(
        v_ref.at[me] if own_slices else v_ref, out_ref.at[me], local_sem
    )
    mine.start()

    def begin(step, carry):
        copy(step).start()
        return carry

    def finish(step, carry):
        copy(step).wait()
        return carry

    lax.fori_loop(1, total, begin, 0)
    mine.wait()
    lax.fori_loop(1, total, finish, 0)


def spread(value, axes, collective_id, own_slices=False):
    counts = tuple(lax.axis_size(axis) for axis in axes)
    total = math.prod(counts)
    shape = value.shape[1:] if own_slices else value.shape
    return pl.pallas_call(
        functools.partial(spread_kernel, axes, counts, own_slices),
        out_shape=jax.ShapeDtypeStruct((total,) + shape, value.dtype),
        in_specs=[pl.BlockSpec(memory_space=pltpu.VMEM)],
        out_specs=pl.BlockSpec(memory_space=pltpu.VMEM),
        scratch_shapes=[
            pltpu.SemaphoreType.DMA,
            pltpu.SemaphoreType.DMA((total,)),
            pltpu.SemaphoreType.DMA((total,)),
        ],
        compiler_params=pltpu.CompilerParams(
            collective_id=collective_id, has_side_effects=True
        ),
        name="spread",
    )(value)


def visiting_order(count):
    order, low, high = [], 0, count - 1
    while low <= high:
        order.append(high)
        high -= 1
        if low <= high:
            order.append(low)
            low += 1
    return order


def reduce_kernel(
    depth, half, p_ref, out_ref, own, one, two, right, left,
    own_sem, s1, r1, s2, r2, sr, rr, sl, rl,
):
    ep = lax.axis_index("ep")
    x = lax.axis_index("x")
    z = ep // 2
    y = lax.rem(ep, 2)
    first = ({"x": 1 - x}, {"ep": z * 2 + 1 - y})
    second = (first[1], first[0])
    up, down = {"ep": ep + 2}, {"ep": ep - 2}
    barrier = pltpu.get_barrier_semaphore()
    greet(first[0])
    greet(first[1])
    pl.when(z < depth - 1)(lambda: greet(up))
    pl.when(z > 0)(lambda: greet(down))
    peers = 2 + (z > 0).astype(jnp.int32) + (z < depth - 1).astype(jnp.int32)
    pl.semaphore_wait(barrier, peers)

    order = visiting_order(depth)
    cols = (pl.ds(0, half), pl.ds(half, half))
    mine = (y, x)

    def block(part, level, step, theirs):
        near = (x, y)[part]
        near = 1 - near if theirs else near
        far = 1 - mine[part] if step == 0 else mine[part]
        at = (far, near) if part == 0 else (near, far)
        return p_ref.at[level, at[0], at[1], :, cols[part]]

    def send_one(part, level, step):
        return remote(
            block(part, level, step, True),
            one.at[part, level, step],
            s1.at[part, level, step],
            r1.at[part, level, step],
            first[part],
        )

    def send_two(part, level):
        return remote(
            one.at[part, level, 0],
            two.at[part, level],
            s2.at[part, level],
            r2.at[part, level],
            second[part],
        )

    def load(part, level, step):
        return pltpu.make_async_copy(
            block(part, level, step, False),
            own.at[part, level, step],
            own_sem.at[part, level, step],
        )

    def go_right(part, level):
        ref = right.at[part, level]
        return remote(ref, ref, sr.at[part, level], rr.at[part, level], up)

    def go_left(part, level):
        ref = left.at[part, level]
        return remote(ref, ref, sl.at[part, level], rl.at[part, level], down)

    for level in order:
        for part in (0, 1):
            send_one(part, level, 0).start()
    for step in (0, 1):
        for level in order:
            for part in (0, 1):
                load(part, level, step).start()
    for level in order:
        for part in (0, 1):
            load(part, level, 0).wait()
            send_one(part, level, 0).wait()
            arrived = one.at[part, level, 0]
            add_into(arrived, [arrived, own.at[part, level, 0]])
            send_two(part, level).start()
            send_one(part, level, 1).start()

    def begin(level):
        for part in (0, 1):
            if level > 0:

                @pl.when(z == 0)
                def _():
                    add_into(right.at[part, level], [two.at[part, level]])
                    go_right(part, level).start()

            if level < depth - 1:

                @pl.when(z == depth - 1)
                def _():
                    add_into(left.at[part, level], [two.at[part, level]])
                    go_left(part, level).start()

    def forward(level):
        for part in (0, 1):

            @pl.when((z > 0) & (z < level))
            def _():
                go_right(part, level).wait_recv()
                ref = right.at[part, level]
                add_into(ref, [ref, two.at[part, level]])
                go_right(part, level).start()

            @pl.when((z < depth - 1) & (z > level))
            def _():
                go_left(part, level).wait_recv()
                ref = left.at[part, level]
                add_into(ref, [ref, two.at[part, level]])
                go_left(part, level).start()

    for turn, level in enumerate(order):
        for part in (0, 1):
            load(part, level, 1).wait()
            send_one(part, level, 1).wait()
            kept = own.at[part, level, 1]
            add_into(kept, [one.at[part, level, 1], kept])
            send_two(part, level).wait()
            add_into(two.at[part, level], [two.at[part, level], kept])
        begin(level)
        if turn > 0:
            forward(order[turn - 1])
    forward(order[-1])
    for level in range(depth):

        @pl.when(z == level)
        def _():
            for part in (0, 1):
                terms = [two.at[part, level]]
                if level > 0:
                    go_right(part, level).wait_recv()
                    terms.append(right.at[part, level])
                if level < depth - 1:
                    go_left(part, level).wait_recv()
                    terms.append(left.at[part, level])
                add_into(out_ref.at[:, cols[part]], terms)

        for part in (0, 1):
            pl.when(z < level)(lambda: go_right(part, level).wait_send())
            pl.when(z > level)(lambda: go_left(part, level).wait_send())


def plane_reduce(parts, collective_id):
    blocks, rows, columns = parts.shape
    ep_count, x_count = lax.axis_size("ep"), lax.axis_size("x")
    if x_count != 2 or ep_count % 2 or blocks * rows * columns > 2**24:
        flat = parts.reshape(blocks * rows, columns)
        return lax.psum_scatter(flat, PLANE, scatter_dimension=0, tiled=True).astype(F32)
    depth, half = ep_count // 2, columns // 2

    def buffer(*lead):
        return pltpu.VMEM(lead + (rows, half), parts.dtype)

    def sems(*lead):
        return pltpu.SemaphoreType.DMA(lead)

    return pl.pallas_call(
        functools.partial(reduce_kernel, depth, half),
        out_shape=jax.ShapeDtypeStruct((rows, columns), F32),
        in_specs=[pl.BlockSpec(memory_space=pl.ANY)],
        out_specs=pl.BlockSpec(memory_space=pltpu.VMEM),
        scratch_shapes=[
            buffer(2, depth, 2), buffer(2, depth, 2),
            buffer(2, depth), buffer(2, depth), buffer(2, depth),
            sems(2, depth, 2), sems(2, depth, 2), sems(2, depth, 2),
            sems(2, depth), sems(2, depth), sems(2, depth),
            sems(2, depth), sems(2, depth), sems(2, depth),
        ],
        compiler_params=pltpu.CompilerParams(
            collective_id=collective_id, has_side_effects=True, vmem_limit_bytes=VMEM_BYTES
        ),
        name="plane_reduce",
    )(parts.reshape(depth, 2, 2, rows, columns))


def turn(value, cosine, sine):
    return value * cosine + pltpu.roll(value, value.shape[-1] // 2, 1) * sine


def turn_back(value, cosine, sine):
    return value * cosine + pltpu.roll(value * sine, value.shape[-1] // 2, 1)


def head_norm(raw):
    inverse = lax.rsqrt(jnp.mean(raw * raw, axis=-1, keepdims=True) + EPS_HEAD)
    return raw * inverse, inverse


def dot_nt(left, right):
    return lax.dot_general(left, right, (((1,), (1,)), ((), ())), preferred_element_type=F32)


def dot_tn(left, right):
    return lax.dot_general(left, right, (((0,), (0,)), ((), ())), preferred_element_type=F32)


def dot_nn(left, right):
    return lax.dot_general(left, right, (((1,), (0,)), ((), ())), preferred_element_type=F32)


def weights_of(q_rows, keys, doc_rows, doc_keys, scale):
    scores = dot_nt(q_rows, keys) * scale
    scores = jnp.where(doc_rows == doc_keys, scores, MASKED)
    lifted = jnp.exp(scores - jnp.max(scores, axis=-1, keepdims=True))
    return lifted / jnp.sum(lifted, axis=-1, keepdims=True)


def attend_kernel(step, q_ref, k_ref, v_ref, qg_ref, kg_ref, cos_ref, sin_ref, dr_ref, dk_ref, o_ref):
    scale = q_ref.shape[-1] ** (-0.5)
    cosine, sine = cos_ref[...], sin_ref[...]
    queries = turn(head_norm(q_ref[...])[0] * qg_ref[...], cosine, sine).astype(BF16)
    keys = turn(head_norm(k_ref[...])[0] * kg_ref[...], cosine, sine).astype(BF16)
    values = v_ref[...].astype(BF16)
    for at in range(0, q_ref.shape[0], step):
        rows = slice(at, at + step)
        weights = weights_of(queries[rows], keys, dr_ref[rows, :], dk_ref[...], scale)
        o_ref[rows, :] = dot_nn(weights.astype(BF16), values).astype(BF16)


def attend_back_kernel(
    step, q_ref, k_ref, v_ref, go_ref, qg_ref, kg_ref, cos_ref, sin_ref, dr_ref, dk_ref,
    gq_ref, gk_ref, gv_ref, gqg_ref, gkg_ref,
):
    scale = q_ref.shape[-1] ** (-0.5)
    cosine, sine = cos_ref[...], sin_ref[...]
    q_normed, q_inverse = head_norm(q_ref[...])
    k_normed, k_inverse = head_norm(k_ref[...])
    queries = turn(q_normed * qg_ref[...], cosine, sine).astype(BF16)
    keys = turn(k_normed * kg_ref[...], cosine, sine).astype(BF16)
    values = v_ref[...].astype(BF16)
    grad_keys = jnp.zeros(k_ref.shape, F32)
    grad_values = jnp.zeros(v_ref.shape, F32)
    grad_queries = []
    for at in range(0, q_ref.shape[0], step):
        rows = slice(at, at + step)
        probs = weights_of(queries[rows], keys, dr_ref[rows, :], dk_ref[...], scale)
        grad_rows = go_ref[rows, :]
        grad_weights = dot_nt(grad_rows, values)
        delta = jnp.sum(grad_weights * probs, axis=-1, keepdims=True)
        grad_scores = (probs * (grad_weights - delta)).astype(BF16)
        grad_queries.append(dot_nn(grad_scores, keys))
        grad_keys = grad_keys + dot_tn(grad_scores, queries[rows])
        grad_values = grad_values + dot_tn(probs.astype(BF16), grad_rows)

    @pl.when(pl.program_id(0) == 0)
    def _():
        gqg_ref[...] = jnp.zeros_like(gqg_ref)
        gkg_ref[...] = jnp.zeros_like(gkg_ref)

    def finish(grad, normed, inverse, gain_ref, out_ref, gain_grad_ref):
        grad = turn_back(grad * scale, cosine, sine)
        gain_grad_ref[...] += jnp.sum(grad * normed, axis=0, keepdims=True)
        lifted = grad * gain_ref[...]
        inner = jnp.mean(lifted * normed, axis=-1, keepdims=True)
        out_ref[...] = ((lifted - normed * inner) * inverse).astype(BF16)

    finish(jnp.concatenate(grad_queries, axis=0), q_normed, q_inverse, qg_ref, gq_ref, gqg_ref)
    finish(grad_keys, k_normed, k_inverse, kg_ref, gk_ref, gkg_ref)
    gv_ref[...] = grad_values.astype(BF16)


def attention_call(kernel, heads, head_dim, seq_len, values, tables, outs, flops):
    column = pl.BlockSpec((seq_len, head_dim), lambda head: (0, head))
    whole = [pl.BlockSpec(t.shape, lambda head: (0, 0)) for t in tables]
    shapes = [
        jax.ShapeDtypeStruct((seq_len, heads * head_dim), BF16) if wide
        else jax.ShapeDtypeStruct((1, head_dim), F32)
        for wide in outs
    ]
    specs = [column if wide else pl.BlockSpec((1, head_dim), lambda head: (0, 0)) for wide in outs]
    return pl.pallas_call(
        functools.partial(kernel, min(512, seq_len)),
        grid=(heads,),
        out_shape=shapes,
        in_specs=[column] * len(values) + whole,
        out_specs=specs,
        compiler_params=pltpu.CompilerParams(vmem_limit_bytes=VMEM_BYTES),
        cost_estimate=pl.CostEstimate(
            flops=flops, bytes_accessed=16 * seq_len * heads * head_dim, transcendentals=heads * seq_len**2
        ),
        name="attention",
    )(*values, *tables)


def params(flops, moved):
    return dict(compiler_params=pltpu.CompilerParams(vmem_limit_bytes=VMEM_BYTES),
        cost_estimate=pl.CostEstimate(flops=flops, bytes_accessed=moved, transcendentals=0))


def combine_kernel(pick_ref, value_ref, out_ref):
    local, _, capacity, width = value_ref.shape
    out_ref[0] = dot_tn(pick_ref[0], value_ref[...].reshape(local*capacity, width)).astype(BF16)


def combine(pick, value):
    blocks, picked, rows = pick.shape
    local, _, capacity, width = value.shape
    return pl.pallas_call(
        combine_kernel, grid=(blocks,),
        out_shape=jax.ShapeDtypeStruct((blocks, rows, width), BF16),
        in_specs=[pl.BlockSpec((1, picked, rows), lambda b: (b, 0, 0)), pl.BlockSpec((local, 1, capacity, width), lambda b: (0, b, 0, 0))],
        out_specs=pl.BlockSpec((1, rows, width), lambda b: (b, 0, 0)),
        name="combine", **params(2*blocks*picked*rows*width, 2*blocks*width*(picked+rows)),
    )(pick, value)


def expert_kernel(x_ref, w0_ref, w1_ref, u0_ref, u1_ref, pr_ref, gx_ref, dots_ref, *outs):
    x = x_ref[0]
    prob = pr_ref[0]
    total = None
    dots = None
    for w_ref, u_ref, hp_ref, ggu_ref in ((w0_ref, u0_ref, outs[0], outs[2]), (w1_ref, u1_ref, outs[1], outs[3])):
        n = u_ref.shape[-1]
        both = dot_nn(x, w_ref[0])
        gate, up = both[:, :n], both[:, n:]
        sigma = jax.nn.sigmoid(gate)
        silu = gate * sigma
        hidden = (silu * up).astype(BF16).astype(F32)
        back = u_ref[0]
        part = jnp.sum(hidden * back, axis=-1, keepdims=True)
        dots = part if dots is None else dots + part
        hp_ref[0] = (hidden * prob).astype(BF16)
        gh = back * prob
        ggu_ref[0, :, :n] = (gh * up * (sigma + silu * (1.0 - sigma))).astype(BF16)
        ggu_ref[0, :, n:] = (gh * silu).astype(BF16)
        part = dot_nt(ggu_ref[0], w_ref[0])
        total = part if total is None else total + part
    gx_ref[0] = total.astype(BF16)
    dots_ref[0] = dots


def expert(x, w0, w1, u0, u1, prob, step):
    local, count, width = x.shape
    n = u0.shape[-1]
    r = lambda c: pl.BlockSpec((1, step, c), lambda e, i: (e, i, 0))
    w = pl.BlockSpec((1, width, 2*n), lambda e, i: (e, 0, 0))
    s = lambda c, t: jax.ShapeDtypeStruct((local, count, c), t)
    return pl.pallas_call(
        expert_kernel, grid=(local, count//step),
        out_shape=[s(width,BF16), s(1,F32), s(n,BF16), s(n,BF16), s(2*n,BF16), s(2*n,BF16)],
        in_specs=[r(width), w, w, r(n), r(n), r(1)],
        out_specs=[r(width), r(1), r(n), r(n), r(2*n), r(2*n)],
        name="expert", **params(16*local*count*width*n, local*(count*(width*4+n*20)+8*width*n)),
    )(x, w0, w1, u0, u1, prob)


def norm_rows(value, gain):
    inverse = lax.rsqrt(jnp.mean(value * value, axis=-1, keepdims=True) + EPS_NORM)
    return value * inverse * gain


def norm_back(value, gain, grad):
    inverse = lax.rsqrt(jnp.mean(value * value, axis=-1, keepdims=True) + EPS_NORM)
    normed = value * inverse
    lifted = grad * gain
    inner = jnp.mean(lifted * normed, axis=-1, keepdims=True)
    return (lifted - normed * inner) * inverse, jnp.sum(grad * normed, axis=0)


def positions(lengths, seq_len):
    ends = jnp.cumsum(lengths)
    starts = ends - lengths
    index = jnp.arange(seq_len, dtype=jnp.int32)
    doc_ids = jnp.sum((index[:, None] >= ends[None, :]).astype(jnp.int32), axis=1)
    member = doc_ids[:, None] == jnp.arange(lengths.shape[0], dtype=jnp.int32)[None, :]
    offset = jnp.sum(jnp.where(member, starts[None, :], 0), axis=1)
    return (doc_ids, index - offset)


def rope_tables(position, head_dim):
    half = head_dim // 2
    freq = ROPE_BASE ** (-(2.0 * jnp.arange(half, dtype=F32)) / head_dim)
    angle = position.astype(F32)[:, None] * freq[None, :]
    return (jnp.cos(angle), jnp.sin(angle))


def einsum(spec, left, right):
    return jnp.einsum(spec, left, right, preferred_element_type=F32)


def swap_cores(value):
    return lax.ppermute(value, "core", [(0, 1), (1, 0)])


def gather(value, axes):
    return lax.all_gather(value, axes, axis=0, tiled=True)


def scatter(value, axes, dim=0):
    return lax.psum_scatter(value, axes, scatter_dimension=dim, tiled=True)


def masked_softmax(logits, mask):
    kept = jnp.where(mask, logits, MASKED)
    lifted = jnp.where(mask, jnp.exp(kept - jnp.max(kept, axis=-1, keepdims=True)), 0.0)
    return lifted / jnp.sum(lifted, axis=-1, keepdims=True)


def route_mask(routes, experts_all):
    ids = jnp.arange(experts_all, dtype=jnp.int32)
    return jnp.any(routes[:, :, None] == ids[None, None, :], axis=1)


def per_device(
    layer_input,
    routes,
    doc_lengths,
    norm1_gain,
    w_qkv,
    q_gain,
    k_gain,
    w_out,
    norm2_gain,
    w_router,
    expert_gate_up,
    expert_down,
    d_out,
):
    rows, width = layer_input.shape
    x_count = lax.axis_size("x")
    ep_count = lax.axis_size("ep")
    seq_len = rows * x_count * 2
    blocks = ep_count * x_count
    topk = routes.shape[1]
    experts_all = w_router.shape[1]
    local = expert_gate_up.shape[0]
    hidden_local = expert_down.shape[1]
    head_dim = q_gain.shape[0]
    qkv_local = w_qkv.shape[2]
    heads = qkv_local // head_dim
    capacity = min(3 * rows * topk // (2 * experts_all), rows)
    my_ep = lax.axis_index("ep")

    gain_one = norm1_gain.astype(F32)
    gain_two = norm2_gain.astype(F32)
    inputs = layer_input.astype(F32)
    grad_out = d_out.astype(F32)
    input_seq = gather(layer_input, GROUP)
    g_flat = gather(d_out, PLANE)
    h_seq = norm_rows(input_seq.astype(F32), gain_one).astype(BF16)
    w_parts = w_qkv.transpose(1, 0, 2)
    raw = [jnp.dot(h_seq, w_parts[part], preferred_element_type=F32) for part in range(3)]
    doc_ids, position = positions(doc_lengths[0], seq_len)
    cosine, sine = rope_tables(position, head_dim)
    tables = (
        q_gain.astype(F32)[None],
        k_gain.astype(F32)[None],
        jnp.concatenate([cosine, cosine], axis=1),
        jnp.concatenate([-sine, sine], axis=1),
        doc_ids[:, None],
        doc_ids[None, :],
    )
    (attn_vals,) = attention_call(
        attend_kernel, heads, head_dim, seq_len, raw, tables, (True,), 4 * seq_len**2 * qkv_local
    )
    attn_out = scatter(jnp.dot(attn_vals, w_out, preferred_element_type=F32).astype(BF16), GROUP)
    middle = inputs + attn_out.astype(F32)
    h_two = norm_rows(middle, gain_two).astype(BF16)

    g_plane = g_flat.reshape(blocks, rows, width)
    routes_plane = spread(routes.T, PLANE, 1).transpose(0, 2, 1).reshape(blocks * rows, topk)
    h_flat = gather(h_two, PLANE)
    pair_other = swap_cores(expert_gate_up.reshape(local, width, 2 * hidden_local))
    down_other = swap_cores(expert_down)
    pair_own = expert_gate_up.reshape(local, width, 2 * hidden_local)

    mask_plane = route_mask(routes_plane, experts_all)
    first = my_ep * local
    mask_here = lax.dynamic_slice_in_dim(mask_plane, first, local, axis=1)
    mask_here = mask_here.reshape(blocks, rows, local).transpose(0, 2, 1)
    before = jnp.triu(jnp.ones((rows, rows), BF16), 1)
    rank = einsum("bet,tu->beu", mask_here.astype(BF16), before).astype(jnp.int32)
    slots = jnp.arange(capacity, dtype=jnp.int32)[None, None, :, None]
    picks = mask_here[:, :, None, :] & (rank[:, :, None, :] == slots)
    pick = picks.astype(BF16)
    pick_rows = pick.reshape(blocks, local * capacity, rows)
    count = blocks * capacity

    g_rows = einsum("bect,btd->ebcd", pick, g_plane).astype(BF16)
    back_own = einsum("ebcd,efd->ebcf", g_rows, expert_down).reshape(local, count, -1)
    back_other = einsum("ebcd,efd->ebcf", g_rows, down_other).reshape(local, count, -1)
    h_flat, back_own, back_other = lax.optimization_barrier((h_flat, back_own, back_other))
    h_plane = h_flat.reshape(blocks, rows, width)
    h_rows = einsum("bect,btd->ebcd", pick, h_plane).astype(BF16)
    logits_plane = jnp.dot(h_flat, w_router, preferred_element_type=F32)
    probs_plane = masked_softmax(logits_plane, mask_plane)
    probs_here = lax.dynamic_slice_in_dim(probs_plane, first, local, axis=1)
    probs_here = probs_here.reshape(blocks, rows, local).transpose(0, 2, 1)
    prob_rows = jnp.sum(jnp.where(picks, probs_here[:, :, None, :], 0.0), axis=-1)
    prob_rows = prob_rows.transpose(1, 0, 2).reshape(local, count, 1)
    h_rows = h_rows.reshape(local, count, width)
    g_rows = g_rows.reshape(local, count, width)
    back_rows, dot_rows, weighted_own, weighted_other, ggu_own, ggu_other = expert(
        h_rows, pair_own, pair_other, back_own, back_other, prob_rows, min(384, count)
    )
    dot_rows = dot_rows.reshape(local, blocks, capacity).transpose(1, 0, 2)
    dots_token = jnp.sum(jnp.where(picks, dot_rows[..., None], 0.0), axis=2)
    grad_probs = spread(dots_token, PLANE, 2, True)
    grad_probs = jnp.sum(grad_probs.reshape(ep_count, x_count, local, rows), axis=1)
    grad_probs = grad_probs.reshape(experts_all, rows).T
    back_part = combine(pick_rows, back_rows.reshape(local, blocks, capacity, width))
    back_sum = plane_reduce(back_part, 3)
    out_rows = (
        einsum("emf,efd->emd", weighted_own, expert_down)
        + einsum("emf,efd->emd", weighted_other, down_other)
    ).astype(BF16)
    out_part = combine(pick_rows, out_rows.reshape(local, blocks, capacity, width))

    grad_pair_own = einsum("emd,emf->edf", h_rows, ggu_own)
    grad_pair_other = einsum("emd,emf->edf", h_rows, ggu_other)
    grad_down_own = einsum("emf,emd->efd", weighted_own, g_rows)
    grad_down_other = einsum("emf,emd->efd", weighted_other, g_rows)
    grad_pair = grad_pair_own + swap_cores(grad_pair_other.astype(BF16)).astype(F32)
    grad_down = grad_down_own + swap_cores(grad_down_other.astype(BF16)).astype(F32)
    grad_gate_up = grad_pair.reshape(local, width, 2, hidden_local)

    mask_own = route_mask(routes, experts_all)
    probs_own = masked_softmax(jnp.dot(h_two, w_router, preferred_element_type=F32), mask_own)
    inner = jnp.sum(probs_own * grad_probs, axis=-1, keepdims=True)
    grad_logits = probs_own * (grad_probs - inner)
    grad_router = jnp.dot(h_two.astype(F32).T, grad_logits, precision=HIGH)
    grad_h_two = back_sum + jnp.dot(
        grad_logits, w_router.astype(F32).T, precision=HIGH
    )
    grad_mid_norm, grad_gain_two = norm_back(middle, gain_two, grad_h_two)
    grad_mid = grad_out + grad_mid_norm

    ga_seq = gather(grad_mid.astype(BF16), GROUP)
    ga_seq, out_part = lax.optimization_barrier((ga_seq, out_part))
    grad_wout = lax.dot_general(
        attn_vals, ga_seq, (((0,), (0,)), ((), ())), preferred_element_type=F32
    )
    grad_vals = lax.dot_general(
        ga_seq, w_out, (((1,), (1,)), ((), ())), preferred_element_type=F32
    )
    *grad_proj, grad_q_gain, grad_k_gain = attention_call(
        attend_back_kernel,
        heads,
        head_dim,
        seq_len,
        (*raw, grad_vals.astype(BF16)),
        tables,
        (True, True, True, False, False),
        10 * seq_len**2 * qkv_local,
    )
    grad_h_part = sum(
        lax.dot_general(grad, w, (((1,), (1,)), ((), ())), preferred_element_type=F32)
        for grad, w in zip(grad_proj, w_parts)
    )
    grad_h_one = scatter(grad_h_part.astype(BF16), GROUP).astype(F32)
    grad_wqkv = jnp.stack(
        [
            lax.dot_general(
                h_seq, grad, (((0,), (0,)), ((), ())), preferred_element_type=F32
            ).astype(BF16)
            for grad in grad_proj
        ],
    )
    grad_in_norm, grad_gain_one = norm_back(inputs, gain_one, grad_h_one)
    grad_input = grad_mid + grad_in_norm
    dense_qkv = scatter(grad_wqkv, "ep", 1).astype(F32)
    dense_out = scatter(grad_wout.astype(BF16), "ep", 1).astype(F32)
    out_part, grad_proj = lax.optimization_barrier((out_part, grad_proj))
    output = (middle + plane_reduce(out_part, 4)).astype(BF16)
    grad_router = lax.psum(grad_router, ALL)
    small = jnp.concatenate([grad_gain_one, grad_gain_two, grad_q_gain[0], grad_k_gain[0]])
    small = jnp.sum(spread(small.reshape(-1, 128), ALL, 5), axis=0).reshape(-1)
    gains = jnp.split(small, (width, 2 * width, 2 * width + head_dim))
    return (
        output,
        grad_input,
        gains[0],
        dense_qkv.transpose(1, 0, 2),
        gains[2],
        gains[3],
        dense_out,
        gains[1],
        grad_router,
        grad_gate_up,
        grad_down,
    )


def solution(mesh):
    ep_count, tp_count = mesh.shape["ep"], mesh.shape["tp"]
    fine = Mesh(mesh.devices.reshape(ep_count, tp_count // 2, 2), ALL)
    in_specs = (
        P(ALL, None),
        P(ALL, None),
        P("ep", None),
        P(),
        P(None, None, GROUP),
        P(),
        P(),
        P(GROUP, None),
        P(),
        P(),
        P("ep", None, None, GROUP),
        P("ep", GROUP, None),
        P(ALL, None),
    )
    out_specs = (
        P(ALL, None),
        P(ALL, None),
        P(),
        P("ep", None, GROUP),
        P(),
        P(),
        P(GROUP, "ep"),
        P(),
        P(),
        P("ep", None, None, GROUP),
        P("ep", GROUP, None),
    )

    return jax.shard_map(
        per_device, mesh=fine, in_specs=in_specs, out_specs=out_specs, check_vma=False
    )
```

```python
import functools
import math

import jax
import jax.numpy as jnp
from jax import lax
from jax.experimental import pallas as pl
from jax.experimental.pallas import tpu as pltpu
from jax.sharding import Mesh
from jax.sharding import PartitionSpec as P


HIGH = lax.Precision.HIGHEST
EPS_NORM = 1e-05
EPS_HEAD = 1e-06
ROPE_BASE = 10000.0
MASKED = -1e30
F32 = jnp.float32
BF16 = jnp.bfloat16
PLANE = ("ep", "x")
GROUP = ("x", "core")
ALL = ("ep", "x", "core")

MESH = pl.DeviceIdType.MESH
VMEM_BYTES = 60 * 1024 * 1024


def remote(source, target, send, recv, where):
    return pltpu.make_async_remote_copy(
        src_ref=source,
        dst_ref=target,
        send_sem=send,
        recv_sem=recv,
        device_id=where,
        device_id_type=MESH,
    )


def greet(where):
    pl.semaphore_signal(
        pltpu.get_barrier_semaphore(), inc=1, device_id=where, device_id_type=MESH
    )


def add_into(target, terms, step=32):
    def body(index, carry):
        at = pl.ds(pl.multiple_of(index * step, step), step)
        total = terms[0][at, :].astype(F32)
        for term in terms[1:]:
            total = total + term[at, :].astype(F32)
        target[at, :] = total.astype(target.dtype)
        return carry

    lax.fori_loop(0, target.shape[0] // step, body, 0)


def peer_of(axes, counts, index):
    where = {}
    for axis, count in reversed(list(zip(axes, counts))):
        where[axis] = lax.rem(index, count)
        index = index // count
    return where


def spread_kernel(axes, counts, own_slices, v_ref, out_ref, local_sem, send, recv):
    total = math.prod(counts)
    me = 0
    for axis, count in zip(axes, counts):
        me = me * count + lax.axis_index(axis)

    def hello(step, carry):
        greet(peer_of(axes, counts, lax.rem(me + step, total)))
        return carry

    lax.fori_loop(1, total, hello, 0)
    pl.semaphore_wait(pltpu.get_barrier_semaphore(), total - 1)

    def copy(step):
        peer = lax.rem(me + step, total)
        source = v_ref.at[peer] if own_slices else v_ref
        return remote(
            source, out_ref.at[me], send.at[step], recv.at[step], peer_of(axes, counts, peer)
        )

    mine = pltpu.make_async_copy(
        v_ref.at[me] if own_slices else v_ref, out_ref.at[me], local_sem
    )
    mine.start()

    def begin(step, carry):
        copy(step).start()
        return carry

    def finish(step, carry):
        copy(step).wait()
        return carry

    lax.fori_loop(1, total, begin, 0)
    mine.wait()
    lax.fori_loop(1, total, finish, 0)


def spread(value, axes, collective_id, own_slices=False):
    counts = tuple(lax.axis_size(axis) for axis in axes)
    total = math.prod(counts)
    shape = value.shape[1:] if own_slices else value.shape
    return pl.pallas_call(
        functools.partial(spread_kernel, axes, counts, own_slices),
        out_shape=jax.ShapeDtypeStruct((total,) + shape, value.dtype),
        in_specs=[pl.BlockSpec(memory_space=pltpu.VMEM)],
        out_specs=pl.BlockSpec(memory_space=pltpu.VMEM),
        scratch_shapes=[
            pltpu.SemaphoreType.DMA,
            pltpu.SemaphoreType.DMA((total,)),
            pltpu.SemaphoreType.DMA((total,)),
        ],
        compiler_params=pltpu.CompilerParams(
            collective_id=collective_id, has_side_effects=True
        ),
        name="spread",
    )(value)


def visiting_order(count):
    order, low, high = [], 0, count - 1
    while low <= high:
        order.append(high)
        high -= 1
        if low <= high:
            order.append(low)
            low += 1
    return order


def reduce_kernel(
    depth, half, p_ref, out_ref, own, one, two, right, left,
    own_sem, s1, r1, s2, r2, sr, rr, sl, rl,
):
    ep = lax.axis_index("ep")
    x = lax.axis_index("x")
    z = ep // 2
    y = lax.rem(ep, 2)
    first = ({"x": 1 - x}, {"ep": z * 2 + 1 - y})
    second = (first[1], first[0])
    up, down = {"ep": ep + 2}, {"ep": ep - 2}
    barrier = pltpu.get_barrier_semaphore()
    greet(first[0])
    greet(first[1])
    pl.when(z < depth - 1)(lambda: greet(up))
    pl.when(z > 0)(lambda: greet(down))
    peers = 2 + (z > 0).astype(jnp.int32) + (z < depth - 1).astype(jnp.int32)
    pl.semaphore_wait(barrier, peers)

    order = visiting_order(depth)
    cols = (pl.ds(0, half), pl.ds(half, half))
    mine = (y, x)

    def block(part, level, step, theirs):
        near = (x, y)[part]
        near = 1 - near if theirs else near
        far = 1 - mine[part] if step == 0 else mine[part]
        at = (far, near) if part == 0 else (near, far)
        return p_ref.at[level, at[0], at[1], :, cols[part]]

    def send_one(part, level, step):
        return remote(
            block(part, level, step, True),
            one.at[part, level, step],
            s1.at[part, level, step],
            r1.at[part, level, step],
            first[part],
        )

    def send_two(part, level):
        return remote(
            one.at[part, level, 0],
            two.at[part, level],
            s2.at[part, level],
            r2.at[part, level],
            second[part],
        )

    def load(part, level, step):
        return pltpu.make_async_copy(
            block(part, level, step, False),
            own.at[part, level, step],
            own_sem.at[part, level, step],
        )

    def go_right(part, level):
        ref = right.at[part, level]
        return remote(ref, ref, sr.at[part, level], rr.at[part, level], up)

    def go_left(part, level):
        ref = left.at[part, level]
        return remote(ref, ref, sl.at[part, level], rl.at[part, level], down)

    for level in order:
        for part in (0, 1):
            send_one(part, level, 0).start()
    for step in (0, 1):
        for level in order:
            for part in (0, 1):
                load(part, level, step).start()
    for level in order:
        for part in (0, 1):
            load(part, level, 0).wait()
            send_one(part, level, 0).wait()
            arrived = one.at[part, level, 0]
            add_into(arrived, [arrived, own.at[part, level, 0]])
            send_two(part, level).start()
            send_one(part, level, 1).start()

    def begin(level):
        for part in (0, 1):
            if level > 0:

                @pl.when(z == 0)
                def _():
                    add_into(right.at[part, level], [two.at[part, level]])
                    go_right(part, level).start()

            if level < depth - 1:

                @pl.when(z == depth - 1)
                def _():
                    add_into(left.at[part, level], [two.at[part, level]])
                    go_left(part, level).start()

    def forward(level):
        for part in (0, 1):

            @pl.when((z > 0) & (z < level))
            def _():
                go_right(part, level).wait_recv()
                ref = right.at[part, level]
                add_into(ref, [ref, two.at[part, level]])
                go_right(part, level).start()

            @pl.when((z < depth - 1) & (z > level))
            def _():
                go_left(part, level).wait_recv()
                ref = left.at[part, level]
                add_into(ref, [ref, two.at[part, level]])
                go_left(part, level).start()

    for turn, level in enumerate(order):
        for part in (0, 1):
            load(part, level, 1).wait()
            send_one(part, level, 1).wait()
            kept = own.at[part, level, 1]
            add_into(kept, [one.at[part, level, 1], kept])
            send_two(part, level).wait()
            add_into(two.at[part, level], [two.at[part, level], kept])
        begin(level)
        if turn > 0:
            forward(order[turn - 1])
    forward(order[-1])
    for level in range(depth):

        @pl.when(z == level)
        def _():
            for part in (0, 1):
                terms = [two.at[part, level]]
                if level > 0:
                    go_right(part, level).wait_recv()
                    terms.append(right.at[part, level])
                if level < depth - 1:
                    go_left(part, level).wait_recv()
                    terms.append(left.at[part, level])
                add_into(out_ref.at[:, cols[part]], terms)

        for part in (0, 1):
            pl.when(z < level)(lambda: go_right(part, level).wait_send())
            pl.when(z > level)(lambda: go_left(part, level).wait_send())


def plane_reduce(parts, collective_id):
    blocks, rows, columns = parts.shape
    ep_count, x_count = lax.axis_size("ep"), lax.axis_size("x")
    if x_count != 2 or ep_count % 2 or blocks * rows * columns > 2**24:
        flat = parts.reshape(blocks * rows, columns)
        return lax.psum_scatter(flat, PLANE, scatter_dimension=0, tiled=True).astype(F32)
    depth, half = ep_count // 2, columns // 2

    def buffer(*lead):
        return pltpu.VMEM(lead + (rows, half), parts.dtype)

    def sems(*lead):
        return pltpu.SemaphoreType.DMA(lead)

    return pl.pallas_call(
        functools.partial(reduce_kernel, depth, half),
        out_shape=jax.ShapeDtypeStruct((rows, columns), F32),
        in_specs=[pl.BlockSpec(memory_space=pl.ANY)],
        out_specs=pl.BlockSpec(memory_space=pltpu.VMEM),
        scratch_shapes=[
            buffer(2, depth, 2), buffer(2, depth, 2),
            buffer(2, depth), buffer(2, depth), buffer(2, depth),
            sems(2, depth, 2), sems(2, depth, 2), sems(2, depth, 2),
            sems(2, depth), sems(2, depth), sems(2, depth),
            sems(2, depth), sems(2, depth), sems(2, depth),
        ],
        compiler_params=pltpu.CompilerParams(
            collective_id=collective_id, has_side_effects=True, vmem_limit_bytes=VMEM_BYTES
        ),
        name="plane_reduce",
    )(parts.reshape(depth, 2, 2, rows, columns))


def group_kernel(pieces, p_ref, out_ref, near, far, kept, got, own_sem, s1, r1, s2, r2, s3, r3):
    x, core = lax.axis_index("x"), lax.axis_index("core")
    partner, across = {"core": 1 - core}, {"x": 1 - x}
    greet(partner)
    greet(across)
    pl.semaphore_wait(pltpu.get_barrier_semaphore(), 2)
    step = out_ref.shape[0] // pieces

    def at(piece):
        return pl.ds(piece * step, step)

    def hand_over(piece):
        return remote(
            p_ref.at[1 - x, 1 - core, at(piece), :],
            near.at[at(piece), :],
            s1.at[piece],
            r1.at[piece],
            partner,
        )

    def send_across(piece):
        return remote(
            far.at[at(piece), :], got.at[at(piece), :], s2.at[piece], r2.at[piece], across
        )

    stay = remote(p_ref.at[x, 1 - core], kept.at[0], s3, r3, partner)
    loads = (
        pltpu.make_async_copy(p_ref.at[1 - x, core], far, own_sem.at[0]),
        pltpu.make_async_copy(p_ref.at[x, core], kept.at[1], own_sem.at[1]),
    )
    loads[0].start()
    for piece in range(pieces):
        hand_over(piece).start()
    stay.start()
    loads[1].start()
    loads[0].wait()
    for piece in range(pieces):
        hand_over(piece).wait()
        mine = far.at[at(piece), :]
        add_into(mine, [mine, near.at[at(piece), :]])
        send_across(piece).start()
    loads[1].wait()
    stay.wait()
    for piece in range(pieces):
        send_across(piece).wait()
        rows = at(piece)
        add_into(
            out_ref.at[rows, :], [kept.at[0, rows, :], kept.at[1, rows, :], got.at[rows, :]]
        )


def group_reduce(parts, collective_id):
    if lax.axis_size("x") != 2:
        return scatter(parts, GROUP).astype(F32)
    rows, columns = parts.shape[0] // 4, parts.shape[1]
    pieces = 4

    def sems(*lead):
        return pltpu.SemaphoreType.DMA(lead)

    return pl.pallas_call(
        functools.partial(group_kernel, pieces),
        out_shape=jax.ShapeDtypeStruct((rows, columns), F32),
        in_specs=[pl.BlockSpec(memory_space=pl.ANY)],
        out_specs=pl.BlockSpec(memory_space=pltpu.VMEM),
        scratch_shapes=[
            pltpu.VMEM((rows, columns), BF16),
            pltpu.VMEM((rows, columns), BF16),
            pltpu.VMEM((2, rows, columns), BF16),
            pltpu.VMEM((rows, columns), BF16),
            sems(2),
            sems(pieces),
            sems(pieces),
            sems(pieces),
            sems(pieces),
            pltpu.SemaphoreType.DMA,
            pltpu.SemaphoreType.DMA,
        ],
        compiler_params=pltpu.CompilerParams(collective_id=collective_id, has_side_effects=True),
        name="group_reduce",
    )(parts.reshape(2, 2, rows, columns))


def turn(value, cosine, sine):
    return value * cosine + pltpu.roll(value, value.shape[-1] // 2, 1) * sine


def turn_back(value, cosine, sine):
    return value * cosine + pltpu.roll(value * sine, value.shape[-1] // 2, 1)


def head_norm(raw):
    inverse = lax.rsqrt(jnp.mean(raw * raw, axis=-1, keepdims=True) + EPS_HEAD)
    return raw * inverse, inverse


def dot_nt(left, right):
    return lax.dot_general(left, right, (((1,), (1,)), ((), ())), preferred_element_type=F32)


def dot_tn(left, right):
    return lax.dot_general(left, right, (((0,), (0,)), ((), ())), preferred_element_type=F32)


def dot_nn(left, right):
    return lax.dot_general(left, right, (((1,), (0,)), ((), ())), preferred_element_type=F32)


def weights_of(q_rows, keys, doc_rows, doc_keys, scale):
    scores = dot_nt(q_rows, keys) * scale
    scores = jnp.where(doc_rows == doc_keys, scores, MASKED)
    lifted = jnp.exp(scores - jnp.max(scores, axis=-1, keepdims=True))
    return lifted / jnp.sum(lifted, axis=-1, keepdims=True)


def attend_kernel(step, q_ref, k_ref, v_ref, qg_ref, kg_ref, cos_ref, sin_ref, dr_ref, dk_ref, o_ref):
    scale = q_ref.shape[-1] ** (-0.5)
    cosine, sine = cos_ref[...], sin_ref[...]
    queries = turn(head_norm(q_ref[...])[0] * qg_ref[...], cosine, sine).astype(BF16)
    keys = turn(head_norm(k_ref[...])[0] * kg_ref[...], cosine, sine).astype(BF16)
    values = v_ref[...].astype(BF16)
    for at in range(0, q_ref.shape[0], step):
        rows = slice(at, at + step)
        weights = weights_of(queries[rows], keys, dr_ref[rows, :], dk_ref[...], scale)
        o_ref[rows, :] = dot_nn(weights.astype(BF16), values).astype(BF16)


def attend_back_kernel(
    step, q_ref, k_ref, v_ref, go_ref, qg_ref, kg_ref, cos_ref, sin_ref, dr_ref, dk_ref,
    gq_ref, gk_ref, gv_ref, gqg_ref, gkg_ref,
):
    scale = q_ref.shape[-1] ** (-0.5)
    cosine, sine = cos_ref[...], sin_ref[...]
    q_normed, q_inverse = head_norm(q_ref[...])
    k_normed, k_inverse = head_norm(k_ref[...])
    queries = turn(q_normed * qg_ref[...], cosine, sine).astype(BF16)
    keys = turn(k_normed * kg_ref[...], cosine, sine).astype(BF16)
    values = v_ref[...].astype(BF16)
    grad_keys = jnp.zeros(k_ref.shape, F32)
    grad_values = jnp.zeros(v_ref.shape, F32)
    grad_queries = []
    for at in range(0, q_ref.shape[0], step):
        rows = slice(at, at + step)
        probs = weights_of(queries[rows], keys, dr_ref[rows, :], dk_ref[...], scale)
        grad_rows = go_ref[rows, :]
        grad_weights = dot_nt(grad_rows, values)
        delta = jnp.sum(grad_weights * probs, axis=-1, keepdims=True)
        grad_scores = (probs * (grad_weights - delta)).astype(BF16)
        grad_queries.append(dot_nn(grad_scores, keys))
        grad_keys = grad_keys + dot_tn(grad_scores, queries[rows])
        grad_values = grad_values + dot_tn(probs.astype(BF16), grad_rows)

    @pl.when(pl.program_id(0) == 0)
    def _():
        gqg_ref[...] = jnp.zeros_like(gqg_ref)
        gkg_ref[...] = jnp.zeros_like(gkg_ref)

    def finish(grad, normed, inverse, gain_ref, out_ref, gain_grad_ref):
        grad = turn_back(grad * scale, cosine, sine)
        gain_grad_ref[...] += jnp.sum(grad * normed, axis=0, keepdims=True)
        lifted = grad * gain_ref[...]
        inner = jnp.mean(lifted * normed, axis=-1, keepdims=True)
        out_ref[...] = ((lifted - normed * inner) * inverse).astype(BF16)

    finish(jnp.concatenate(grad_queries, axis=0), q_normed, q_inverse, qg_ref, gq_ref, gqg_ref)
    finish(grad_keys, k_normed, k_inverse, kg_ref, gk_ref, gkg_ref)
    gv_ref[...] = grad_values.astype(BF16)


def attention_call(kernel, heads, head_dim, seq_len, values, tables, outs, flops):
    column = pl.BlockSpec((seq_len, head_dim), lambda head: (0, head))
    whole = [pl.BlockSpec(t.shape, lambda head: (0, 0)) for t in tables]
    shapes = [
        jax.ShapeDtypeStruct((seq_len, heads * head_dim), BF16) if wide
        else jax.ShapeDtypeStruct((1, head_dim), F32)
        for wide in outs
    ]
    specs = [column if wide else pl.BlockSpec((1, head_dim), lambda head: (0, 0)) for wide in outs]
    return pl.pallas_call(
        functools.partial(kernel, min(512, seq_len)),
        grid=(heads,),
        out_shape=shapes,
        in_specs=[column] * len(values) + whole,
        out_specs=specs,
        compiler_params=pltpu.CompilerParams(vmem_limit_bytes=VMEM_BYTES),
        cost_estimate=pl.CostEstimate(
            flops=flops, bytes_accessed=16 * seq_len * heads * head_dim, transcendentals=heads * seq_len**2
        ),
        name="attention",
    )(*values, *tables)


def params(flops, moved):
    return dict(compiler_params=pltpu.CompilerParams(vmem_limit_bytes=VMEM_BYTES),
        cost_estimate=pl.CostEstimate(flops=flops, bytes_accessed=moved, transcendentals=0))


def pick_rows_of(pick, value, out_ref, index):
    local, _, capacity, _ = out_ref.shape
    rows = dot_nn(pick, value).astype(BF16)
    for expert_at in range(local):
        out_ref[expert_at, index] = rows[expert_at * capacity : (expert_at + 1) * capacity]


def dispatch_kernel(pick_ref, value_ref, out_ref):
    for index in range(pick_ref.shape[0]):
        pick_rows_of(pick_ref[index], value_ref[index], out_ref, index)


def route_kernel(pick_ref, value_ref, mask_ref, router_ref, select_ref, out_ref, prob_ref):
    local, _, capacity, _ = out_ref.shape
    for index in range(pick_ref.shape[0]):
        pick, value, mask = pick_ref[index], value_ref[index], mask_ref[index] > 0
        pick_rows_of(pick, value, out_ref, index)
        kept = jnp.where(mask, dot_nn(value, router_ref[...]), MASKED)
        lifted = jnp.exp(kept - jnp.max(kept, axis=-1, keepdims=True))
        lifted = jnp.where(mask, lifted, 0.0)
        rest = lifted / jnp.sum(lifted, axis=-1, keepdims=True)
        picked = jnp.zeros((pick.shape[0], rest.shape[1]), F32)
        for _ in range(3):
            piece = rest.astype(BF16)
            rest = rest - piece.astype(F32)
            picked = picked + dot_nn(pick, piece)
        prob = jnp.sum(picked * select_ref[...], axis=-1, keepdims=True)
        for expert_at in range(local):
            prob_ref[expert_at, index] = prob[expert_at * capacity : (expert_at + 1) * capacity]


def dispatch(pick, value, local, routing=None, group=2):
    blocks, picked, rows = pick.shape
    width = value.shape[-1]
    capacity = picked // local

    def block(*shape):
        return pl.BlockSpec((group,) + shape, lambda b: (b, 0, 0))

    def result(columns):
        return pl.BlockSpec((local, group, capacity, columns), lambda b: (0, b, 0, 0))

    def shape(columns, kind):
        return jax.ShapeDtypeStruct((local, blocks, capacity, columns), kind)

    ins, specs = [pick, value], [block(picked, rows), block(rows, width)]
    shapes, outs = [shape(width, BF16)], [result(width)]
    if routing is not None:
        mask, router, select = routing
        ins += [mask, router, select]
        specs += [block(rows, mask.shape[-1])]
        specs += [pl.BlockSpec(t.shape, lambda b: (0, 0)) for t in (router, select)]
        shapes += [shape(1, F32)]
        outs += [result(1)]
    return pl.pallas_call(
        dispatch_kernel if routing is None else route_kernel,
        grid=(blocks // group,),
        out_shape=shapes,
        in_specs=specs,
        out_specs=outs,
        name="dispatch",
        **params(2 * blocks * picked * rows * width, 2 * blocks * width * (picked + rows)),
    )(*ins)


def combine_kernel(pick_ref, value_ref, *refs):
    local, group, capacity, width = value_ref.shape
    out_ref = refs[-2] if len(refs) == 3 else refs[0]
    for index in range(group):
        pick = pick_ref[index]
        if group == 1:
            value = value_ref[...].reshape(local * capacity, width)
        else:
            value = jnp.concatenate([value_ref[e, index] for e in range(local)], axis=0)
        out_ref[index] = dot_tn(pick, value).astype(BF16)
        if len(refs) == 3:
            for e in range(local):
                part = pick[e * capacity : (e + 1) * capacity].astype(F32)
                refs[2][index, e : e + 1, :] = jnp.sum(
                    part * refs[0][e, index], axis=0, keepdims=True
                )


def combine(pick, value, dots=None, group=2):
    blocks, picked, rows = pick.shape
    local, _, capacity, width = value.shape

    def rows_of(columns):
        return pl.BlockSpec((local, group, capacity, columns), lambda b: (0, b, 0, 0))

    ins, specs = [pick, value], [pl.BlockSpec((group, picked, rows), lambda b: (b, 0, 0)), rows_of(width)]
    shapes = [jax.ShapeDtypeStruct((blocks, rows, width), BF16)]
    outs = [pl.BlockSpec((group, rows, width), lambda b: (b, 0, 0))]
    if dots is not None:
        ins += [dots]
        specs += [rows_of(1)]
        shapes += [jax.ShapeDtypeStruct((blocks, local, rows), F32)]
        outs += [pl.BlockSpec((group, local, rows), lambda b: (b, 0, 0))]
    return pl.pallas_call(
        combine_kernel,
        grid=(blocks // group,),
        out_shape=shapes,
        in_specs=specs,
        out_specs=outs,
        name="combine",
        **params(2 * blocks * picked * rows * width, 2 * blocks * width * (picked + rows)),
    )(*ins)


def down_kernel(h0_ref, h1_ref, w0_ref, w1_ref, out_ref):
    out_ref[0] = (dot_nn(h0_ref[0], w0_ref[0]) + dot_nn(h1_ref[0], w1_ref[0])).astype(BF16)


def down_rows(h0, h1, w0, w1, step):
    local, count, hidden = h0.shape
    width = w0.shape[-1]
    rows = pl.BlockSpec((1, step, hidden), lambda e, i: (e, i, 0))
    weight = pl.BlockSpec((1, hidden, width), lambda e, i: (e, 0, 0))
    return pl.pallas_call(
        down_kernel,
        grid=(local, count // step),
        out_shape=jax.ShapeDtypeStruct((local, count, width), BF16),
        in_specs=[rows, rows, weight, weight],
        out_specs=pl.BlockSpec((1, step, width), lambda e, i: (e, i, 0)),
        name="down_rows",
        **params(4 * local * count * hidden * width, 2 * local * (count + 2 * hidden) * width),
    )(h0, h1, w0, w1)


def expert_kernel(x_ref, w0_ref, w1_ref, u0_ref, u1_ref, pr_ref, gx_ref, dots_ref, *outs):
    x = x_ref[0]
    prob = pr_ref[0]
    total = None
    dots = None
    for w_ref, u_ref, hp_ref, ggu_ref in ((w0_ref, u0_ref, outs[0], outs[2]), (w1_ref, u1_ref, outs[1], outs[3])):
        n = u_ref.shape[-1]
        both = dot_nn(x, w_ref[0])
        gate, up = both[:, :n], both[:, n:]
        sigma = jax.nn.sigmoid(gate)
        silu = gate * sigma
        hidden = (silu * up).astype(BF16).astype(F32)
        back = u_ref[0]
        part = jnp.sum(hidden * back, axis=-1, keepdims=True)
        dots = part if dots is None else dots + part
        hp_ref[0] = (hidden * prob).astype(BF16)
        gh = back * prob
        ggu_ref[0, :, :n] = (gh * up * (sigma + silu * (1.0 - sigma))).astype(BF16)
        ggu_ref[0, :, n:] = (gh * silu).astype(BF16)
        part = dot_nt(ggu_ref[0], w_ref[0])
        total = part if total is None else total + part
    gx_ref[0] = total.astype(BF16)
    dots_ref[0] = dots


def expert(x, w0, w1, u0, u1, prob, step):
    local, count, width = x.shape
    n = u0.shape[-1]
    r = lambda c: pl.BlockSpec((1, step, c), lambda e, i: (e, i, 0))
    w = pl.BlockSpec((1, width, 2*n), lambda e, i: (e, 0, 0))
    s = lambda c, t: jax.ShapeDtypeStruct((local, count, c), t)
    return pl.pallas_call(
        expert_kernel, grid=(local, count//step),
        out_shape=[s(width,BF16), s(1,F32), s(n,BF16), s(n,BF16), s(2*n,BF16), s(2*n,BF16)],
        in_specs=[r(width), w, w, r(n), r(n), r(1)],
        out_specs=[r(width), r(1), r(n), r(n), r(2*n), r(2*n)],
        name="expert", **params(16*local*count*width*n, local*(count*(width*4+n*20)+8*width*n)),
    )(x, w0, w1, u0, u1, prob)


def norm_rows(value, gain):
    inverse = lax.rsqrt(jnp.mean(value * value, axis=-1, keepdims=True) + EPS_NORM)
    return value * inverse * gain


def norm_back(value, gain, grad):
    inverse = lax.rsqrt(jnp.mean(value * value, axis=-1, keepdims=True) + EPS_NORM)
    normed = value * inverse
    lifted = grad * gain
    inner = jnp.mean(lifted * normed, axis=-1, keepdims=True)
    return (lifted - normed * inner) * inverse, jnp.sum(grad * normed, axis=0)


def positions(lengths, seq_len):
    ends = jnp.cumsum(lengths)
    starts = ends - lengths
    index = jnp.arange(seq_len, dtype=jnp.int32)
    doc_ids = jnp.sum((index[:, None] >= ends[None, :]).astype(jnp.int32), axis=1)
    member = doc_ids[:, None] == jnp.arange(lengths.shape[0], dtype=jnp.int32)[None, :]
    offset = jnp.sum(jnp.where(member, starts[None, :], 0), axis=1)
    return (doc_ids, index - offset)


def rope_tables(position, head_dim):
    half = head_dim // 2
    freq = ROPE_BASE ** (-(2.0 * jnp.arange(half, dtype=F32)) / head_dim)
    angle = position.astype(F32)[:, None] * freq[None, :]
    return (jnp.cos(angle), jnp.sin(angle))


def einsum(spec, left, right):
    return jnp.einsum(spec, left, right, preferred_element_type=F32)


def swap_cores(value):
    return lax.ppermute(value, "core", [(0, 1), (1, 0)])


def gather(value, axes):
    return lax.all_gather(value, axes, axis=0, tiled=True)


def scatter(value, axes, dim=0):
    return lax.psum_scatter(value, axes, scatter_dimension=dim, tiled=True)


def masked_softmax(logits, mask):
    kept = jnp.where(mask, logits, MASKED)
    lifted = jnp.where(mask, jnp.exp(kept - jnp.max(kept, axis=-1, keepdims=True)), 0.0)
    return lifted / jnp.sum(lifted, axis=-1, keepdims=True)


def route_mask(routes, experts_all):
    ids = jnp.arange(experts_all, dtype=jnp.int32)
    return jnp.any(routes[:, :, None] == ids[None, None, :], axis=1)


def per_device(
    layer_input,
    routes,
    doc_lengths,
    norm1_gain,
    w_qkv,
    q_gain,
    k_gain,
    w_out,
    norm2_gain,
    w_router,
    expert_gate_up,
    expert_down,
    d_out,
):
    rows, width = layer_input.shape
    x_count = lax.axis_size("x")
    ep_count = lax.axis_size("ep")
    seq_len = rows * x_count * 2
    blocks = ep_count * x_count
    topk = routes.shape[1]
    experts_all = w_router.shape[1]
    local = expert_gate_up.shape[0]
    hidden_local = expert_down.shape[1]
    head_dim = q_gain.shape[0]
    qkv_local = w_qkv.shape[2]
    heads = qkv_local // head_dim
    capacity = min(3 * rows * topk // (2 * experts_all), rows)
    my_ep = lax.axis_index("ep")

    gain_one = norm1_gain.astype(F32)
    gain_two = norm2_gain.astype(F32)
    inputs = layer_input.astype(F32)
    grad_out = d_out.astype(F32)
    input_seq = gather(layer_input, GROUP)
    g_flat = gather(d_out, PLANE)
    h_seq = norm_rows(input_seq.astype(F32), gain_one).astype(BF16)
    w_parts = w_qkv.transpose(1, 0, 2)
    raw = [jnp.dot(h_seq, w_parts[part], preferred_element_type=F32) for part in range(3)]
    doc_ids, position = positions(doc_lengths[0], seq_len)
    cosine, sine = rope_tables(position, head_dim)
    tables = (
        q_gain.astype(F32)[None],
        k_gain.astype(F32)[None],
        jnp.concatenate([cosine, cosine], axis=1),
        jnp.concatenate([-sine, sine], axis=1),
        doc_ids[:, None],
        doc_ids[None, :],
    )
    (attn_vals,) = attention_call(
        attend_kernel, heads, head_dim, seq_len, raw, tables, (True,), 4 * seq_len**2 * qkv_local
    )
    attn_part = jnp.dot(attn_vals, w_out, preferred_element_type=F32).astype(BF16)
    attn_out = group_reduce(attn_part, 7)
    middle = inputs + attn_out
    h_two = norm_rows(middle, gain_two).astype(BF16)

    g_plane = g_flat.reshape(blocks, rows, width)
    routes_plane = spread(routes.T, PLANE, 1).transpose(0, 2, 1).reshape(blocks * rows, topk)
    h_flat = gather(h_two, PLANE)
    pair_other = swap_cores(expert_gate_up.reshape(local, width, 2 * hidden_local))
    down_other = swap_cores(expert_down)
    pair_own = expert_gate_up.reshape(local, width, 2 * hidden_local)

    mask_plane = route_mask(routes_plane, experts_all)
    first = my_ep * local
    mask_here = lax.dynamic_slice_in_dim(mask_plane, first, local, axis=1)
    mask_here = mask_here.reshape(blocks, rows, local).transpose(0, 2, 1)
    before = jnp.triu(jnp.ones((rows, rows), BF16), 1)
    rank = einsum("bet,tu->beu", mask_here.astype(BF16), before).astype(jnp.int32)
    slots = jnp.arange(capacity, dtype=jnp.int32)[None, None, :, None]
    picks = mask_here[:, :, None, :] & (rank[:, :, None, :] == slots)
    pick = picks.astype(BF16)
    pick_rows = pick.reshape(blocks, local * capacity, rows)
    count = blocks * capacity

    (g_rows,) = dispatch(pick_rows, g_plane, local, group=4)
    g_rows = g_rows.reshape(local, count, width)
    back_own = einsum("emd,efd->emf", g_rows, expert_down)
    back_other = einsum("emd,efd->emf", g_rows, down_other)
    h_flat, back_own, back_other = lax.optimization_barrier((h_flat, back_own, back_other))
    select_column = first + jnp.arange(local * capacity, dtype=jnp.int32) // capacity
    select = select_column[:, None] == jnp.arange(experts_all, dtype=jnp.int32)[None, :]
    routing = (
        mask_plane.astype(F32).reshape(blocks, rows, experts_all),
        w_router,
        select.astype(F32),
    )
    h_rows, prob_rows = dispatch(
        pick_rows, h_flat.reshape(blocks, rows, width), local, routing, group=2
    )
    h_rows = h_rows.reshape(local, count, width)
    prob_rows = prob_rows.reshape(local, count, 1)
    back_rows, dot_rows, weighted_own, weighted_other, ggu_own, ggu_other = expert(
        h_rows, pair_own, pair_other, back_own, back_other, prob_rows, min(384, count)
    )
    back_part, dots_token = combine(
        pick_rows,
        back_rows.reshape(local, blocks, capacity, width),
        dot_rows.reshape(local, blocks, capacity, 1),
        group=2,
    )
    grad_probs = spread(dots_token, PLANE, 2, True)
    grad_probs = jnp.sum(grad_probs.reshape(ep_count, x_count, local, rows), axis=1)
    grad_probs = grad_probs.reshape(experts_all, rows).T
    back_sum = plane_reduce(back_part, 3)
    out_rows = down_rows(
        weighted_own, weighted_other, expert_down, down_other, min(384, count)
    )
    (out_part,) = combine(
        pick_rows, out_rows.reshape(local, blocks, capacity, width), group=4
    )

    grad_pair_own = einsum("emd,emf->edf", h_rows, ggu_own)
    grad_pair_other = einsum("emd,emf->edf", h_rows, ggu_other)
    grad_down_own = einsum("emf,emd->efd", weighted_own, g_rows)
    grad_down_other = einsum("emf,emd->efd", weighted_other, g_rows)
    grad_pair = grad_pair_own + swap_cores(grad_pair_other.astype(BF16)).astype(F32)
    grad_down = grad_down_own + swap_cores(grad_down_other.astype(BF16)).astype(F32)
    grad_gate_up = grad_pair.reshape(local, width, 2, hidden_local)

    mask_own = route_mask(routes, experts_all)
    probs_own = masked_softmax(jnp.dot(h_two, w_router, preferred_element_type=F32), mask_own)
    inner = jnp.sum(probs_own * grad_probs, axis=-1, keepdims=True)
    grad_logits = probs_own * (grad_probs - inner)
    grad_router = lax.dot_general(
        grad_logits, h_two.astype(F32), (((0,), (0,)), ((), ())), precision=HIGH
    )
    grad_h_two = back_sum + jnp.dot(
        grad_logits, w_router.astype(F32).T, precision=HIGH
    )
    grad_mid_norm, grad_gain_two = norm_back(middle, gain_two, grad_h_two)
    grad_mid = grad_out + grad_mid_norm

    ga_seq = gather(grad_mid.astype(BF16), GROUP)
    ga_seq, out_part = lax.optimization_barrier((ga_seq, out_part))
    grad_wout = lax.dot_general(
        attn_vals, ga_seq, (((0,), (0,)), ((), ())), preferred_element_type=F32
    )
    grad_vals = lax.dot_general(
        ga_seq, w_out, (((1,), (1,)), ((), ())), preferred_element_type=F32
    )
    *grad_proj, grad_q_gain, grad_k_gain = attention_call(
        attend_back_kernel,
        heads,
        head_dim,
        seq_len,
        (*raw, grad_vals.astype(BF16)),
        tables,
        (True, True, True, False, False),
        10 * seq_len**2 * qkv_local,
    )
    grad_h_part = sum(
        lax.dot_general(grad, w, (((1,), (1,)), ((), ())), preferred_element_type=F32)
        for grad, w in zip(grad_proj, w_parts)
    )
    grad_h_one = scatter(grad_h_part.astype(BF16), GROUP).astype(F32)
    grad_wqkv = jnp.stack(
        [
            lax.dot_general(
                h_seq, grad, (((0,), (0,)), ((), ())), preferred_element_type=F32
            ).astype(BF16)
            for grad in grad_proj
        ],
    )
    grad_in_norm, grad_gain_one = norm_back(inputs, gain_one, grad_h_one)
    grad_input = grad_mid + grad_in_norm
    dense_qkv = scatter(grad_wqkv, "ep", 1).astype(F32)
    dense_out = scatter(grad_wout.astype(BF16), "ep", 1).astype(F32)
    devices = blocks * 2
    small = jnp.concatenate(
        [grad_router.reshape(-1), grad_gain_one, grad_gain_two, grad_q_gain[0], grad_k_gain[0]]
    )
    length = small.shape[0]
    padded = -(-length // (devices * 1024)) * devices * 1024
    small = jnp.pad(small, (0, padded - length)).reshape(devices, -1, 128)
    small = jnp.sum(spread(small, ALL, 5, True), axis=0)
    small = spread(small, ALL, 6).reshape(-1)
    out_part, small = lax.optimization_barrier((out_part, small))
    output = (middle + plane_reduce(out_part, 4)).astype(BF16)
    cuts = (experts_all * width, width, width, head_dim, head_dim)
    starts = [sum(cuts[:index]) for index in range(5)]
    router_sum, *gains = (small[at : at + cut] for at, cut in zip(starts, cuts))
    grad_router = router_sum.reshape(experts_all, width).T
    return (
        output,
        grad_input,
        gains[0],
        dense_qkv.transpose(1, 0, 2),
        gains[2],
        gains[3],
        dense_out,
        gains[1],
        grad_router,
        grad_gate_up,
        grad_down,
    )


def solution(mesh):
    ep_count, tp_count = mesh.shape["ep"], mesh.shape["tp"]
    fine = Mesh(mesh.devices.reshape(ep_count, tp_count // 2, 2), ALL)
    in_specs = (
        P(ALL, None),
        P(ALL, None),
        P("ep", None),
        P(),
        P(None, None, GROUP),
        P(),
        P(),
        P(GROUP, None),
        P(),
        P(),
        P("ep", None, None, GROUP),
        P("ep", GROUP, None),
        P(ALL, None),
    )
    out_specs = (
        P(ALL, None),
        P(ALL, None),
        P(),
        P("ep", None, GROUP),
        P(),
        P(),
        P(GROUP, "ep"),
        P(),
        P(),
        P("ep", None, None, GROUP),
        P("ep", GROUP, None),
    )

    return jax.shard_map(
        per_device, mesh=fine, in_specs=in_specs, out_specs=out_specs, check_vma=False
    )
```

```python
import functools
import math

import jax
import jax.numpy as jnp
from jax import lax
from jax.experimental import pallas as pl
from jax.experimental.pallas import tpu as pltpu
from jax.sharding import Mesh
from jax.sharding import PartitionSpec as P


HIGH = lax.Precision.HIGHEST
EPS_NORM = 1e-05
EPS_HEAD = 1e-06
ROPE_BASE = 10000.0
MASKED = -1e30
F32 = jnp.float32
BF16 = jnp.bfloat16
PLANE = ("ep", "x")
GROUP = ("x", "core")
ALL = ("ep", "x", "core")

MESH = pl.DeviceIdType.MESH
VMEM_BYTES = 60 * 1024 * 1024


def remote(source, target, send, recv, where):
    return pltpu.make_async_remote_copy(
        src_ref=source,
        dst_ref=target,
        send_sem=send,
        recv_sem=recv,
        device_id=where,
        device_id_type=MESH,
    )


def greet(where):
    pl.semaphore_signal(
        pltpu.get_barrier_semaphore(), inc=1, device_id=where, device_id_type=MESH
    )


def add_into(target, terms, step=32):
    def body(index, carry):
        at = pl.ds(pl.multiple_of(index * step, step), step)
        total = terms[0][at, :].astype(F32)
        for term in terms[1:]:
            total = total + term[at, :].astype(F32)
        target[at, :] = total.astype(target.dtype)
        return carry

    lax.fori_loop(0, target.shape[0] // step, body, 0)


def peer_of(axes, counts, index):
    where = {}
    for axis, count in reversed(list(zip(axes, counts))):
        where[axis] = lax.rem(index, count)
        index = index // count
    return where


def spread_kernel(axes, counts, own_slices, v_ref, out_ref, local_sem, send, recv):
    total = math.prod(counts)
    me = 0
    for axis, count in zip(axes, counts):
        me = me * count + lax.axis_index(axis)

    def hello(step, carry):
        greet(peer_of(axes, counts, lax.rem(me + step, total)))
        return carry

    lax.fori_loop(1, total, hello, 0)
    pl.semaphore_wait(pltpu.get_barrier_semaphore(), total - 1)

    def copy(step):
        peer = lax.rem(me + step, total)
        source = v_ref.at[peer] if own_slices else v_ref
        return remote(
            source, out_ref.at[me], send.at[step], recv.at[step], peer_of(axes, counts, peer)
        )

    mine = pltpu.make_async_copy(
        v_ref.at[me] if own_slices else v_ref, out_ref.at[me], local_sem
    )
    mine.start()

    def begin(step, carry):
        copy(step).start()
        return carry

    def finish(step, carry):
        copy(step).wait()
        return carry

    lax.fori_loop(1, total, begin, 0)
    mine.wait()
    lax.fori_loop(1, total, finish, 0)


def spread(value, axes, collective_id, own_slices=False):
    counts = tuple(lax.axis_size(axis) for axis in axes)
    total = math.prod(counts)
    shape = value.shape[1:] if own_slices else value.shape
    return pl.pallas_call(
        functools.partial(spread_kernel, axes, counts, own_slices),
        out_shape=jax.ShapeDtypeStruct((total,) + shape, value.dtype),
        in_specs=[pl.BlockSpec(memory_space=pltpu.VMEM)],
        out_specs=pl.BlockSpec(memory_space=pltpu.VMEM),
        scratch_shapes=[
            pltpu.SemaphoreType.DMA,
            pltpu.SemaphoreType.DMA((total,)),
            pltpu.SemaphoreType.DMA((total,)),
        ],
        compiler_params=pltpu.CompilerParams(
            collective_id=collective_id, has_side_effects=True
        ),
        name="spread",
    )(value)


def visiting_order(count):
    order, low, high = [], 0, count - 1
    while low <= high:
        order.append(high)
        high -= 1
        if low <= high:
            order.append(low)
            low += 1
    return order


def fill_job(big_hbm, small_hbm, own_hbm, other_hbm, big_is_left, big, small, wide, narrow, sems):
    tile = big.shape[-1]
    columns = small_hbm[0].shape[-1]
    tiles = big_hbm.shape[-1] // tile
    small_at = pl.ds(0, columns)

    def loads(unit, slot):
        expert_at, tile_at = unit // tiles, lax.rem(unit, tiles)
        cut = pl.ds(pl.multiple_of(tile_at * tile, tile), tile)
        yield pltpu.make_async_copy(big_hbm.at[expert_at, :, cut], big.at[slot], sems.at[slot, 0])
        for side in (0, 1):
            yield pltpu.make_async_copy(
                small_hbm[side].at[expert_at],
                small.at[slot, side, :, small_at],
                sems.at[slot, 1 + side],
            )

    def stores(unit):
        expert_at, tile_at = unit // tiles, lax.rem(unit, tiles)
        cut = pl.ds(pl.multiple_of(tile_at * tile, tile), tile)
        for side, (stage, target) in enumerate(((wide, own_hbm), (narrow, other_hbm))):
            if big_is_left:
                source, where = stage.at[:, small_at], target.at[expert_at, cut, :]
            else:
                source, where = stage.at[small_at, :], target.at[expert_at, :, cut]
            yield pltpu.make_async_copy(source, where, sems.at[2, side])

    def run(start, count):
        for copy in loads(start, 0):
            copy.start()

        def body(index, carry):
            slot = lax.rem(index, 2)

            @pl.when(index + 1 < count)
            def _():
                for copy in loads(start + index + 1, 1 - slot):
                    copy.start()

            for copy in loads(start + index, slot):
                copy.wait()
            sums = []
            for side in (0, 1):
                left, right = big[slot], small[slot, side, :, small_at]
                sums.append(dot_tn(left, right) if big_is_left else dot_tn(right, left))

            @pl.when(index > 0)
            def _():
                for copy in stores(start + index - 1):
                    copy.wait()

            for stage, total in zip((wide, narrow), sums):
                if big_is_left:
                    stage[:, small_at] = total.astype(stage.dtype)
                else:
                    stage[small_at, :] = total.astype(stage.dtype)
            for copy in stores(start + index):
                copy.start()
            return carry

        lax.fori_loop(0, count, body, 0)
        for copy in stores(start + count - 1):
            copy.wait()

    return run, tiles


def reduce_kernel(depth, half, filled, *refs):
    refs = list(refs)

    def take(count):
        taken = refs[:count]
        del refs[:count]
        return taken

    pick_ref, rows_ref = take(2)
    factors = take(6) if filled else ()
    (out_ref,) = take(1)
    grads = take(4) if filled else ()
    part, value, pick, one, two, right, left = take(7)
    load_sem, s1, r1, s2, r2, sr, rr, sl, rl = take(9)
    ep = lax.axis_index("ep")
    x = lax.axis_index("x")
    z = ep // 2
    y = lax.rem(ep, 2)
    first = ({"x": 1 - x}, {"ep": z * 2 + 1 - y})
    second = (first[1], first[0])
    up, down = {"ep": ep + 2}, {"ep": ep - 2}
    barrier = pltpu.get_barrier_semaphore()
    greet(first[0])
    greet(first[1])
    pl.when(z < depth - 1)(lambda: greet(up))
    pl.when(z > 0)(lambda: greet(down))
    peers = 2 + (z > 0).astype(jnp.int32) + (z < depth - 1).astype(jnp.int32)
    pl.semaphore_wait(barrier, peers)

    local, _, capacity, _ = rows_ref.shape
    total = 4 * depth

    def level_of(turn):
        return jnp.where(lax.rem(turn, 2) == 0, depth - 1 - turn // 2, turn // 2)

    def place(number):
        later = number - depth
        level = jnp.where(later < 0, level_of(number), level_of(later // 3))
        kind = jnp.where(later < 0, 0, 1 + lax.rem(later, 3))
        return level, kind

    def fetch(number, slot):
        level, kind = place(number)
        near_y = jnp.where(lax.rem(kind, 2) == 1, y, 1 - y)
        near_x = jnp.where(kind >= 2, x, 1 - x)
        block = (level * 2 + near_y) * 2 + near_x
        yield pltpu.make_async_copy(rows_ref.at[:, block], value.at[slot], load_sem.at[slot, 0])
        yield pltpu.make_async_copy(pick_ref.at[block], pick.at[slot], load_sem.at[slot, 1])

    def compute(number):
        slot = lax.rem(number, 2)

        @pl.when(number + 1 < total)
        def _():
            for copy in fetch(number + 1, 1 - slot):
                copy.start()

        for copy in fetch(number, slot):
            copy.wait()
        level, kind = place(number)
        for side in (0, 1):
            picked = value[slot, :, :, side * half : (side + 1) * half]
            picked = picked.reshape(local * capacity, half)
            part[level, kind, side] = dot_tn(pick[slot], picked).astype(BF16)

    def send_one(side, level, step):
        return remote(
            part.at[level, 0 if step == 0 else 1 + side, side],
            one.at[side, level, step],
            s1.at[side, level, step],
            r1.at[side, level, step],
            first[side],
        )

    def send_two(side, level):
        return remote(
            one.at[side, level, 0],
            two.at[side, level],
            s2.at[side, level],
            r2.at[side, level],
            second[side],
        )

    def go_right(side, level):
        ref = right.at[side, level]
        return remote(ref, ref, sr.at[side, level], rr.at[side, level], up)

    def go_left(side, level):
        ref = left.at[side, level]
        return remote(ref, ref, sl.at[side, level], rl.at[side, level], down)

    fills = []
    if filled:
        hidden, gates, outs = factors[:3], factors[3:], grads
        scratch = take(5)
        fills.append(fill_job(gates[0], gates[1:], outs[0], outs[1], True, *scratch))
        fills.append(fill_job(hidden[0], hidden[1:], outs[2], outs[3], False, *scratch))

    for copy in fetch(0, 0):
        copy.start()

    def open_turn(turn, carry):
        compute(turn)
        level = level_of(turn)
        for side in (0, 1):
            send_one(side, level, 0).start()
        return carry

    lax.fori_loop(0, depth, open_turn, 0)

    def turn_one(turn, carry):
        lax.fori_loop(0, 3, lambda k, c: (compute(depth + turn * 3 + k), c)[1], 0)
        level = level_of(turn)
        for side in (0, 1):
            send_one(side, level, 0).wait()
            arrived = one.at[side, level, 0]
            add_into(arrived, [arrived, part.at[level, 2 - side, side]])
            send_two(side, level).start()
            send_one(side, level, 1).start()
        for run, tiles in fills:
            share = local * tiles // depth
            run(turn * share, share)
        return carry

    lax.fori_loop(0, depth, turn_one, 0)

    def begin(level):
        for side in (0, 1):
            if level > 0:

                @pl.when(z == 0)
                def _():
                    add_into(right.at[side, level], [two.at[side, level]])
                    go_right(side, level).start()

            if level < depth - 1:

                @pl.when(z == depth - 1)
                def _():
                    add_into(left.at[side, level], [two.at[side, level]])
                    go_left(side, level).start()

    def forward(level):
        for side in (0, 1):

            @pl.when((z > 0) & (z < level))
            def _():
                go_right(side, level).wait_recv()
                ref = right.at[side, level]
                add_into(ref, [ref, two.at[side, level]])
                go_right(side, level).start()

            @pl.when((z < depth - 1) & (z > level))
            def _():
                go_left(side, level).wait_recv()
                ref = left.at[side, level]
                add_into(ref, [ref, two.at[side, level]])
                go_left(side, level).start()

    order = visiting_order(depth)
    for turn, level in enumerate(order):
        for side in (0, 1):
            send_one(side, level, 1).wait()
            kept = part.at[level, 3, side]
            add_into(kept, [one.at[side, level, 1], kept])
            send_two(side, level).wait()
            add_into(two.at[side, level], [two.at[side, level], kept])
        begin(level)
        if turn > 0:
            forward(order[turn - 1])
    forward(order[-1])
    for level in range(depth):

        @pl.when(z == level)
        def _():
            for side in (0, 1):
                terms = [two.at[side, level]]
                if level > 0:
                    go_right(side, level).wait_recv()
                    terms.append(right.at[side, level])
                if level < depth - 1:
                    go_left(side, level).wait_recv()
                    terms.append(left.at[side, level])
                add_into(out_ref.at[:, pl.ds(side * half, half)], terms)

        for side in (0, 1):
            pl.when(z < level)(lambda: go_right(side, level).wait_send())
            pl.when(z > level)(lambda: go_left(side, level).wait_send())


def plane_reduce(pick, values, collective_id, factors=()):
    local, blocks, capacity, columns = values.shape
    rows = pick.shape[-1]
    ep_count, x_count = lax.axis_size("ep"), lax.axis_size("x")
    if x_count != 2 or ep_count % 2 or blocks * rows * columns > 2**23 or local * 4 % ep_count:
        (flat,) = combine(pick, values, group=4)
        flat = flat.reshape(blocks * rows, columns)
        total = lax.psum_scatter(flat, PLANE, scatter_dimension=0, tiled=True).astype(F32)
        if not factors:
            return total
        g_rows, h0, h1, h_rows, g0, g1 = factors
        return (
            total,
            einsum("emd,emf->edf", h_rows, g0),
            einsum("emd,emf->edf", h_rows, g1).astype(BF16),
            einsum("emf,emd->efd", h0, g_rows),
            einsum("emf,emd->efd", h1, g_rows).astype(BF16),
        )
    depth, half = ep_count // 2, columns // 2

    def buffer(*lead):
        return pltpu.VMEM(lead + (rows, half), BF16)

    def sems(*lead):
        return pltpu.SemaphoreType.DMA(lead)

    shapes = [jax.ShapeDtypeStruct((rows, columns), F32)]
    scratch = [
        buffer(depth, 4, 2),
        pltpu.VMEM((2, local, capacity, columns), BF16),
        pltpu.VMEM((2, local * capacity, rows), BF16),
        buffer(2, depth, 2), buffer(2, depth), buffer(2, depth), buffer(2, depth),
        sems(2, 2), sems(2, depth, 2), sems(2, depth, 2),
        sems(2, depth), sems(2, depth), sems(2, depth),
        sems(2, depth), sems(2, depth), sems(2, depth),
    ]
    if factors:
        count, hidden, gates = factors[0].shape[1], factors[1].shape[2], factors[4].shape[2]
        shapes += [
            jax.ShapeDtypeStruct((local, columns, gates), F32),
            jax.ShapeDtypeStruct((local, columns, gates), BF16),
            jax.ShapeDtypeStruct((local, hidden, columns), F32),
            jax.ShapeDtypeStruct((local, hidden, columns), BF16),
        ]
        scratch += [
            pltpu.VMEM((2, count, gates), BF16),
            pltpu.VMEM((2, 2, count, gates), BF16),
            pltpu.VMEM((gates, gates), F32),
            pltpu.VMEM((gates, gates), BF16),
            sems(3, 3),
        ]
    anywhere = pl.BlockSpec(memory_space=pl.ANY)
    results = pl.pallas_call(
        functools.partial(reduce_kernel, depth, half, bool(factors)),
        out_shape=shapes,
        in_specs=[anywhere] * (2 + len(factors)),
        out_specs=[pl.BlockSpec(memory_space=pltpu.VMEM)] + [anywhere] * (len(shapes) - 1),
        scratch_shapes=scratch,
        compiler_params=pltpu.CompilerParams(
            collective_id=collective_id, has_side_effects=True, vmem_limit_bytes=VMEM_BYTES
        ),
        name="plane_reduce",
    )(pick, values, *factors)
    return results if factors else results[0]


def group_kernel(pieces, p_ref, out_ref, near, far, kept, got, own_sem, s1, r1, s2, r2, s3, r3):
    x, core = lax.axis_index("x"), lax.axis_index("core")
    partner, across = {"core": 1 - core}, {"x": 1 - x}
    greet(partner)
    greet(across)
    pl.semaphore_wait(pltpu.get_barrier_semaphore(), 2)
    step = out_ref.shape[0] // pieces

    def at(piece):
        return pl.ds(piece * step, step)

    def hand_over(piece):
        return remote(
            p_ref.at[1 - x, 1 - core, at(piece), :],
            near.at[at(piece), :],
            s1.at[piece],
            r1.at[piece],
            partner,
        )

    def send_across(piece):
        return remote(
            far.at[at(piece), :], got.at[at(piece), :], s2.at[piece], r2.at[piece], across
        )

    stay = remote(p_ref.at[x, 1 - core], kept.at[0], s3, r3, partner)
    loads = (
        pltpu.make_async_copy(p_ref.at[1 - x, core], far, own_sem.at[0]),
        pltpu.make_async_copy(p_ref.at[x, core], kept.at[1], own_sem.at[1]),
    )
    loads[0].start()
    for piece in range(pieces):
        hand_over(piece).start()
    stay.start()
    loads[1].start()
    loads[0].wait()
    for piece in range(pieces):
        hand_over(piece).wait()
        mine = far.at[at(piece), :]
        add_into(mine, [mine, near.at[at(piece), :]])
        send_across(piece).start()
    loads[1].wait()
    stay.wait()
    for piece in range(pieces):
        send_across(piece).wait()
        rows = at(piece)
        add_into(
            out_ref.at[rows, :], [kept.at[0, rows, :], kept.at[1, rows, :], got.at[rows, :]]
        )


def group_reduce(parts, collective_id):
    if lax.axis_size("x") != 2:
        return scatter(parts, GROUP).astype(F32)
    rows, columns = parts.shape[0] // 4, parts.shape[1]
    pieces = 4

    def sems(*lead):
        return pltpu.SemaphoreType.DMA(lead)

    return pl.pallas_call(
        functools.partial(group_kernel, pieces),
        out_shape=jax.ShapeDtypeStruct((rows, columns), F32),
        in_specs=[pl.BlockSpec(memory_space=pl.ANY)],
        out_specs=pl.BlockSpec(memory_space=pltpu.VMEM),
        scratch_shapes=[
            pltpu.VMEM((rows, columns), BF16),
            pltpu.VMEM((rows, columns), BF16),
            pltpu.VMEM((2, rows, columns), BF16),
            pltpu.VMEM((rows, columns), BF16),
            sems(2),
            sems(pieces),
            sems(pieces),
            sems(pieces),
            sems(pieces),
            pltpu.SemaphoreType.DMA,
            pltpu.SemaphoreType.DMA,
        ],
        compiler_params=pltpu.CompilerParams(collective_id=collective_id, has_side_effects=True),
        name="group_reduce",
    )(parts.reshape(2, 2, rows, columns))


def turn(value, cosine, sine):
    return value * cosine + pltpu.roll(value, value.shape[-1] // 2, 1) * sine


def turn_back(value, cosine, sine):
    return value * cosine + pltpu.roll(value * sine, value.shape[-1] // 2, 1)


def head_norm(raw):
    inverse = lax.rsqrt(jnp.mean(raw * raw, axis=-1, keepdims=True) + EPS_HEAD)
    return raw * inverse, inverse


def dot_nt(left, right):
    return lax.dot_general(left, right, (((1,), (1,)), ((), ())), preferred_element_type=F32)


def dot_tn(left, right):
    return lax.dot_general(left, right, (((0,), (0,)), ((), ())), preferred_element_type=F32)


def dot_nn(left, right):
    return lax.dot_general(left, right, (((1,), (0,)), ((), ())), preferred_element_type=F32)


def weights_of(q_rows, keys, doc_rows, doc_keys, scale):
    scores = dot_nt(q_rows, keys) * scale
    scores = jnp.where(doc_rows == doc_keys, scores, MASKED)
    lifted = jnp.exp(scores - jnp.max(scores, axis=-1, keepdims=True))
    return lifted / jnp.sum(lifted, axis=-1, keepdims=True)


def attend_kernel(step, q_ref, k_ref, v_ref, qg_ref, kg_ref, cos_ref, sin_ref, dr_ref, dk_ref, o_ref):
    scale = q_ref.shape[-1] ** (-0.5)
    cosine, sine = cos_ref[...], sin_ref[...]
    queries = turn(head_norm(q_ref[...])[0] * qg_ref[...], cosine, sine).astype(BF16)
    keys = turn(head_norm(k_ref[...])[0] * kg_ref[...], cosine, sine).astype(BF16)
    values = v_ref[...].astype(BF16)
    for at in range(0, q_ref.shape[0], step):
        rows = slice(at, at + step)
        weights = weights_of(queries[rows], keys, dr_ref[rows, :], dk_ref[...], scale)
        o_ref[rows, :] = dot_nn(weights.astype(BF16), values).astype(BF16)


def attend_back_kernel(
    step, q_ref, k_ref, v_ref, go_ref, qg_ref, kg_ref, cos_ref, sin_ref, dr_ref, dk_ref,
    gq_ref, gk_ref, gv_ref, gqg_ref, gkg_ref,
):
    scale = q_ref.shape[-1] ** (-0.5)
    cosine, sine = cos_ref[...], sin_ref[...]
    q_normed, q_inverse = head_norm(q_ref[...])
    k_normed, k_inverse = head_norm(k_ref[...])
    queries = turn(q_normed * qg_ref[...], cosine, sine).astype(BF16)
    keys = turn(k_normed * kg_ref[...], cosine, sine).astype(BF16)
    values = v_ref[...].astype(BF16)
    grad_keys = jnp.zeros(k_ref.shape, F32)
    grad_values = jnp.zeros(v_ref.shape, F32)
    grad_queries = []
    for at in range(0, q_ref.shape[0], step):
        rows = slice(at, at + step)
        probs = weights_of(queries[rows], keys, dr_ref[rows, :], dk_ref[...], scale)
        grad_rows = go_ref[rows, :]
        grad_weights = dot_nt(grad_rows, values)
        delta = jnp.sum(grad_weights * probs, axis=-1, keepdims=True)
        grad_scores = (probs * (grad_weights - delta)).astype(BF16)
        grad_queries.append(dot_nn(grad_scores, keys))
        grad_keys = grad_keys + dot_tn(grad_scores, queries[rows])
        grad_values = grad_values + dot_tn(probs.astype(BF16), grad_rows)

    @pl.when(pl.program_id(0) == 0)
    def _():
        gqg_ref[...] = jnp.zeros_like(gqg_ref)
        gkg_ref[...] = jnp.zeros_like(gkg_ref)

    def finish(grad, normed, inverse, gain_ref, out_ref, gain_grad_ref):
        grad = turn_back(grad * scale, cosine, sine)
        gain_grad_ref[...] += jnp.sum(grad * normed, axis=0, keepdims=True)
        lifted = grad * gain_ref[...]
        inner = jnp.mean(lifted * normed, axis=-1, keepdims=True)
        out_ref[...] = ((lifted - normed * inner) * inverse).astype(BF16)

    finish(jnp.concatenate(grad_queries, axis=0), q_normed, q_inverse, qg_ref, gq_ref, gqg_ref)
    finish(grad_keys, k_normed, k_inverse, kg_ref, gk_ref, gkg_ref)
    gv_ref[...] = grad_values.astype(BF16)


def attention_call(kernel, heads, head_dim, seq_len, values, tables, outs, flops):
    column = pl.BlockSpec((seq_len, head_dim), lambda head: (0, head))
    whole = [pl.BlockSpec(t.shape, lambda head: (0, 0)) for t in tables]
    shapes = [
        jax.ShapeDtypeStruct((seq_len, heads * head_dim), BF16) if wide
        else jax.ShapeDtypeStruct((1, head_dim), F32)
        for wide in outs
    ]
    specs = [column if wide else pl.BlockSpec((1, head_dim), lambda head: (0, 0)) for wide in outs]
    return pl.pallas_call(
        functools.partial(kernel, min(512, seq_len)),
        grid=(heads,),
        out_shape=shapes,
        in_specs=[column] * len(values) + whole,
        out_specs=specs,
        compiler_params=pltpu.CompilerParams(vmem_limit_bytes=VMEM_BYTES),
        cost_estimate=pl.CostEstimate(
            flops=flops, bytes_accessed=16 * seq_len * heads * head_dim, transcendentals=heads * seq_len**2
        ),
        name="attention",
    )(*values, *tables)


def params(flops, moved):
    return dict(compiler_params=pltpu.CompilerParams(vmem_limit_bytes=VMEM_BYTES),
        cost_estimate=pl.CostEstimate(flops=flops, bytes_accessed=moved, transcendentals=0))


def pick_rows_of(pick, value, out_ref, index):
    local, _, capacity, _ = out_ref.shape
    rows = dot_nn(pick, value).astype(BF16)
    for expert_at in range(local):
        out_ref[expert_at, index] = rows[expert_at * capacity : (expert_at + 1) * capacity]


def dispatch_kernel(pick_ref, value_ref, out_ref):
    for index in range(pick_ref.shape[0]):
        pick_rows_of(pick_ref[index], value_ref[index], out_ref, index)


def dispatch(pick, value, local, group):
    blocks, picked, rows = pick.shape
    width = value.shape[-1]
    capacity = picked // local
    return pl.pallas_call(
        dispatch_kernel,
        grid=(blocks // group,),
        out_shape=jax.ShapeDtypeStruct((local, blocks, capacity, width), BF16),
        in_specs=[
            pl.BlockSpec((group, picked, rows), lambda b: (b, 0, 0)),
            pl.BlockSpec((group, rows, width), lambda b: (b, 0, 0)),
        ],
        out_specs=pl.BlockSpec((local, group, capacity, width), lambda b: (0, b, 0, 0)),
        name="dispatch",
        **params(2 * blocks * picked * rows * width, 2 * blocks * width * (picked + rows)),
    )(pick, value)


def combine_kernel(pick_ref, value_ref, *refs):
    local, group, capacity, width = value_ref.shape
    out_ref = refs[-2] if len(refs) == 3 else refs[0]
    for index in range(group):
        pick = pick_ref[index]
        if group == 1:
            value = value_ref[...].reshape(local * capacity, width)
        else:
            value = jnp.concatenate([value_ref[e, index] for e in range(local)], axis=0)
        out_ref[index] = dot_tn(pick, value).astype(BF16)
        if len(refs) == 3:
            for e in range(local):
                part = pick[e * capacity : (e + 1) * capacity].astype(F32)
                refs[2][index, e : e + 1, :] = jnp.sum(
                    part * refs[0][e, index], axis=0, keepdims=True
                )


def combine(pick, value, dots=None, group=2):
    blocks, picked, rows = pick.shape
    local, _, capacity, width = value.shape

    def rows_of(columns):
        return pl.BlockSpec((local, group, capacity, columns), lambda b: (0, b, 0, 0))

    ins, specs = [pick, value], [pl.BlockSpec((group, picked, rows), lambda b: (b, 0, 0)), rows_of(width)]
    shapes = [jax.ShapeDtypeStruct((blocks, rows, width), BF16)]
    outs = [pl.BlockSpec((group, rows, width), lambda b: (b, 0, 0))]
    if dots is not None:
        ins += [dots]
        specs += [rows_of(1)]
        shapes += [jax.ShapeDtypeStruct((blocks, local, rows), F32)]
        outs += [pl.BlockSpec((group, local, rows), lambda b: (b, 0, 0))]
    return pl.pallas_call(
        combine_kernel,
        grid=(blocks // group,),
        out_shape=shapes,
        in_specs=specs,
        out_specs=outs,
        name="combine",
        **params(2 * blocks * picked * rows * width, 2 * blocks * width * (picked + rows)),
    )(*ins)


def down_kernel(h0_ref, h1_ref, w0_ref, w1_ref, out_ref):
    out_ref[0] = (dot_nn(h0_ref[0], w0_ref[0]) + dot_nn(h1_ref[0], w1_ref[0])).astype(BF16)


def down_rows(h0, h1, w0, w1, step):
    local, count, hidden = h0.shape
    width = w0.shape[-1]
    rows = pl.BlockSpec((1, step, hidden), lambda e, i: (e, i, 0))
    weight = pl.BlockSpec((1, hidden, width), lambda e, i: (e, 0, 0))
    return pl.pallas_call(
        down_kernel,
        grid=(local, count // step),
        out_shape=jax.ShapeDtypeStruct((local, count, width), BF16),
        in_specs=[rows, rows, weight, weight],
        out_specs=pl.BlockSpec((1, step, width), lambda e, i: (e, i, 0)),
        name="down_rows",
        **params(4 * local * count * hidden * width, 2 * local * (count + 2 * hidden) * width),
    )(h0, h1, w0, w1)


def expert_kernel(x_ref, w0_ref, w1_ref, u0_ref, u1_ref, pr_ref, gx_ref, dots_ref, *outs):
    x = x_ref[0]
    prob = pr_ref[0]
    total = None
    dots = None
    for w_ref, u_ref, hp_ref, ggu_ref in ((w0_ref, u0_ref, outs[0], outs[2]), (w1_ref, u1_ref, outs[1], outs[3])):
        n = u_ref.shape[-1]
        both = dot_nn(x, w_ref[0])
        gate, up = both[:, :n], both[:, n:]
        sigma = jax.nn.sigmoid(gate)
        silu = gate * sigma
        hidden = (silu * up).astype(BF16).astype(F32)
        back = u_ref[0]
        part = jnp.sum(hidden * back, axis=-1, keepdims=True)
        dots = part if dots is None else dots + part
        hp_ref[0] = (hidden * prob).astype(BF16)
        gh = back * prob
        ggu_ref[0, :, :n] = (gh * up * (sigma + silu * (1.0 - sigma))).astype(BF16)
        ggu_ref[0, :, n:] = (gh * silu).astype(BF16)
        part = dot_nt(ggu_ref[0], w_ref[0])
        total = part if total is None else total + part
    gx_ref[0] = total.astype(BF16)
    dots_ref[0] = dots


def expert(x, w0, w1, u0, u1, prob, step):
    local, count, width = x.shape
    n = u0.shape[-1]
    r = lambda c: pl.BlockSpec((1, step, c), lambda e, i: (e, i, 0))
    w = pl.BlockSpec((1, width, 2*n), lambda e, i: (e, 0, 0))
    s = lambda c, t: jax.ShapeDtypeStruct((local, count, c), t)
    return pl.pallas_call(
        expert_kernel, grid=(local, count//step),
        out_shape=[s(width,BF16), s(1,F32), s(n,BF16), s(n,BF16), s(2*n,BF16), s(2*n,BF16)],
        in_specs=[r(width), w, w, r(n), r(n), r(1)],
        out_specs=[r(width), r(1), r(n), r(n), r(2*n), r(2*n)],
        name="expert", **params(16*local*count*width*n, local*(count*(width*4+n*20)+8*width*n)),
    )(x, w0, w1, u0, u1, prob)


def norm_rows(value, gain):
    inverse = lax.rsqrt(jnp.mean(value * value, axis=-1, keepdims=True) + EPS_NORM)
    return value * inverse * gain


def norm_back(value, gain, grad):
    inverse = lax.rsqrt(jnp.mean(value * value, axis=-1, keepdims=True) + EPS_NORM)
    normed = value * inverse
    lifted = grad * gain
    inner = jnp.mean(lifted * normed, axis=-1, keepdims=True)
    return (lifted - normed * inner) * inverse, jnp.sum(grad * normed, axis=0)


def positions(lengths, seq_len):
    ends = jnp.cumsum(lengths)
    starts = ends - lengths
    index = jnp.arange(seq_len, dtype=jnp.int32)
    doc_ids = jnp.sum((index[:, None] >= ends[None, :]).astype(jnp.int32), axis=1)
    member = doc_ids[:, None] == jnp.arange(lengths.shape[0], dtype=jnp.int32)[None, :]
    offset = jnp.sum(jnp.where(member, starts[None, :], 0), axis=1)
    return (doc_ids, index - offset)


def rope_tables(position, head_dim):
    half = head_dim // 2
    freq = ROPE_BASE ** (-(2.0 * jnp.arange(half, dtype=F32)) / head_dim)
    angle = position.astype(F32)[:, None] * freq[None, :]
    return (jnp.cos(angle), jnp.sin(angle))


def einsum(spec, left, right):
    return jnp.einsum(spec, left, right, preferred_element_type=F32)


def swap_cores(value):
    return lax.ppermute(value, "core", [(0, 1), (1, 0)])


def gather(value, axes):
    return lax.all_gather(value, axes, axis=0, tiled=True)


def scatter(value, axes, dim=0):
    return lax.psum_scatter(value, axes, scatter_dimension=dim, tiled=True)


def masked_softmax(logits, mask):
    kept = jnp.where(mask, logits, MASKED)
    lifted = jnp.where(mask, jnp.exp(kept - jnp.max(kept, axis=-1, keepdims=True)), 0.0)
    return lifted / jnp.sum(lifted, axis=-1, keepdims=True)


def route_mask(routes, experts_all):
    ids = jnp.arange(experts_all, dtype=jnp.int32)
    return jnp.any(routes[:, :, None] == ids[None, None, :], axis=1)


def per_device(
    layer_input,
    routes,
    doc_lengths,
    norm1_gain,
    w_qkv,
    q_gain,
    k_gain,
    w_out,
    norm2_gain,
    w_router,
    expert_gate_up,
    expert_down,
    d_out,
):
    rows, width = layer_input.shape
    x_count = lax.axis_size("x")
    ep_count = lax.axis_size("ep")
    seq_len = rows * x_count * 2
    blocks = ep_count * x_count
    topk = routes.shape[1]
    experts_all = w_router.shape[1]
    local = expert_gate_up.shape[0]
    hidden_local = expert_down.shape[1]
    head_dim = q_gain.shape[0]
    qkv_local = w_qkv.shape[2]
    heads = qkv_local // head_dim
    capacity = min(3 * rows * topk // (2 * experts_all), rows)
    my_ep = lax.axis_index("ep")

    gain_one = norm1_gain.astype(F32)
    gain_two = norm2_gain.astype(F32)
    inputs = layer_input.astype(F32)
    grad_out = d_out.astype(F32)
    input_seq = gather(layer_input, GROUP)
    g_flat = gather(d_out, PLANE)
    h_seq = norm_rows(input_seq.astype(F32), gain_one).astype(BF16)
    w_parts = w_qkv.transpose(1, 0, 2)
    raw = [jnp.dot(h_seq, w_parts[part], preferred_element_type=F32) for part in range(3)]
    doc_ids, position = positions(doc_lengths[0], seq_len)
    cosine, sine = rope_tables(position, head_dim)
    tables = (
        q_gain.astype(F32)[None],
        k_gain.astype(F32)[None],
        jnp.concatenate([cosine, cosine], axis=1),
        jnp.concatenate([-sine, sine], axis=1),
        doc_ids[:, None],
        doc_ids[None, :],
    )
    (attn_vals,) = attention_call(
        attend_kernel, heads, head_dim, seq_len, raw, tables, (True,), 4 * seq_len**2 * qkv_local
    )
    attn_part = jnp.dot(attn_vals, w_out, preferred_element_type=F32).astype(BF16)
    attn_out = group_reduce(attn_part, 7)
    middle = inputs + attn_out
    h_two = norm_rows(middle, gain_two).astype(BF16)

    g_plane = g_flat.reshape(blocks, rows, width)
    mask_own = route_mask(routes, experts_all)
    probs_own = masked_softmax(jnp.dot(h_two, w_router, preferred_element_type=F32), mask_own)
    shared = spread(jnp.where(mask_own, probs_own, -1.0).T, PLANE, 1)
    h_flat = gather(h_two, PLANE)
    pair_other = swap_cores(expert_gate_up.reshape(local, width, 2 * hidden_local))
    down_other = swap_cores(expert_down)
    pair_own = expert_gate_up.reshape(local, width, 2 * hidden_local)

    first = my_ep * local
    here = lax.dynamic_slice_in_dim(shared, first, local, axis=1)
    mask_here = here >= 0.0
    before = jnp.triu(jnp.ones((rows, rows), BF16), 1)
    rank = einsum("bet,tu->beu", mask_here.astype(BF16), before).astype(jnp.int32)
    slots = jnp.arange(capacity, dtype=jnp.int32)[None, None, :, None]
    picks = mask_here[:, :, None, :] & (rank[:, :, None, :] == slots)
    pick = picks.astype(BF16)
    pick_rows = pick.reshape(blocks, local * capacity, rows)
    count = blocks * capacity

    g_rows = dispatch(pick_rows, g_plane, local, group=4)
    g_rows = g_rows.reshape(local, count, width)
    back_own = einsum("emd,efd->emf", g_rows, expert_down)
    back_other = einsum("emd,efd->emf", g_rows, down_other)
    prob_rows = jnp.sum(jnp.where(picks, here[:, :, None, :], 0.0), axis=-1)
    prob_rows = prob_rows.transpose(1, 0, 2).reshape(local, count, 1)
    h_flat, back_own, back_other, prob_rows = lax.optimization_barrier(
        (h_flat, back_own, back_other, prob_rows)
    )
    h_rows = dispatch(pick_rows, h_flat.reshape(blocks, rows, width), local, group=4)
    h_rows = h_rows.reshape(local, count, width)
    back_rows, dot_rows, weighted_own, weighted_other, ggu_own, ggu_other = expert(
        h_rows, pair_own, pair_other, back_own, back_other, prob_rows, min(384, count)
    )
    dot_rows = dot_rows.reshape(local, blocks, capacity).transpose(1, 0, 2)
    dots_token = jnp.sum(jnp.where(picks, dot_rows[..., None], 0.0), axis=2)
    grad_probs = spread(dots_token, PLANE, 2, True)
    grad_probs = jnp.sum(grad_probs.reshape(ep_count, x_count, local, rows), axis=1)
    grad_probs = grad_probs.reshape(experts_all, rows).T
    back_sum, grad_pair_own, grad_pair_other, grad_down_own, grad_down_other = plane_reduce(
        pick_rows,
        back_rows.reshape(local, blocks, capacity, width),
        3,
        (g_rows, weighted_own, weighted_other, h_rows, ggu_own, ggu_other),
    )
    out_rows = down_rows(
        weighted_own, weighted_other, expert_down, down_other, min(384, count)
    ).reshape(local, blocks, capacity, width)

    grad_pair = grad_pair_own + swap_cores(grad_pair_other).astype(F32)
    grad_down = grad_down_own + swap_cores(grad_down_other).astype(F32)
    grad_gate_up = grad_pair.reshape(local, width, 2, hidden_local)

    inner = jnp.sum(probs_own * grad_probs, axis=-1, keepdims=True)
    grad_logits = probs_own * (grad_probs - inner)
    grad_router = lax.dot_general(
        grad_logits, h_two.astype(F32), (((0,), (0,)), ((), ())), precision=HIGH
    )
    grad_h_two = back_sum + jnp.dot(
        grad_logits, w_router.astype(F32).T, precision=HIGH
    )
    grad_mid_norm, grad_gain_two = norm_back(middle, gain_two, grad_h_two)
    grad_mid = grad_out + grad_mid_norm

    ga_seq = gather(grad_mid.astype(BF16), GROUP)
    ga_seq, out_rows = lax.optimization_barrier((ga_seq, out_rows))
    grad_wout = lax.dot_general(
        attn_vals, ga_seq, (((0,), (0,)), ((), ())), preferred_element_type=F32
    )
    grad_vals = lax.dot_general(
        ga_seq, w_out, (((1,), (1,)), ((), ())), preferred_element_type=F32
    )
    *grad_proj, grad_q_gain, grad_k_gain = attention_call(
        attend_back_kernel,
        heads,
        head_dim,
        seq_len,
        (*raw, grad_vals.astype(BF16)),
        tables,
        (True, True, True, False, False),
        10 * seq_len**2 * qkv_local,
    )
    grad_h_part = sum(
        lax.dot_general(grad, w, (((1,), (1,)), ((), ())), preferred_element_type=F32)
        for grad, w in zip(grad_proj, w_parts)
    )
    grad_h_one = scatter(grad_h_part.astype(BF16), GROUP).astype(F32)
    grad_wqkv = jnp.stack(
        [
            lax.dot_general(
                h_seq, grad, (((0,), (0,)), ((), ())), preferred_element_type=F32
            ).astype(BF16)
            for grad in grad_proj
        ],
    )
    grad_in_norm, grad_gain_one = norm_back(inputs, gain_one, grad_h_one)
    grad_input = grad_mid + grad_in_norm
    dense_qkv = scatter(grad_wqkv, "ep", 1).astype(F32)
    dense_out = scatter(grad_wout.astype(BF16), "ep", 1).astype(F32)
    devices = blocks * 2
    small = jnp.concatenate(
        [grad_router.reshape(-1), grad_gain_one, grad_gain_two, grad_q_gain[0], grad_k_gain[0]]
    )
    length = small.shape[0]
    padded = -(-length // (devices * 1024)) * devices * 1024
    small = jnp.pad(small, (0, padded - length)).reshape(devices, -1, 128)
    small = jnp.sum(spread(small, ALL, 5, True), axis=0)
    small = spread(small, ALL, 6).reshape(-1)
    out_rows, small = lax.optimization_barrier((out_rows, small))
    output = (middle + plane_reduce(pick_rows, out_rows, 4)).astype(BF16)
    cuts = (experts_all * width, width, width, head_dim, head_dim)
    starts = [sum(cuts[:index]) for index in range(5)]
    router_sum, *gains = (small[at : at + cut] for at, cut in zip(starts, cuts))
    grad_router = router_sum.reshape(experts_all, width).T
    return (
        output,
        grad_input,
        gains[0],
        dense_qkv.transpose(1, 0, 2),
        gains[2],
        gains[3],
        dense_out,
        gains[1],
        grad_router,
        grad_gate_up,
        grad_down,
    )


def solution(mesh):
    ep_count, tp_count = mesh.shape["ep"], mesh.shape["tp"]
    fine = Mesh(mesh.devices.reshape(ep_count, tp_count // 2, 2), ALL)
    in_specs = (
        P(ALL, None),
        P(ALL, None),
        P("ep", None),
        P(),
        P(None, None, GROUP),
        P(),
        P(),
        P(GROUP, None),
        P(),
        P(),
        P("ep", None, None, GROUP),
        P("ep", GROUP, None),
        P(ALL, None),
    )
    out_specs = (
        P(ALL, None),
        P(ALL, None),
        P(),
        P("ep", None, GROUP),
        P(),
        P(),
        P(GROUP, "ep"),
        P(),
        P(),
        P("ep", None, None, GROUP),
        P("ep", GROUP, None),
    )

    return jax.shard_map(
        per_device, mesh=fine, in_specs=in_specs, out_specs=out_specs, check_vma=False
    )
```

```python
import functools
import math

import jax
import jax.numpy as jnp
from jax import lax
from jax.experimental import pallas as pl
from jax.experimental.pallas import tpu as pltpu
from jax.sharding import Mesh
from jax.sharding import PartitionSpec as P


HIGH = lax.Precision.HIGHEST
EPS_NORM = 1e-05
EPS_HEAD = 1e-06
ROPE_BASE = 10000.0
MASKED = -1e30
F32 = jnp.float32
BF16 = jnp.bfloat16
PLANE = ("ep", "x")
GROUP = ("x", "core")
ALL = ("ep", "x", "core")

MESH = pl.DeviceIdType.MESH
VMEM_BYTES = 60 * 1024 * 1024


def remote(source, target, send, recv, where):
    return pltpu.make_async_remote_copy(
        src_ref=source,
        dst_ref=target,
        send_sem=send,
        recv_sem=recv,
        device_id=where,
        device_id_type=MESH,
    )


def greet(where):
    pl.semaphore_signal(
        pltpu.get_barrier_semaphore(), inc=1, device_id=where, device_id_type=MESH
    )


def add_into(target, terms, step=32):
    def body(index, carry):
        at = pl.ds(pl.multiple_of(index * step, step), step)
        total = terms[0][at, :].astype(F32)
        for term in terms[1:]:
            total = total + term[at, :].astype(F32)
        target[at, :] = total.astype(target.dtype)
        return carry

    lax.fori_loop(0, target.shape[0] // step, body, 0)


def peer_of(axes, counts, index):
    where = {}
    for axis, count in reversed(list(zip(axes, counts))):
        where[axis] = lax.rem(index, count)
        index = index // count
    return where


def spread_kernel(axes, counts, own_slices, v_ref, out_ref, local_sem, send, recv):
    total = math.prod(counts)
    me = 0
    for axis, count in zip(axes, counts):
        me = me * count + lax.axis_index(axis)

    def hello(step, carry):
        greet(peer_of(axes, counts, lax.rem(me + step, total)))
        return carry

    lax.fori_loop(1, total, hello, 0)
    pl.semaphore_wait(pltpu.get_barrier_semaphore(), total - 1)

    def copy(step):
        peer = lax.rem(me + step, total)
        source = v_ref.at[peer] if own_slices else v_ref
        return remote(
            source, out_ref.at[me], send.at[step], recv.at[step], peer_of(axes, counts, peer)
        )

    mine = pltpu.make_async_copy(
        v_ref.at[me] if own_slices else v_ref, out_ref.at[me], local_sem
    )
    mine.start()

    def begin(step, carry):
        copy(step).start()
        return carry

    def finish(step, carry):
        copy(step).wait()
        return carry

    lax.fori_loop(1, total, begin, 0)
    mine.wait()
    lax.fori_loop(1, total, finish, 0)


def spread(value, axes, collective_id, own_slices=False):
    counts = tuple(lax.axis_size(axis) for axis in axes)
    total = math.prod(counts)
    shape = value.shape[1:] if own_slices else value.shape
    return pl.pallas_call(
        functools.partial(spread_kernel, axes, counts, own_slices),
        out_shape=jax.ShapeDtypeStruct((total,) + shape, value.dtype),
        in_specs=[pl.BlockSpec(memory_space=pltpu.VMEM)],
        out_specs=pl.BlockSpec(memory_space=pltpu.VMEM),
        scratch_shapes=[
            pltpu.SemaphoreType.DMA,
            pltpu.SemaphoreType.DMA((total,)),
            pltpu.SemaphoreType.DMA((total,)),
        ],
        compiler_params=pltpu.CompilerParams(
            collective_id=collective_id, has_side_effects=True
        ),
        name="spread",
    )(value)


def visiting_order(count):
    order, low, high = [], 0, count - 1
    while low <= high:
        order.append(high)
        high -= 1
        if low <= high:
            order.append(low)
            low += 1
    return order


def fill_job(big_hbm, small_hbm, own_hbm, other_hbm, big_is_left, big, small, wide, narrow, sems):
    tile = big.shape[-1]
    columns = small_hbm[0].shape[-1]
    tiles = big_hbm.shape[-1] // tile
    small_at = pl.ds(0, columns)

    def loads(unit, slot):
        expert_at, tile_at = unit // tiles, lax.rem(unit, tiles)
        cut = pl.ds(pl.multiple_of(tile_at * tile, tile), tile)
        yield pltpu.make_async_copy(big_hbm.at[expert_at, :, cut], big.at[slot], sems.at[slot, 0])
        for side in (0, 1):
            yield pltpu.make_async_copy(
                small_hbm[side].at[expert_at],
                small.at[slot, side, :, small_at],
                sems.at[slot, 1 + side],
            )

    def stores(unit):
        expert_at, tile_at = unit // tiles, lax.rem(unit, tiles)
        cut = pl.ds(pl.multiple_of(tile_at * tile, tile), tile)
        for side, (stage, target) in enumerate(((wide, own_hbm), (narrow, other_hbm))):
            if big_is_left:
                source, where = stage.at[:, small_at], target.at[expert_at, cut, :]
            else:
                source, where = stage.at[small_at, :], target.at[expert_at, :, cut]
            yield pltpu.make_async_copy(source, where, sems.at[2, side])

    def run(start, count):
        for copy in loads(start, 0):
            copy.start()

        def body(index, carry):
            slot = lax.rem(index, 2)

            @pl.when(index + 1 < count)
            def _():
                for copy in loads(start + index + 1, 1 - slot):
                    copy.start()

            for copy in loads(start + index, slot):
                copy.wait()
            sums = []
            for side in (0, 1):
                left, right = big[slot], small[slot, side, :, small_at]
                sums.append(dot_tn(left, right) if big_is_left else dot_tn(right, left))

            @pl.when(index > 0)
            def _():
                for copy in stores(start + index - 1):
                    copy.wait()

            for stage, total in zip((wide, narrow), sums):
                if big_is_left:
                    stage[:, small_at] = total.astype(stage.dtype)
                else:
                    stage[small_at, :] = total.astype(stage.dtype)
            for copy in stores(start + index):
                copy.start()
            return carry

        lax.fori_loop(0, count, body, 0)
        for copy in stores(start + count - 1):
            copy.wait()

    return run, tiles


def reduce_kernel(depth, half, filled, *refs):
    refs = list(refs)

    def take(count):
        taken = refs[:count]
        del refs[:count]
        return taken

    pick_ref, rows_ref = take(2)
    factors = take(6) if filled else ()
    (out_ref,) = take(1)
    grads = take(4) if filled else ()
    part, value, pick, one, two, right, left = take(7)
    load_sem, s1, r1, s2, r2, sr, rr, sl, rl = take(9)
    ep = lax.axis_index("ep")
    x = lax.axis_index("x")
    z = ep // 2
    y = lax.rem(ep, 2)
    first = ({"x": 1 - x}, {"ep": z * 2 + 1 - y})
    second = (first[1], first[0])
    up, down = {"ep": ep + 2}, {"ep": ep - 2}
    barrier = pltpu.get_barrier_semaphore()
    greet(first[0])
    greet(first[1])
    pl.when(z < depth - 1)(lambda: greet(up))
    pl.when(z > 0)(lambda: greet(down))
    peers = 2 + (z > 0).astype(jnp.int32) + (z < depth - 1).astype(jnp.int32)
    pl.semaphore_wait(barrier, peers)

    local, _, capacity, _ = rows_ref.shape
    total = 4 * depth

    def level_of(turn):
        return jnp.where(lax.rem(turn, 2) == 0, depth - 1 - turn // 2, turn // 2)

    def place(number):
        later = number - depth
        level = jnp.where(later < 0, level_of(number), level_of(later // 3))
        kind = jnp.where(later < 0, 0, 1 + lax.rem(later, 3))
        return level, kind

    def fetch(number, slot):
        level, kind = place(number)
        near_y = jnp.where(lax.rem(kind, 2) == 1, y, 1 - y)
        near_x = jnp.where(kind >= 2, x, 1 - x)
        block = (level * 2 + near_y) * 2 + near_x
        yield pltpu.make_async_copy(rows_ref.at[:, block], value.at[slot], load_sem.at[slot, 0])
        yield pltpu.make_async_copy(pick_ref.at[block], pick.at[slot], load_sem.at[slot, 1])

    def compute(number):
        slot = lax.rem(number, 2)

        @pl.when(number + 1 < total)
        def _():
            for copy in fetch(number + 1, 1 - slot):
                copy.start()

        for copy in fetch(number, slot):
            copy.wait()
        level, kind = place(number)
        for side in (0, 1):
            picked = value[slot, :, :, side * half : (side + 1) * half]
            picked = picked.reshape(local * capacity, half)
            part[level, kind, side] = dot_tn(pick[slot], picked).astype(BF16)

    def send_one(side, level, step):
        return remote(
            part.at[level, 0 if step == 0 else 1 + side, side],
            one.at[side, level, step],
            s1.at[side, level, step],
            r1.at[side, level, step],
            first[side],
        )

    def send_two(side, level):
        return remote(
            one.at[side, level, 0],
            two.at[side, level],
            s2.at[side, level],
            r2.at[side, level],
            second[side],
        )

    def go_right(side, level):
        ref = right.at[side, level]
        return remote(ref, ref, sr.at[side, level], rr.at[side, level], up)

    def go_left(side, level):
        ref = left.at[side, level]
        return remote(ref, ref, sl.at[side, level], rl.at[side, level], down)

    fills = []
    if filled:
        hidden, gates, outs = factors[:3], factors[3:], grads
        scratch = take(5)
        fills.append(fill_job(gates[0], gates[1:], outs[0], outs[1], True, *scratch))
        fills.append(fill_job(hidden[0], hidden[1:], outs[2], outs[3], False, *scratch))

    for copy in fetch(0, 0):
        copy.start()

    def open_turn(turn, carry):
        compute(turn)
        level = level_of(turn)
        for side in (0, 1):
            send_one(side, level, 0).start()
        return carry

    lax.fori_loop(0, depth, open_turn, 0)

    def turn_one(turn, carry):
        lax.fori_loop(0, 3, lambda k, c: (compute(depth + turn * 3 + k), c)[1], 0)
        level = level_of(turn)
        for side in (0, 1):
            send_one(side, level, 0).wait()
            arrived = one.at[side, level, 0]
            add_into(arrived, [arrived, part.at[level, 2 - side, side]])
            send_two(side, level).start()
            send_one(side, level, 1).start()
        for run, tiles in fills:
            share = local * tiles // depth
            run(turn * share, share)
        return carry

    lax.fori_loop(0, depth, turn_one, 0)

    def begin(level):
        for side in (0, 1):
            if level > 0:

                @pl.when(z == 0)
                def _():
                    add_into(right.at[side, level], [two.at[side, level]])
                    go_right(side, level).start()

            if level < depth - 1:

                @pl.when(z == depth - 1)
                def _():
                    add_into(left.at[side, level], [two.at[side, level]])
                    go_left(side, level).start()

    def forward(level):
        for side in (0, 1):

            @pl.when((z > 0) & (z < level))
            def _():
                go_right(side, level).wait_recv()
                ref = right.at[side, level]
                add_into(ref, [ref, two.at[side, level]])
                go_right(side, level).start()

            @pl.when((z < depth - 1) & (z > level))
            def _():
                go_left(side, level).wait_recv()
                ref = left.at[side, level]
                add_into(ref, [ref, two.at[side, level]])
                go_left(side, level).start()

    order = visiting_order(depth)
    for turn, level in enumerate(order):
        for side in (0, 1):
            send_one(side, level, 1).wait()
            kept = part.at[level, 3, side]
            add_into(kept, [one.at[side, level, 1], kept])
            send_two(side, level).wait()
            add_into(two.at[side, level], [two.at[side, level], kept])
        begin(level)
        if turn > 0:
            forward(order[turn - 1])
    forward(order[-1])
    for level in range(depth):

        @pl.when(z == level)
        def _():
            for side in (0, 1):
                terms = [two.at[side, level]]
                if level > 0:
                    go_right(side, level).wait_recv()
                    terms.append(right.at[side, level])
                if level < depth - 1:
                    go_left(side, level).wait_recv()
                    terms.append(left.at[side, level])
                add_into(out_ref.at[:, pl.ds(side * half, half)], terms)

        for side in (0, 1):
            pl.when(z < level)(lambda: go_right(side, level).wait_send())
            pl.when(z > level)(lambda: go_left(side, level).wait_send())


def plane_reduce(pick, values, collective_id, factors=()):
    local, blocks, capacity, columns = values.shape
    rows = pick.shape[-1]
    ep_count, x_count = lax.axis_size("ep"), lax.axis_size("x")
    if x_count != 2 or ep_count % 2 or blocks * rows * columns > 2**23 or local * 4 % ep_count:
        (flat,) = combine(pick, values, group=4)
        flat = flat.reshape(blocks * rows, columns)
        total = lax.psum_scatter(flat, PLANE, scatter_dimension=0, tiled=True).astype(F32)
        if not factors:
            return total
        g_rows, h0, h1, h_rows, g0, g1 = factors
        return (
            total,
            einsum("emd,emf->edf", h_rows, g0),
            einsum("emd,emf->edf", h_rows, g1).astype(BF16),
            einsum("emf,emd->efd", h0, g_rows),
            einsum("emf,emd->efd", h1, g_rows).astype(BF16),
        )
    depth, half = ep_count // 2, columns // 2

    def buffer(*lead):
        return pltpu.VMEM(lead + (rows, half), BF16)

    def sems(*lead):
        return pltpu.SemaphoreType.DMA(lead)

    shapes = [jax.ShapeDtypeStruct((rows, columns), F32)]
    scratch = [
        buffer(depth, 4, 2),
        pltpu.VMEM((2, local, capacity, columns), BF16),
        pltpu.VMEM((2, local * capacity, rows), BF16),
        buffer(2, depth, 2), buffer(2, depth), buffer(2, depth), buffer(2, depth),
        sems(2, 2), sems(2, depth, 2), sems(2, depth, 2),
        sems(2, depth), sems(2, depth), sems(2, depth),
        sems(2, depth), sems(2, depth), sems(2, depth),
    ]
    if factors:
        count, hidden, gates = factors[0].shape[1], factors[1].shape[2], factors[4].shape[2]
        shapes += [
            jax.ShapeDtypeStruct((local, columns, gates), F32),
            jax.ShapeDtypeStruct((local, columns, gates), BF16),
            jax.ShapeDtypeStruct((local, hidden, columns), F32),
            jax.ShapeDtypeStruct((local, hidden, columns), BF16),
        ]
        scratch += [
            pltpu.VMEM((2, count, gates), BF16),
            pltpu.VMEM((2, 2, count, gates), BF16),
            pltpu.VMEM((gates, gates), F32),
            pltpu.VMEM((gates, gates), BF16),
            sems(3, 3),
        ]
    anywhere = pl.BlockSpec(memory_space=pl.ANY)
    results = pl.pallas_call(
        functools.partial(reduce_kernel, depth, half, bool(factors)),
        out_shape=shapes,
        in_specs=[anywhere] * (2 + len(factors)),
        out_specs=[pl.BlockSpec(memory_space=pltpu.VMEM)] + [anywhere] * (len(shapes) - 1),
        scratch_shapes=scratch,
        compiler_params=pltpu.CompilerParams(
            collective_id=collective_id, has_side_effects=True, vmem_limit_bytes=VMEM_BYTES
        ),
        name="plane_reduce",
    )(pick, values, *factors)
    return results if factors else results[0]


def group_kernel(pieces, p_ref, out_ref, near, far, kept, got, own_sem, s1, r1, s2, r2, s3, r3):
    x, core = lax.axis_index("x"), lax.axis_index("core")
    partner, across = {"core": 1 - core}, {"x": 1 - x}
    greet(partner)
    greet(across)
    pl.semaphore_wait(pltpu.get_barrier_semaphore(), 2)
    step = out_ref.shape[0] // pieces

    def at(piece):
        return pl.ds(piece * step, step)

    def hand_over(piece):
        return remote(
            p_ref.at[1 - x, 1 - core, at(piece), :],
            near.at[at(piece), :],
            s1.at[piece],
            r1.at[piece],
            partner,
        )

    def send_across(piece):
        return remote(
            far.at[at(piece), :], got.at[at(piece), :], s2.at[piece], r2.at[piece], across
        )

    stay = remote(p_ref.at[x, 1 - core], kept.at[0], s3, r3, partner)
    loads = (
        pltpu.make_async_copy(p_ref.at[1 - x, core], far, own_sem.at[0]),
        pltpu.make_async_copy(p_ref.at[x, core], kept.at[1], own_sem.at[1]),
    )
    loads[0].start()
    for piece in range(pieces):
        hand_over(piece).start()
    stay.start()
    loads[1].start()
    loads[0].wait()
    for piece in range(pieces):
        hand_over(piece).wait()
        mine = far.at[at(piece), :]
        add_into(mine, [mine, near.at[at(piece), :]])
        send_across(piece).start()
    loads[1].wait()
    stay.wait()
    for piece in range(pieces):
        send_across(piece).wait()
        rows = at(piece)
        add_into(
            out_ref.at[rows, :], [kept.at[0, rows, :], kept.at[1, rows, :], got.at[rows, :]]
        )


def group_reduce(parts, collective_id):
    if lax.axis_size("x") != 2:
        return scatter(parts, GROUP).astype(F32)
    rows, columns = parts.shape[0] // 4, parts.shape[1]
    pieces = 4

    def sems(*lead):
        return pltpu.SemaphoreType.DMA(lead)

    return pl.pallas_call(
        functools.partial(group_kernel, pieces),
        out_shape=jax.ShapeDtypeStruct((rows, columns), F32),
        in_specs=[pl.BlockSpec(memory_space=pl.ANY)],
        out_specs=pl.BlockSpec(memory_space=pltpu.VMEM),
        scratch_shapes=[
            pltpu.VMEM((rows, columns), BF16),
            pltpu.VMEM((rows, columns), BF16),
            pltpu.VMEM((2, rows, columns), BF16),
            pltpu.VMEM((rows, columns), BF16),
            sems(2),
            sems(pieces),
            sems(pieces),
            sems(pieces),
            sems(pieces),
            pltpu.SemaphoreType.DMA,
            pltpu.SemaphoreType.DMA,
        ],
        compiler_params=pltpu.CompilerParams(collective_id=collective_id, has_side_effects=True),
        name="group_reduce",
    )(parts.reshape(2, 2, rows, columns))


def group_gather_kernel(pieces, v_ref, out_ref, local_sem, s1, r1, s2, r2, s3, r3):
    x, core = lax.axis_index("x"), lax.axis_index("core")
    partner, across = {"core": 1 - core}, {"x": 1 - x}
    greet(partner)
    greet(across)
    pl.semaphore_wait(pltpu.get_barrier_semaphore(), 2)
    step = v_ref.shape[0] // pieces

    def over(piece):
        at = pl.ds(piece * step, step)
        return remote(
            v_ref.at[at, :], out_ref.at[x, core, at, :], s2.at[piece], r2.at[piece], across
        )

    def pass_on(piece):
        ref = out_ref.at[1 - x, core, pl.ds(piece * step, step), :]
        return remote(ref, ref, s3.at[piece], r3.at[piece], partner)

    direct = remote(v_ref, out_ref.at[x, core], s1, r1, partner)
    mine = pltpu.make_async_copy(v_ref, out_ref.at[x, core], local_sem)
    for piece in range(pieces):
        over(piece).start()
    direct.start()
    mine.start()
    for piece in range(pieces):
        over(piece).wait()
        pass_on(piece).start()
    mine.wait()
    direct.wait()
    for piece in range(pieces):
        pass_on(piece).wait()


def group_gather(value, collective_id):
    if lax.axis_size("x") != 2:
        return gather(value, GROUP)
    rows, columns = value.shape
    pieces = 4

    def sems(*lead):
        return pltpu.SemaphoreType.DMA(lead)

    gathered = pl.pallas_call(
        functools.partial(group_gather_kernel, pieces),
        out_shape=jax.ShapeDtypeStruct((2, 2, rows, columns), value.dtype),
        in_specs=[pl.BlockSpec(memory_space=pltpu.VMEM)],
        out_specs=pl.BlockSpec(memory_space=pltpu.VMEM),
        scratch_shapes=[
            pltpu.SemaphoreType.DMA,
            pltpu.SemaphoreType.DMA,
            pltpu.SemaphoreType.DMA,
            sems(pieces),
            sems(pieces),
            sems(pieces),
            sems(pieces),
        ],
        compiler_params=pltpu.CompilerParams(collective_id=collective_id, has_side_effects=True),
        name="group_gather",
    )(value)
    return gathered.reshape(4 * rows, columns)


def turn(value, cosine, sine):
    return value * cosine + pltpu.roll(value, value.shape[-1] // 2, 1) * sine


def turn_back(value, cosine, sine):
    return value * cosine + pltpu.roll(value * sine, value.shape[-1] // 2, 1)


def head_norm(raw):
    inverse = lax.rsqrt(jnp.mean(raw * raw, axis=-1, keepdims=True) + EPS_HEAD)
    return raw * inverse, inverse


def dot_nt(left, right):
    return lax.dot_general(left, right, (((1,), (1,)), ((), ())), preferred_element_type=F32)


def dot_tn(left, right):
    return lax.dot_general(left, right, (((0,), (0,)), ((), ())), preferred_element_type=F32)


def dot_nn(left, right):
    return lax.dot_general(left, right, (((1,), (0,)), ((), ())), preferred_element_type=F32)


def weights_of(q_rows, keys, doc_rows, doc_keys, scale):
    scores = dot_nt(q_rows, keys) * scale
    scores = jnp.where(doc_rows == doc_keys, scores, MASKED)
    lifted = jnp.exp(scores - jnp.max(scores, axis=-1, keepdims=True))
    return lifted / jnp.sum(lifted, axis=-1, keepdims=True)


def attend_kernel(step, q_ref, k_ref, v_ref, qg_ref, kg_ref, cos_ref, sin_ref, dr_ref, dk_ref, o_ref):
    scale = q_ref.shape[-1] ** (-0.5)
    cosine, sine = cos_ref[...], sin_ref[...]
    queries = turn(head_norm(q_ref[...])[0] * qg_ref[...], cosine, sine).astype(BF16)
    keys = turn(head_norm(k_ref[...])[0] * kg_ref[...], cosine, sine).astype(BF16)
    values = v_ref[...].astype(BF16)
    for at in range(0, q_ref.shape[0], step):
        rows = slice(at, at + step)
        weights = weights_of(queries[rows], keys, dr_ref[rows, :], dk_ref[...], scale)
        o_ref[rows, :] = dot_nn(weights.astype(BF16), values).astype(BF16)


def attend_back_kernel(
    step, q_ref, k_ref, v_ref, go_ref, qg_ref, kg_ref, cos_ref, sin_ref, dr_ref, dk_ref,
    gq_ref, gk_ref, gv_ref, gqg_ref, gkg_ref,
):
    scale = q_ref.shape[-1] ** (-0.5)
    cosine, sine = cos_ref[...], sin_ref[...]
    q_normed, q_inverse = head_norm(q_ref[...])
    k_normed, k_inverse = head_norm(k_ref[...])
    queries = turn(q_normed * qg_ref[...], cosine, sine).astype(BF16)
    keys = turn(k_normed * kg_ref[...], cosine, sine).astype(BF16)
    values = v_ref[...].astype(BF16)
    grad_keys = jnp.zeros(k_ref.shape, F32)
    grad_values = jnp.zeros(v_ref.shape, F32)
    grad_queries = []
    for at in range(0, q_ref.shape[0], step):
        rows = slice(at, at + step)
        probs = weights_of(queries[rows], keys, dr_ref[rows, :], dk_ref[...], scale)
        grad_rows = go_ref[rows, :]
        grad_weights = dot_nt(grad_rows, values)
        delta = jnp.sum(grad_weights * probs, axis=-1, keepdims=True)
        grad_scores = (probs * (grad_weights - delta)).astype(BF16)
        grad_queries.append(dot_nn(grad_scores, keys))
        grad_keys = grad_keys + dot_tn(grad_scores, queries[rows])
        grad_values = grad_values + dot_tn(probs.astype(BF16), grad_rows)

    @pl.when(pl.program_id(0) == 0)
    def _():
        gqg_ref[...] = jnp.zeros_like(gqg_ref)
        gkg_ref[...] = jnp.zeros_like(gkg_ref)

    def finish(grad, normed, inverse, gain_ref, out_ref, gain_grad_ref):
        grad = turn_back(grad * scale, cosine, sine)
        gain_grad_ref[...] += jnp.sum(grad * normed, axis=0, keepdims=True)
        lifted = grad * gain_ref[...]
        inner = jnp.mean(lifted * normed, axis=-1, keepdims=True)
        out_ref[...] = ((lifted - normed * inner) * inverse).astype(BF16)

    finish(jnp.concatenate(grad_queries, axis=0), q_normed, q_inverse, qg_ref, gq_ref, gqg_ref)
    finish(grad_keys, k_normed, k_inverse, kg_ref, gk_ref, gkg_ref)
    gv_ref[...] = grad_values.astype(BF16)


def attention_call(kernel, heads, head_dim, seq_len, values, tables, outs, flops):
    column = pl.BlockSpec((seq_len, head_dim), lambda head: (0, head))
    whole = [pl.BlockSpec(t.shape, lambda head: (0, 0)) for t in tables]
    shapes = [
        jax.ShapeDtypeStruct((seq_len, heads * head_dim), BF16) if wide
        else jax.ShapeDtypeStruct((1, head_dim), F32)
        for wide in outs
    ]
    specs = [column if wide else pl.BlockSpec((1, head_dim), lambda head: (0, 0)) for wide in outs]
    return pl.pallas_call(
        functools.partial(kernel, min(512, seq_len)),
        grid=(heads,),
        out_shape=shapes,
        in_specs=[column] * len(values) + whole,
        out_specs=specs,
        compiler_params=pltpu.CompilerParams(vmem_limit_bytes=VMEM_BYTES),
        cost_estimate=pl.CostEstimate(
            flops=flops, bytes_accessed=16 * seq_len * heads * head_dim, transcendentals=heads * seq_len**2
        ),
        name="attention",
    )(*values, *tables)


def params(flops, moved):
    return dict(compiler_params=pltpu.CompilerParams(vmem_limit_bytes=VMEM_BYTES),
        cost_estimate=pl.CostEstimate(flops=flops, bytes_accessed=moved, transcendentals=0))


def pick_rows_of(pick, value, out_ref, index):
    local, _, capacity, _ = out_ref.shape
    rows = dot_nn(pick, value).astype(BF16)
    for expert_at in range(local):
        out_ref[expert_at, index] = rows[expert_at * capacity : (expert_at + 1) * capacity]


def dispatch_kernel(pick_ref, value_ref, out_ref):
    for index in range(pick_ref.shape[0]):
        pick_rows_of(pick_ref[index], value_ref[index], out_ref, index)


def dispatch(pick, value, local, group):
    blocks, picked, rows = pick.shape
    width = value.shape[-1]
    capacity = picked // local
    return pl.pallas_call(
        dispatch_kernel,
        grid=(blocks // group,),
        out_shape=jax.ShapeDtypeStruct((local, blocks, capacity, width), BF16),
        in_specs=[
            pl.BlockSpec((group, picked, rows), lambda b: (b, 0, 0)),
            pl.BlockSpec((group, rows, width), lambda b: (b, 0, 0)),
        ],
        out_specs=pl.BlockSpec((local, group, capacity, width), lambda b: (0, b, 0, 0)),
        name="dispatch",
        **params(2 * blocks * picked * rows * width, 2 * blocks * width * (picked + rows)),
    )(pick, value)


def combine_kernel(pick_ref, value_ref, *refs):
    local, group, capacity, width = value_ref.shape
    out_ref = refs[-2] if len(refs) == 3 else refs[0]
    for index in range(group):
        pick = pick_ref[index]
        if group == 1:
            value = value_ref[...].reshape(local * capacity, width)
        else:
            value = jnp.concatenate([value_ref[e, index] for e in range(local)], axis=0)
        out_ref[index] = dot_tn(pick, value).astype(BF16)
        if len(refs) == 3:
            for e in range(local):
                part = pick[e * capacity : (e + 1) * capacity].astype(F32)
                refs[2][index, e : e + 1, :] = jnp.sum(
                    part * refs[0][e, index], axis=0, keepdims=True
                )


def combine(pick, value, dots=None, group=2):
    blocks, picked, rows = pick.shape
    local, _, capacity, width = value.shape

    def rows_of(columns):
        return pl.BlockSpec((local, group, capacity, columns), lambda b: (0, b, 0, 0))

    ins, specs = [pick, value], [pl.BlockSpec((group, picked, rows), lambda b: (b, 0, 0)), rows_of(width)]
    shapes = [jax.ShapeDtypeStruct((blocks, rows, width), BF16)]
    outs = [pl.BlockSpec((group, rows, width), lambda b: (b, 0, 0))]
    if dots is not None:
        ins += [dots]
        specs += [rows_of(1)]
        shapes += [jax.ShapeDtypeStruct((blocks, local, rows), F32)]
        outs += [pl.BlockSpec((group, local, rows), lambda b: (b, 0, 0))]
    return pl.pallas_call(
        combine_kernel,
        grid=(blocks // group,),
        out_shape=shapes,
        in_specs=specs,
        out_specs=outs,
        name="combine",
        **params(2 * blocks * picked * rows * width, 2 * blocks * width * (picked + rows)),
    )(*ins)


def down_kernel(h0_ref, h1_ref, w0_ref, w1_ref, out_ref):
    out_ref[0] = (dot_nn(h0_ref[0], w0_ref[0]) + dot_nn(h1_ref[0], w1_ref[0])).astype(BF16)


def down_rows(h0, h1, w0, w1, step):
    local, count, hidden = h0.shape
    width = w0.shape[-1]
    rows = pl.BlockSpec((1, step, hidden), lambda e, i: (e, i, 0))
    weight = pl.BlockSpec((1, hidden, width), lambda e, i: (e, 0, 0))
    return pl.pallas_call(
        down_kernel,
        grid=(local, count // step),
        out_shape=jax.ShapeDtypeStruct((local, count, width), BF16),
        in_specs=[rows, rows, weight, weight],
        out_specs=pl.BlockSpec((1, step, width), lambda e, i: (e, i, 0)),
        name="down_rows",
        **params(4 * local * count * hidden * width, 2 * local * (count + 2 * hidden) * width),
    )(h0, h1, w0, w1)


def expert_kernel(x_ref, w0_ref, w1_ref, u0_ref, u1_ref, pr_ref, gx_ref, dots_ref, *outs):
    x = x_ref[0]
    prob = pr_ref[0]
    total = None
    dots = None
    for w_ref, u_ref, hp_ref, ggu_ref in ((w0_ref, u0_ref, outs[0], outs[2]), (w1_ref, u1_ref, outs[1], outs[3])):
        n = u_ref.shape[-1]
        both = dot_nn(x, w_ref[0])
        gate, up = both[:, :n], both[:, n:]
        sigma = jax.nn.sigmoid(gate)
        silu = gate * sigma
        hidden = (silu * up).astype(BF16).astype(F32)
        back = u_ref[0]
        part = jnp.sum(hidden * back, axis=-1, keepdims=True)
        dots = part if dots is None else dots + part
        hp_ref[0] = (hidden * prob).astype(BF16)
        gh = back * prob
        ggu_ref[0, :, :n] = (gh * up * (sigma + silu * (1.0 - sigma))).astype(BF16)
        ggu_ref[0, :, n:] = (gh * silu).astype(BF16)
        part = dot_nt(ggu_ref[0], w_ref[0])
        total = part if total is None else total + part
    gx_ref[0] = total.astype(BF16)
    dots_ref[0] = dots


def expert(x, w0, w1, u0, u1, prob, step):
    local, count, width = x.shape
    n = u0.shape[-1]
    r = lambda c: pl.BlockSpec((1, step, c), lambda e, i: (e, i, 0))
    w = pl.BlockSpec((1, width, 2*n), lambda e, i: (e, 0, 0))
    s = lambda c, t: jax.ShapeDtypeStruct((local, count, c), t)
    return pl.pallas_call(
        expert_kernel, grid=(local, count//step),
        out_shape=[s(width,BF16), s(1,F32), s(n,BF16), s(n,BF16), s(2*n,BF16), s(2*n,BF16)],
        in_specs=[r(width), w, w, r(n), r(n), r(1)],
        out_specs=[r(width), r(1), r(n), r(n), r(2*n), r(2*n)],
        name="expert", **params(16*local*count*width*n, local*(count*(width*4+n*20)+8*width*n)),
    )(x, w0, w1, u0, u1, prob)


def norm_rows(value, gain):
    inverse = lax.rsqrt(jnp.mean(value * value, axis=-1, keepdims=True) + EPS_NORM)
    return value * inverse * gain


def norm_back(value, gain, grad):
    inverse = lax.rsqrt(jnp.mean(value * value, axis=-1, keepdims=True) + EPS_NORM)
    normed = value * inverse
    lifted = grad * gain
    inner = jnp.mean(lifted * normed, axis=-1, keepdims=True)
    return (lifted - normed * inner) * inverse, jnp.sum(grad * normed, axis=0)


def positions(lengths, seq_len):
    ends = jnp.cumsum(lengths)
    starts = ends - lengths
    index = jnp.arange(seq_len, dtype=jnp.int32)
    doc_ids = jnp.sum((index[:, None] >= ends[None, :]).astype(jnp.int32), axis=1)
    member = doc_ids[:, None] == jnp.arange(lengths.shape[0], dtype=jnp.int32)[None, :]
    offset = jnp.sum(jnp.where(member, starts[None, :], 0), axis=1)
    return (doc_ids, index - offset)


def rope_tables(position, head_dim):
    half = head_dim // 2
    freq = ROPE_BASE ** (-(2.0 * jnp.arange(half, dtype=F32)) / head_dim)
    angle = position.astype(F32)[:, None] * freq[None, :]
    return (jnp.cos(angle), jnp.sin(angle))


def einsum(spec, left, right):
    return jnp.einsum(spec, left, right, preferred_element_type=F32)


def swap_cores(value):
    return lax.ppermute(value, "core", [(0, 1), (1, 0)])


def gather(value, axes):
    return lax.all_gather(value, axes, axis=0, tiled=True)


def scatter(value, axes, dim=0):
    return lax.psum_scatter(value, axes, scatter_dimension=dim, tiled=True)


def masked_softmax(logits, mask):
    kept = jnp.where(mask, logits, MASKED)
    lifted = jnp.where(mask, jnp.exp(kept - jnp.max(kept, axis=-1, keepdims=True)), 0.0)
    return lifted / jnp.sum(lifted, axis=-1, keepdims=True)


def route_mask(routes, experts_all):
    ids = jnp.arange(experts_all, dtype=jnp.int32)
    return jnp.any(routes[:, :, None] == ids[None, None, :], axis=1)


def per_device(
    layer_input,
    routes,
    doc_lengths,
    norm1_gain,
    w_qkv,
    q_gain,
    k_gain,
    w_out,
    norm2_gain,
    w_router,
    expert_gate_up,
    expert_down,
    d_out,
):
    rows, width = layer_input.shape
    x_count = lax.axis_size("x")
    ep_count = lax.axis_size("ep")
    seq_len = rows * x_count * 2
    blocks = ep_count * x_count
    topk = routes.shape[1]
    experts_all = w_router.shape[1]
    local = expert_gate_up.shape[0]
    hidden_local = expert_down.shape[1]
    head_dim = q_gain.shape[0]
    qkv_local = w_qkv.shape[2]
    heads = qkv_local // head_dim
    capacity = min(3 * rows * topk // (2 * experts_all), rows)
    my_ep = lax.axis_index("ep")

    gain_one = norm1_gain.astype(F32)
    gain_two = norm2_gain.astype(F32)
    inputs = layer_input.astype(F32)
    grad_out = d_out.astype(F32)
    input_seq = group_gather(layer_input, 8)
    g_flat = gather(d_out, PLANE)
    h_seq = norm_rows(input_seq.astype(F32), gain_one).astype(BF16)
    w_parts = w_qkv.transpose(1, 0, 2)
    raw = [jnp.dot(h_seq, w_parts[part], preferred_element_type=F32) for part in range(3)]
    doc_ids, position = positions(doc_lengths[0], seq_len)
    cosine, sine = rope_tables(position, head_dim)
    tables = (
        q_gain.astype(F32)[None],
        k_gain.astype(F32)[None],
        jnp.concatenate([cosine, cosine], axis=1),
        jnp.concatenate([-sine, sine], axis=1),
        doc_ids[:, None],
        doc_ids[None, :],
    )
    (attn_vals,) = attention_call(
        attend_kernel, heads, head_dim, seq_len, raw, tables, (True,), 4 * seq_len**2 * qkv_local
    )
    attn_part = jnp.dot(attn_vals, w_out, preferred_element_type=F32).astype(BF16)
    attn_out = group_reduce(attn_part, 7)
    middle = inputs + attn_out
    h_two = norm_rows(middle, gain_two).astype(BF16)

    g_plane = g_flat.reshape(blocks, rows, width)
    mask_own = route_mask(routes, experts_all)
    probs_own = masked_softmax(jnp.dot(h_two, w_router, preferred_element_type=F32), mask_own)
    shared = spread(jnp.where(mask_own, probs_own, -1.0).T, PLANE, 1)
    h_flat = gather(h_two, PLANE)
    pair_other = swap_cores(expert_gate_up.reshape(local, width, 2 * hidden_local))
    down_other = swap_cores(expert_down)
    pair_own = expert_gate_up.reshape(local, width, 2 * hidden_local)

    first = my_ep * local
    here = lax.dynamic_slice_in_dim(shared, first, local, axis=1)
    mask_here = here >= 0.0
    before = jnp.triu(jnp.ones((rows, rows), BF16), 1)
    rank = einsum("bet,tu->beu", mask_here.astype(BF16), before).astype(jnp.int32)
    slots = jnp.arange(capacity, dtype=jnp.int32)[None, None, :, None]
    picks = mask_here[:, :, None, :] & (rank[:, :, None, :] == slots)
    pick = picks.astype(BF16)
    pick_rows = pick.reshape(blocks, local * capacity, rows)
    count = blocks * capacity

    g_rows = dispatch(pick_rows, g_plane, local, group=4)
    g_rows = g_rows.reshape(local, count, width)
    back_own = einsum("emd,efd->emf", g_rows, expert_down)
    back_other = einsum("emd,efd->emf", g_rows, down_other)
    prob_rows = jnp.sum(jnp.where(picks, here[:, :, None, :], 0.0), axis=-1)
    prob_rows = prob_rows.transpose(1, 0, 2).reshape(local, count, 1)
    h_flat, back_own, back_other, prob_rows = lax.optimization_barrier(
        (h_flat, back_own, back_other, prob_rows)
    )
    h_rows = dispatch(pick_rows, h_flat.reshape(blocks, rows, width), local, group=4)
    h_rows = h_rows.reshape(local, count, width)
    back_rows, dot_rows, weighted_own, weighted_other, ggu_own, ggu_other = expert(
        h_rows, pair_own, pair_other, back_own, back_other, prob_rows, min(384, count)
    )
    dot_rows = dot_rows.reshape(local, blocks, capacity).transpose(1, 0, 2)
    dots_token = jnp.sum(jnp.where(picks, dot_rows[..., None], 0.0), axis=2)
    grad_probs = spread(dots_token, PLANE, 2, True)
    grad_probs = jnp.sum(grad_probs.reshape(ep_count, x_count, local, rows), axis=1)
    grad_probs = grad_probs.reshape(experts_all, rows).T
    back_sum, grad_pair_own, grad_pair_other, grad_down_own, grad_down_other = plane_reduce(
        pick_rows,
        back_rows.reshape(local, blocks, capacity, width),
        3,
        (g_rows, weighted_own, weighted_other, h_rows, ggu_own, ggu_other),
    )
    out_rows = down_rows(
        weighted_own, weighted_other, expert_down, down_other, min(384, count)
    ).reshape(local, blocks, capacity, width)

    grad_pair = grad_pair_own + swap_cores(grad_pair_other).astype(F32)
    grad_down = grad_down_own + swap_cores(grad_down_other).astype(F32)

    inner = jnp.sum(probs_own * grad_probs, axis=-1, keepdims=True)
    grad_logits = probs_own * (grad_probs - inner)
    grad_router = lax.dot_general(
        grad_logits, h_two.astype(F32), (((0,), (0,)), ((), ())), precision=HIGH
    )
    grad_h_two = back_sum + jnp.dot(
        grad_logits, w_router.astype(F32).T, precision=HIGH
    )
    grad_mid_norm, grad_gain_two = norm_back(middle, gain_two, grad_h_two)
    grad_mid = grad_out + grad_mid_norm

    ga_seq = gather(grad_mid.astype(BF16), GROUP)
    ga_seq, out_rows, grad_down, grad_pair = lax.optimization_barrier(
        (ga_seq, out_rows, grad_down, grad_pair)
    )
    grad_gate_up = grad_pair.reshape(local, width, 2, hidden_local)
    grad_wout = lax.dot_general(
        attn_vals, ga_seq, (((0,), (0,)), ((), ())), preferred_element_type=F32
    )
    grad_vals = lax.dot_general(
        ga_seq, w_out, (((1,), (1,)), ((), ())), preferred_element_type=F32
    )
    *grad_proj, grad_q_gain, grad_k_gain = attention_call(
        attend_back_kernel,
        heads,
        head_dim,
        seq_len,
        (*raw, grad_vals.astype(BF16)),
        tables,
        (True, True, True, False, False),
        10 * seq_len**2 * qkv_local,
    )
    grad_h_part = sum(
        lax.dot_general(grad, w, (((1,), (1,)), ((), ())), preferred_element_type=F32)
        for grad, w in zip(grad_proj, w_parts)
    )
    grad_h_one = scatter(grad_h_part.astype(BF16), GROUP).astype(F32)
    grad_wqkv = jnp.stack(
        [
            lax.dot_general(
                h_seq, grad, (((0,), (0,)), ((), ())), preferred_element_type=F32
            ).astype(BF16)
            for grad in grad_proj
        ],
    )
    grad_in_norm, grad_gain_one = norm_back(inputs, gain_one, grad_h_one)
    grad_input = grad_mid + grad_in_norm
    dense_qkv = scatter(grad_wqkv, "ep", 1).astype(F32)
    dense_out = scatter(grad_wout.astype(BF16), "ep", 1).astype(F32)
    devices = blocks * 2
    small = jnp.concatenate(
        [grad_router.reshape(-1), grad_gain_one, grad_gain_two, grad_q_gain[0], grad_k_gain[0]]
    )
    length = small.shape[0]
    padded = -(-length // (devices * 1024)) * devices * 1024
    small = jnp.pad(small, (0, padded - length)).reshape(devices, -1, 128)
    small = jnp.sum(spread(small, ALL, 5, True), axis=0)
    small = spread(small, ALL, 6).reshape(-1)
    out_rows, small = lax.optimization_barrier((out_rows, small))
    output = (middle + plane_reduce(pick_rows, out_rows, 4)).astype(BF16)
    cuts = (experts_all * width, width, width, head_dim, head_dim)
    starts = [sum(cuts[:index]) for index in range(5)]
    router_sum, *gains = (small[at : at + cut] for at, cut in zip(starts, cuts))
    grad_router = router_sum.reshape(experts_all, width).T
    return (
        output,
        grad_input,
        gains[0],
        dense_qkv.transpose(1, 0, 2),
        gains[2],
        gains[3],
        dense_out,
        gains[1],
        grad_router,
        grad_gate_up,
        grad_down,
    )


def solution(mesh):
    ep_count, tp_count = mesh.shape["ep"], mesh.shape["tp"]
    fine = Mesh(mesh.devices.reshape(ep_count, tp_count // 2, 2), ALL)
    in_specs = (
        P(ALL, None),
        P(ALL, None),
        P("ep", None),
        P(),
        P(None, None, GROUP),
        P(),
        P(),
        P(GROUP, None),
        P(),
        P(),
        P("ep", None, None, GROUP),
        P("ep", GROUP, None),
        P(ALL, None),
    )
    out_specs = (
        P(ALL, None),
        P(ALL, None),
        P(),
        P("ep", None, GROUP),
        P(),
        P(),
        P(GROUP, "ep"),
        P(),
        P(),
        P("ep", None, None, GROUP),
        P("ep", GROUP, None),
    )

    return jax.shard_map(
        per_device, mesh=fine, in_specs=in_specs, out_specs=out_specs, check_vma=False
    )
```

```python
import functools
import math

import jax
import jax.numpy as jnp
from jax import lax
from jax.experimental import pallas as pl
from jax.experimental.pallas import tpu as pltpu
from jax.sharding import Mesh
from jax.sharding import PartitionSpec as P


HIGH = lax.Precision.HIGHEST
EPS_NORM = 1e-05
EPS_HEAD = 1e-06
ROPE_BASE = 10000.0
MASKED = -1e30
F32 = jnp.float32
BF16 = jnp.bfloat16
PLANE = ("ep", "x")
GROUP = ("x", "core")
ALL = ("ep", "x", "core")

MESH = pl.DeviceIdType.MESH
VMEM_BYTES = 60 * 1024 * 1024


def remote(source, target, send, recv, where):
    return pltpu.make_async_remote_copy(
        src_ref=source,
        dst_ref=target,
        send_sem=send,
        recv_sem=recv,
        device_id=where,
        device_id_type=MESH,
    )


def greet(where):
    pl.semaphore_signal(
        pltpu.get_barrier_semaphore(), inc=1, device_id=where, device_id_type=MESH
    )


def add_into(target, terms, step=32):
    def body(index, carry):
        at = pl.ds(pl.multiple_of(index * step, step), step)
        total = terms[0][at, :].astype(F32)
        for term in terms[1:]:
            total = total + term[at, :].astype(F32)
        target[at, :] = total.astype(target.dtype)
        return carry

    lax.fori_loop(0, target.shape[0] // step, body, 0)


def peer_of(axes, counts, index):
    where = {}
    for axis, count in reversed(list(zip(axes, counts))):
        where[axis] = lax.rem(index, count)
        index = index // count
    return where


def spread_kernel(axes, counts, own_slices, v_ref, out_ref, local_sem, send, recv):
    total = math.prod(counts)
    me = 0
    for axis, count in zip(axes, counts):
        me = me * count + lax.axis_index(axis)

    def hello(step, carry):
        greet(peer_of(axes, counts, lax.rem(me + step, total)))
        return carry

    lax.fori_loop(1, total, hello, 0)
    pl.semaphore_wait(pltpu.get_barrier_semaphore(), total - 1)

    def copy(step):
        peer = lax.rem(me + step, total)
        source = v_ref.at[peer] if own_slices else v_ref
        return remote(
            source, out_ref.at[me], send.at[step], recv.at[step], peer_of(axes, counts, peer)
        )

    mine = pltpu.make_async_copy(
        v_ref.at[me] if own_slices else v_ref, out_ref.at[me], local_sem
    )
    mine.start()

    def begin(step, carry):
        copy(step).start()
        return carry

    def finish(step, carry):
        copy(step).wait()
        return carry

    lax.fori_loop(1, total, begin, 0)
    mine.wait()
    lax.fori_loop(1, total, finish, 0)


def spread(value, axes, collective_id, own_slices=False):
    counts = tuple(lax.axis_size(axis) for axis in axes)
    total = math.prod(counts)
    shape = value.shape[1:] if own_slices else value.shape
    return pl.pallas_call(
        functools.partial(spread_kernel, axes, counts, own_slices),
        out_shape=jax.ShapeDtypeStruct((total,) + shape, value.dtype),
        in_specs=[pl.BlockSpec(memory_space=pltpu.VMEM)],
        out_specs=pl.BlockSpec(memory_space=pltpu.VMEM),
        scratch_shapes=[
            pltpu.SemaphoreType.DMA,
            pltpu.SemaphoreType.DMA((total,)),
            pltpu.SemaphoreType.DMA((total,)),
        ],
        compiler_params=pltpu.CompilerParams(
            collective_id=collective_id, has_side_effects=True
        ),
        name="spread",
    )(value)


def visiting_order(count):
    order, low, high = [], 0, count - 1
    while low <= high:
        order.append(high)
        high -= 1
        if low <= high:
            order.append(low)
            low += 1
    return order


def fill_job(big_hbm, small_hbm, own_hbm, other_hbm, big_is_left, big, small, wide, narrow, sems):
    tile = big.shape[-1]
    columns = small_hbm[0].shape[-1]
    tiles = big_hbm.shape[-1] // tile
    small_at = pl.ds(0, columns)

    def loads(unit, slot):
        expert_at, tile_at = unit // tiles, lax.rem(unit, tiles)
        cut = pl.ds(pl.multiple_of(tile_at * tile, tile), tile)
        yield pltpu.make_async_copy(big_hbm.at[expert_at, :, cut], big.at[slot], sems.at[slot, 0])
        for side in (0, 1):
            yield pltpu.make_async_copy(
                small_hbm[side].at[expert_at],
                small.at[slot, side, :, small_at],
                sems.at[slot, 1 + side],
            )

    def stores(unit):
        expert_at, tile_at = unit // tiles, lax.rem(unit, tiles)
        cut = pl.ds(pl.multiple_of(tile_at * tile, tile), tile)
        for side, (stage, target) in enumerate(((wide, own_hbm), (narrow, other_hbm))):
            if big_is_left:
                source, where = stage.at[:, small_at], target.at[expert_at, cut, :]
            else:
                source, where = stage.at[small_at, :], target.at[expert_at, :, cut]
            yield pltpu.make_async_copy(source, where, sems.at[2, side])

    def run(start, count):
        for copy in loads(start, 0):
            copy.start()

        def body(index, carry):
            slot = lax.rem(index, 2)

            @pl.when(index + 1 < count)
            def _():
                for copy in loads(start + index + 1, 1 - slot):
                    copy.start()

            for copy in loads(start + index, slot):
                copy.wait()
            sums = []
            for side in (0, 1):
                left, right = big[slot], small[slot, side, :, small_at]
                sums.append(dot_tn(left, right) if big_is_left else dot_tn(right, left))

            @pl.when(index > 0)
            def _():
                for copy in stores(start + index - 1):
                    copy.wait()

            for stage, total in zip((wide, narrow), sums):
                if big_is_left:
                    stage[:, small_at] = total.astype(stage.dtype)
                else:
                    stage[small_at, :] = total.astype(stage.dtype)
            for copy in stores(start + index):
                copy.start()
            return carry

        lax.fori_loop(0, count, body, 0)
        for copy in stores(start + count - 1):
            copy.wait()

    return run, tiles


def reduce_kernel(depth, half, sides, filled, *refs):
    refs = list(refs)

    def take(count):
        taken = refs[:count]
        del refs[:count]
        return taken

    pick_ref, rows_ref = take(2)
    factors = take(6) if filled else ()
    (out_ref,) = take(1)
    grads = take(4) if filled else ()
    part, value, pick, one, two, right, left = take(7)
    load_sem, s1, r1, s2, r2, sr, rr, sl, rl = take(9)
    ep = lax.axis_index("ep")
    x = lax.axis_index("x")
    z = ep // 2
    y = lax.rem(ep, 2)
    first = ({"x": 1 - x}, {"ep": z * 2 + 1 - y})
    second = (first[1], first[0])
    up, down = {"ep": ep + 2}, {"ep": ep - 2}
    barrier = pltpu.get_barrier_semaphore()
    greet(first[0])
    greet(first[1])
    pl.when(z < depth - 1)(lambda: greet(up))
    pl.when(z > 0)(lambda: greet(down))
    peers = 2 + (z > 0).astype(jnp.int32) + (z < depth - 1).astype(jnp.int32)
    pl.semaphore_wait(barrier, peers)

    local, _, capacity, _ = rows_ref.shape
    total = 4 * depth

    def level_of(turn):
        return jnp.where(lax.rem(turn, 2) == 0, depth - 1 - turn // 2, turn // 2)

    def place(number):
        later = number - depth
        level = jnp.where(later < 0, level_of(number), level_of(later // 3))
        kind = jnp.where(later < 0, 0, 1 + lax.rem(later, 3))
        return level, kind

    def fetch(number, slot):
        level, kind = place(number)
        near_y = jnp.where(lax.rem(kind, 2) == 1, y, 1 - y)
        near_x = jnp.where(kind >= 2, x, 1 - x)
        block = (level * 2 + near_y) * 2 + near_x
        yield pltpu.make_async_copy(rows_ref.at[:, block], value.at[slot], load_sem.at[slot, 0])
        yield pltpu.make_async_copy(pick_ref.at[block], pick.at[slot], load_sem.at[slot, 1])

    def compute(number):
        slot = lax.rem(number, 2)

        @pl.when(number + 1 < total)
        def _():
            for copy in fetch(number + 1, 1 - slot):
                copy.start()

        for copy in fetch(number, slot):
            copy.wait()
        level, kind = place(number)
        for side in range(sides):
            picked = value[slot, :, :, side * half : (side + 1) * half]
            picked = picked.reshape(local * capacity, half)
            part[level, kind, side] = dot_tn(pick[slot], picked).astype(BF16)

    def send_one(side, level, step):
        return remote(
            part.at[level, 0 if step == 0 else 1 + side, side],
            one.at[side, level, step],
            s1.at[side, level, step],
            r1.at[side, level, step],
            first[side],
        )

    def send_two(side, level):
        return remote(
            one.at[side, level, 0],
            two.at[side, level],
            s2.at[side, level],
            r2.at[side, level],
            second[side],
        )

    def go_right(side, level):
        ref = right.at[side, level]
        return remote(ref, ref, sr.at[side, level], rr.at[side, level], up)

    def go_left(side, level):
        ref = left.at[side, level]
        return remote(ref, ref, sl.at[side, level], rl.at[side, level], down)

    fills = []
    if filled:
        hidden, gates, outs = factors[:3], factors[3:], grads
        scratch = take(5)
        fills.append(fill_job(gates[0], gates[1:], outs[0], outs[1], True, *scratch))
        fills.append(fill_job(hidden[0], hidden[1:], outs[2], outs[3], False, *scratch))

    for copy in fetch(0, 0):
        copy.start()

    def open_turn(turn, carry):
        compute(turn)
        level = level_of(turn)
        for side in range(sides):
            send_one(side, level, 0).start()
        return carry

    lax.fori_loop(0, depth, open_turn, 0)

    def turn_one(turn, carry):
        lax.fori_loop(0, 3, lambda k, c: (compute(depth + turn * 3 + k), c)[1], 0)
        level = level_of(turn)
        for side in range(sides):
            send_one(side, level, 0).wait()
            arrived = one.at[side, level, 0]
            add_into(arrived, [arrived, part.at[level, 2 - side, side]])
            send_two(side, level).start()
            send_one(side, level, 1).start()
        for run, tiles in fills:
            share = local * tiles // depth
            run(turn * share, share)
        return carry

    lax.fori_loop(0, depth, turn_one, 0)

    def begin(level):
        for side in range(sides):
            if level > 0:

                @pl.when(z == 0)
                def _():
                    add_into(right.at[side, level], [two.at[side, level]])
                    go_right(side, level).start()

            if level < depth - 1:

                @pl.when(z == depth - 1)
                def _():
                    add_into(left.at[side, level], [two.at[side, level]])
                    go_left(side, level).start()

    def forward(level):
        for side in range(sides):

            @pl.when((z > 0) & (z < level))
            def _():
                go_right(side, level).wait_recv()
                ref = right.at[side, level]
                add_into(ref, [ref, two.at[side, level]])
                go_right(side, level).start()

            @pl.when((z < depth - 1) & (z > level))
            def _():
                go_left(side, level).wait_recv()
                ref = left.at[side, level]
                add_into(ref, [ref, two.at[side, level]])
                go_left(side, level).start()

    order = visiting_order(depth)
    for turn, level in enumerate(order):
        for side in range(sides):
            send_one(side, level, 1).wait()
            kept = part.at[level, 3, side]
            add_into(kept, [one.at[side, level, 1], kept])
            send_two(side, level).wait()
            add_into(two.at[side, level], [two.at[side, level], kept])
        begin(level)
        if turn > 0:
            forward(order[turn - 1])
    forward(order[-1])
    for level in range(depth):

        @pl.when(z == level)
        def _():
            for side in range(sides):
                terms = [two.at[side, level]]
                if level > 0:
                    go_right(side, level).wait_recv()
                    terms.append(right.at[side, level])
                if level < depth - 1:
                    go_left(side, level).wait_recv()
                    terms.append(left.at[side, level])
                add_into(out_ref.at[:, pl.ds(side * half, half)], terms)

        for side in range(sides):
            pl.when(z < level)(lambda: go_right(side, level).wait_send())
            pl.when(z > level)(lambda: go_left(side, level).wait_send())


def plane_reduce(pick, values, collective_id, factors=(), sides=2):
    local, blocks, capacity, columns = values.shape
    rows = pick.shape[-1]
    ep_count, x_count = lax.axis_size("ep"), lax.axis_size("x")
    if x_count != 2 or ep_count % 2 or blocks * rows * columns > 2**23 or local * 4 % ep_count:
        (flat,) = combine(pick, values, group=4)
        flat = flat.reshape(blocks * rows, columns)
        total = lax.psum_scatter(flat, PLANE, scatter_dimension=0, tiled=True).astype(F32)
        if not factors:
            return total
        g_rows, h0, h1, h_rows, g0, g1 = factors
        return (
            total,
            einsum("emd,emf->edf", h_rows, g0),
            einsum("emd,emf->edf", h_rows, g1).astype(BF16),
            einsum("emf,emd->efd", h0, g_rows),
            einsum("emf,emd->efd", h1, g_rows).astype(BF16),
        )
    depth, half = ep_count // 2, columns // sides

    def buffer(*lead):
        return pltpu.VMEM(lead + (rows, half), BF16)

    def sems(*lead):
        return pltpu.SemaphoreType.DMA(lead)

    shapes = [jax.ShapeDtypeStruct((rows, columns), F32)]
    scratch = [
        buffer(depth, 4, sides),
        pltpu.VMEM((2, local, capacity, columns), BF16),
        pltpu.VMEM((2, local * capacity, rows), BF16),
        buffer(sides, depth, 2),
        buffer(sides, depth), buffer(sides, depth), buffer(sides, depth),
        sems(2, 2), sems(2, depth, 2), sems(2, depth, 2),
        sems(2, depth), sems(2, depth), sems(2, depth),
        sems(2, depth), sems(2, depth), sems(2, depth),
    ]
    if factors:
        count, hidden, gates = factors[0].shape[1], factors[1].shape[2], factors[4].shape[2]
        shapes += [
            jax.ShapeDtypeStruct((local, columns, gates), F32),
            jax.ShapeDtypeStruct((local, columns, gates), BF16),
            jax.ShapeDtypeStruct((local, hidden, columns), F32),
            jax.ShapeDtypeStruct((local, hidden, columns), BF16),
        ]
        scratch += [
            pltpu.VMEM((2, count, gates), BF16),
            pltpu.VMEM((2, 2, count, gates), BF16),
            pltpu.VMEM((gates, gates), F32),
            pltpu.VMEM((gates, gates), BF16),
            sems(3, 3),
        ]
    anywhere = pl.BlockSpec(memory_space=pl.ANY)
    results = pl.pallas_call(
        functools.partial(reduce_kernel, depth, half, sides, bool(factors)),
        out_shape=shapes,
        in_specs=[anywhere] * (2 + len(factors)),
        out_specs=[pl.BlockSpec(memory_space=pltpu.VMEM)] + [anywhere] * (len(shapes) - 1),
        scratch_shapes=scratch,
        compiler_params=pltpu.CompilerParams(
            collective_id=collective_id, has_side_effects=True, vmem_limit_bytes=VMEM_BYTES
        ),
        name="plane_reduce",
    )(pick, values, *factors)
    return results if factors else results[0]


def group_kernel(pieces, p_ref, out_ref, near, far, kept, got, own_sem, s1, r1, s2, r2, s3, r3):
    x, core = lax.axis_index("x"), lax.axis_index("core")
    partner, across = {"core": 1 - core}, {"x": 1 - x}
    greet(partner)
    greet(across)
    pl.semaphore_wait(pltpu.get_barrier_semaphore(), 2)
    step = out_ref.shape[0] // pieces

    def at(piece):
        return pl.ds(piece * step, step)

    def hand_over(piece):
        return remote(
            p_ref.at[1 - x, 1 - core, at(piece), :],
            near.at[at(piece), :],
            s1.at[piece],
            r1.at[piece],
            partner,
        )

    def send_across(piece):
        return remote(
            far.at[at(piece), :], got.at[at(piece), :], s2.at[piece], r2.at[piece], across
        )

    stay = remote(p_ref.at[x, 1 - core], kept.at[0], s3, r3, partner)
    loads = (
        pltpu.make_async_copy(p_ref.at[1 - x, core], far, own_sem.at[0]),
        pltpu.make_async_copy(p_ref.at[x, core], kept.at[1], own_sem.at[1]),
    )
    loads[0].start()
    for piece in range(pieces):
        hand_over(piece).start()
    stay.start()
    loads[1].start()
    loads[0].wait()
    for piece in range(pieces):
        hand_over(piece).wait()
        mine = far.at[at(piece), :]
        add_into(mine, [mine, near.at[at(piece), :]])
        send_across(piece).start()
    loads[1].wait()
    stay.wait()
    for piece in range(pieces):
        send_across(piece).wait()
        rows = at(piece)
        add_into(
            out_ref.at[rows, :], [kept.at[0, rows, :], kept.at[1, rows, :], got.at[rows, :]]
        )


def group_reduce(parts, collective_id):
    if lax.axis_size("x") != 2:
        return scatter(parts, GROUP).astype(F32)
    rows, columns = parts.shape[0] // 4, parts.shape[1]
    pieces = 4

    def sems(*lead):
        return pltpu.SemaphoreType.DMA(lead)

    return pl.pallas_call(
        functools.partial(group_kernel, pieces),
        out_shape=jax.ShapeDtypeStruct((rows, columns), F32),
        in_specs=[pl.BlockSpec(memory_space=pl.ANY)],
        out_specs=pl.BlockSpec(memory_space=pltpu.VMEM),
        scratch_shapes=[
            pltpu.VMEM((rows, columns), BF16),
            pltpu.VMEM((rows, columns), BF16),
            pltpu.VMEM((2, rows, columns), BF16),
            pltpu.VMEM((rows, columns), BF16),
            sems(2),
            sems(pieces),
            sems(pieces),
            sems(pieces),
            sems(pieces),
            pltpu.SemaphoreType.DMA,
            pltpu.SemaphoreType.DMA,
        ],
        compiler_params=pltpu.CompilerParams(collective_id=collective_id, has_side_effects=True),
        name="group_reduce",
    )(parts.reshape(2, 2, rows, columns))


def group_gather_kernel(pieces, v_ref, out_ref, local_sem, s1, r1, s2, r2, s3, r3):
    x, core = lax.axis_index("x"), lax.axis_index("core")
    partner, across = {"core": 1 - core}, {"x": 1 - x}
    greet(partner)
    greet(across)
    pl.semaphore_wait(pltpu.get_barrier_semaphore(), 2)
    step = v_ref.shape[0] // pieces

    def over(piece):
        at = pl.ds(piece * step, step)
        return remote(
            v_ref.at[at, :], out_ref.at[x, core, at, :], s2.at[piece], r2.at[piece], across
        )

    def pass_on(piece):
        ref = out_ref.at[1 - x, core, pl.ds(piece * step, step), :]
        return remote(ref, ref, s3.at[piece], r3.at[piece], partner)

    direct = remote(v_ref, out_ref.at[x, core], s1, r1, partner)
    mine = pltpu.make_async_copy(v_ref, out_ref.at[x, core], local_sem)
    for piece in range(pieces):
        over(piece).start()
    direct.start()
    mine.start()
    for piece in range(pieces):
        over(piece).wait()
        pass_on(piece).start()
    mine.wait()
    direct.wait()
    for piece in range(pieces):
        pass_on(piece).wait()


def group_gather(value, collective_id):
    if lax.axis_size("x") != 2:
        return gather(value, GROUP)
    rows, columns = value.shape
    pieces = 4

    def sems(*lead):
        return pltpu.SemaphoreType.DMA(lead)

    gathered = pl.pallas_call(
        functools.partial(group_gather_kernel, pieces),
        out_shape=jax.ShapeDtypeStruct((2, 2, rows, columns), value.dtype),
        in_specs=[pl.BlockSpec(memory_space=pltpu.VMEM)],
        out_specs=pl.BlockSpec(memory_space=pltpu.VMEM),
        scratch_shapes=[
            pltpu.SemaphoreType.DMA,
            pltpu.SemaphoreType.DMA,
            pltpu.SemaphoreType.DMA,
            sems(pieces),
            sems(pieces),
            sems(pieces),
            sems(pieces),
        ],
        compiler_params=pltpu.CompilerParams(collective_id=collective_id, has_side_effects=True),
        name="group_gather",
    )(value)
    return gathered.reshape(4 * rows, columns)


def turn(value, cosine, sine):
    return value * cosine + pltpu.roll(value, value.shape[-1] // 2, 1) * sine


def turn_back(value, cosine, sine):
    return value * cosine + pltpu.roll(value * sine, value.shape[-1] // 2, 1)


def head_norm(raw):
    inverse = lax.rsqrt(jnp.mean(raw * raw, axis=-1, keepdims=True) + EPS_HEAD)
    return raw * inverse, inverse


def dot_nt(left, right):
    return lax.dot_general(left, right, (((1,), (1,)), ((), ())), preferred_element_type=F32)


def dot_tn(left, right):
    return lax.dot_general(left, right, (((0,), (0,)), ((), ())), preferred_element_type=F32)


def dot_nn(left, right):
    return lax.dot_general(left, right, (((1,), (0,)), ((), ())), preferred_element_type=F32)


def weights_of(q_rows, keys, doc_rows, doc_keys, scale):
    scores = dot_nt(q_rows, keys) * scale
    scores = jnp.where(doc_rows == doc_keys, scores, MASKED)
    lifted = jnp.exp(scores - jnp.max(scores, axis=-1, keepdims=True))
    return lifted / jnp.sum(lifted, axis=-1, keepdims=True)


def attend_kernel(step, q_ref, k_ref, v_ref, qg_ref, kg_ref, cos_ref, sin_ref, dr_ref, dk_ref, o_ref):
    scale = q_ref.shape[-1] ** (-0.5)
    cosine, sine = cos_ref[...], sin_ref[...]
    queries = turn(head_norm(q_ref[...])[0] * qg_ref[...], cosine, sine).astype(BF16)
    keys = turn(head_norm(k_ref[...])[0] * kg_ref[...], cosine, sine).astype(BF16)
    values = v_ref[...].astype(BF16)
    for at in range(0, q_ref.shape[0], step):
        rows = slice(at, at + step)
        weights = weights_of(queries[rows], keys, dr_ref[rows, :], dk_ref[...], scale)
        o_ref[rows, :] = dot_nn(weights.astype(BF16), values).astype(BF16)


def attend_back_kernel(
    step, q_ref, k_ref, v_ref, go_ref, qg_ref, kg_ref, cos_ref, sin_ref, dr_ref, dk_ref,
    gq_ref, gk_ref, gv_ref, gqg_ref, gkg_ref,
):
    scale = q_ref.shape[-1] ** (-0.5)
    cosine, sine = cos_ref[...], sin_ref[...]
    q_normed, q_inverse = head_norm(q_ref[...])
    k_normed, k_inverse = head_norm(k_ref[...])
    queries = turn(q_normed * qg_ref[...], cosine, sine).astype(BF16)
    keys = turn(k_normed * kg_ref[...], cosine, sine).astype(BF16)
    values = v_ref[...].astype(BF16)
    grad_keys = jnp.zeros(k_ref.shape, F32)
    grad_values = jnp.zeros(v_ref.shape, F32)
    grad_queries = []
    for at in range(0, q_ref.shape[0], step):
        rows = slice(at, at + step)
        probs = weights_of(queries[rows], keys, dr_ref[rows, :], dk_ref[...], scale)
        grad_rows = go_ref[rows, :]
        grad_weights = dot_nt(grad_rows, values)
        delta = jnp.sum(grad_weights * probs, axis=-1, keepdims=True)
        grad_scores = (probs * (grad_weights - delta)).astype(BF16)
        grad_queries.append(dot_nn(grad_scores, keys))
        grad_keys = grad_keys + dot_tn(grad_scores, queries[rows])
        grad_values = grad_values + dot_tn(probs.astype(BF16), grad_rows)

    @pl.when(pl.program_id(0) == 0)
    def _():
        gqg_ref[...] = jnp.zeros_like(gqg_ref)
        gkg_ref[...] = jnp.zeros_like(gkg_ref)

    def finish(grad, normed, inverse, gain_ref, out_ref, gain_grad_ref):
        grad = turn_back(grad * scale, cosine, sine)
        gain_grad_ref[...] += jnp.sum(grad * normed, axis=0, keepdims=True)
        lifted = grad * gain_ref[...]
        inner = jnp.mean(lifted * normed, axis=-1, keepdims=True)
        out_ref[...] = ((lifted - normed * inner) * inverse).astype(BF16)

    finish(jnp.concatenate(grad_queries, axis=0), q_normed, q_inverse, qg_ref, gq_ref, gqg_ref)
    finish(grad_keys, k_normed, k_inverse, kg_ref, gk_ref, gkg_ref)
    gv_ref[...] = grad_values.astype(BF16)


def attention_call(kernel, heads, head_dim, seq_len, values, tables, outs, flops):
    column = pl.BlockSpec((seq_len, head_dim), lambda head: (0, head))
    whole = [pl.BlockSpec(t.shape, lambda head: (0, 0)) for t in tables]
    shapes = [
        jax.ShapeDtypeStruct((seq_len, heads * head_dim), BF16) if wide
        else jax.ShapeDtypeStruct((1, head_dim), F32)
        for wide in outs
    ]
    specs = [column if wide else pl.BlockSpec((1, head_dim), lambda head: (0, 0)) for wide in outs]
    return pl.pallas_call(
        functools.partial(kernel, min(512, seq_len)),
        grid=(heads,),
        out_shape=shapes,
        in_specs=[column] * len(values) + whole,
        out_specs=specs,
        compiler_params=pltpu.CompilerParams(vmem_limit_bytes=VMEM_BYTES),
        cost_estimate=pl.CostEstimate(
            flops=flops, bytes_accessed=16 * seq_len * heads * head_dim, transcendentals=heads * seq_len**2
        ),
        name="attention",
    )(*values, *tables)


def params(flops, moved):
    return dict(compiler_params=pltpu.CompilerParams(vmem_limit_bytes=VMEM_BYTES),
        cost_estimate=pl.CostEstimate(flops=flops, bytes_accessed=moved, transcendentals=0))


def pick_rows_of(pick, value, out_ref, index):
    local, _, capacity, _ = out_ref.shape
    rows = dot_nn(pick, value).astype(BF16)
    for expert_at in range(local):
        out_ref[expert_at, index] = rows[expert_at * capacity : (expert_at + 1) * capacity]


def dispatch_kernel(pick_ref, value_ref, out_ref):
    for index in range(pick_ref.shape[0]):
        pick_rows_of(pick_ref[index], value_ref[index], out_ref, index)


def dispatch(pick, value, local, group):
    blocks, picked, rows = pick.shape
    width = value.shape[-1]
    capacity = picked // local
    return pl.pallas_call(
        dispatch_kernel,
        grid=(blocks // group,),
        out_shape=jax.ShapeDtypeStruct((local, blocks, capacity, width), BF16),
        in_specs=[
            pl.BlockSpec((group, picked, rows), lambda b: (b, 0, 0)),
            pl.BlockSpec((group, rows, width), lambda b: (b, 0, 0)),
        ],
        out_specs=pl.BlockSpec((local, group, capacity, width), lambda b: (0, b, 0, 0)),
        name="dispatch",
        **params(2 * blocks * picked * rows * width, 2 * blocks * width * (picked + rows)),
    )(pick, value)


def combine_kernel(pick_ref, value_ref, *refs):
    local, group, capacity, width = value_ref.shape
    out_ref = refs[-2] if len(refs) == 3 else refs[0]
    for index in range(group):
        pick = pick_ref[index]
        if group == 1:
            value = value_ref[...].reshape(local * capacity, width)
        else:
            value = jnp.concatenate([value_ref[e, index] for e in range(local)], axis=0)
        out_ref[index] = dot_tn(pick, value).astype(BF16)
        if len(refs) == 3:
            for e in range(local):
                part = pick[e * capacity : (e + 1) * capacity].astype(F32)
                refs[2][index, e : e + 1, :] = jnp.sum(
                    part * refs[0][e, index], axis=0, keepdims=True
                )


def combine(pick, value, dots=None, group=2):
    blocks, picked, rows = pick.shape
    local, _, capacity, width = value.shape

    def rows_of(columns):
        return pl.BlockSpec((local, group, capacity, columns), lambda b: (0, b, 0, 0))

    ins, specs = [pick, value], [pl.BlockSpec((group, picked, rows), lambda b: (b, 0, 0)), rows_of(width)]
    shapes = [jax.ShapeDtypeStruct((blocks, rows, width), BF16)]
    outs = [pl.BlockSpec((group, rows, width), lambda b: (b, 0, 0))]
    if dots is not None:
        ins += [dots]
        specs += [rows_of(1)]
        shapes += [jax.ShapeDtypeStruct((blocks, local, rows), F32)]
        outs += [pl.BlockSpec((group, local, rows), lambda b: (b, 0, 0))]
    return pl.pallas_call(
        combine_kernel,
        grid=(blocks // group,),
        out_shape=shapes,
        in_specs=specs,
        out_specs=outs,
        name="combine",
        **params(2 * blocks * picked * rows * width, 2 * blocks * width * (picked + rows)),
    )(*ins)


def down_kernel(h0_ref, h1_ref, w0_ref, w1_ref, out_ref):
    out_ref[0] = (dot_nn(h0_ref[0], w0_ref[0]) + dot_nn(h1_ref[0], w1_ref[0])).astype(BF16)


def down_rows(h0, h1, w0, w1, step):
    local, count, hidden = h0.shape
    width = w0.shape[-1]
    rows = pl.BlockSpec((1, step, hidden), lambda e, i: (e, i, 0))
    weight = pl.BlockSpec((1, hidden, width), lambda e, i: (e, 0, 0))
    return pl.pallas_call(
        down_kernel,
        grid=(local, count // step),
        out_shape=jax.ShapeDtypeStruct((local, count, width), BF16),
        in_specs=[rows, rows, weight, weight],
        out_specs=pl.BlockSpec((1, step, width), lambda e, i: (e, i, 0)),
        name="down_rows",
        **params(4 * local * count * hidden * width, 2 * local * (count + 2 * hidden) * width),
    )(h0, h1, w0, w1)


def expert_kernel(x_ref, w0_ref, w1_ref, u0_ref, u1_ref, pr_ref, gx_ref, dots_ref, *outs):
    x = x_ref[0]
    prob = pr_ref[0]
    total = None
    dots = None
    for w_ref, u_ref, hp_ref, ggu_ref in ((w0_ref, u0_ref, outs[0], outs[2]), (w1_ref, u1_ref, outs[1], outs[3])):
        n = u_ref.shape[-1]
        both = dot_nn(x, w_ref[0])
        gate, up = both[:, :n], both[:, n:]
        sigma = jax.nn.sigmoid(gate)
        silu = gate * sigma
        hidden = (silu * up).astype(BF16).astype(F32)
        back = u_ref[0]
        part = jnp.sum(hidden * back, axis=-1, keepdims=True)
        dots = part if dots is None else dots + part
        hp_ref[0] = (hidden * prob).astype(BF16)
        gh = back * prob
        ggu_ref[0, :, :n] = (gh * up * (sigma + silu * (1.0 - sigma))).astype(BF16)
        ggu_ref[0, :, n:] = (gh * silu).astype(BF16)
        part = dot_nt(ggu_ref[0], w_ref[0])
        total = part if total is None else total + part
    gx_ref[0] = total.astype(BF16)
    dots_ref[0] = dots


def expert(x, w0, w1, u0, u1, prob, step):
    local, count, width = x.shape
    n = u0.shape[-1]
    r = lambda c: pl.BlockSpec((1, step, c), lambda e, i: (e, i, 0))
    w = pl.BlockSpec((1, width, 2*n), lambda e, i: (e, 0, 0))
    s = lambda c, t: jax.ShapeDtypeStruct((local, count, c), t)
    return pl.pallas_call(
        expert_kernel, grid=(local, count//step),
        out_shape=[s(width,BF16), s(1,F32), s(n,BF16), s(n,BF16), s(2*n,BF16), s(2*n,BF16)],
        in_specs=[r(width), w, w, r(n), r(n), r(1)],
        out_specs=[r(width), r(1), r(n), r(n), r(2*n), r(2*n)],
        name="expert", **params(16*local*count*width*n, local*(count*(width*4+n*20)+8*width*n)),
    )(x, w0, w1, u0, u1, prob)


def norm_rows(value, gain):
    inverse = lax.rsqrt(jnp.mean(value * value, axis=-1, keepdims=True) + EPS_NORM)
    return value * inverse * gain


def norm_back(value, gain, grad):
    inverse = lax.rsqrt(jnp.mean(value * value, axis=-1, keepdims=True) + EPS_NORM)
    normed = value * inverse
    lifted = grad * gain
    inner = jnp.mean(lifted * normed, axis=-1, keepdims=True)
    return (lifted - normed * inner) * inverse, jnp.sum(grad * normed, axis=0)


def positions(lengths, seq_len):
    ends = jnp.cumsum(lengths)
    starts = ends - lengths
    index = jnp.arange(seq_len, dtype=jnp.int32)
    doc_ids = jnp.sum((index[:, None] >= ends[None, :]).astype(jnp.int32), axis=1)
    member = doc_ids[:, None] == jnp.arange(lengths.shape[0], dtype=jnp.int32)[None, :]
    offset = jnp.sum(jnp.where(member, starts[None, :], 0), axis=1)
    return (doc_ids, index - offset)


def rope_tables(position, head_dim):
    half = head_dim // 2
    freq = ROPE_BASE ** (-(2.0 * jnp.arange(half, dtype=F32)) / head_dim)
    angle = position.astype(F32)[:, None] * freq[None, :]
    return (jnp.cos(angle), jnp.sin(angle))


def einsum(spec, left, right):
    return jnp.einsum(spec, left, right, preferred_element_type=F32)


def swap_cores(value):
    return lax.ppermute(value, "core", [(0, 1), (1, 0)])


def gather(value, axes):
    return lax.all_gather(value, axes, axis=0, tiled=True)


def scatter(value, axes, dim=0):
    return lax.psum_scatter(value, axes, scatter_dimension=dim, tiled=True)


def masked_softmax(logits, mask):
    kept = jnp.where(mask, logits, MASKED)
    lifted = jnp.where(mask, jnp.exp(kept - jnp.max(kept, axis=-1, keepdims=True)), 0.0)
    return lifted / jnp.sum(lifted, axis=-1, keepdims=True)


def route_mask(routes, experts_all):
    ids = jnp.arange(experts_all, dtype=jnp.int32)
    return jnp.any(routes[:, :, None] == ids[None, None, :], axis=1)


def per_device(
    layer_input,
    routes,
    doc_lengths,
    norm1_gain,
    w_qkv,
    q_gain,
    k_gain,
    w_out,
    norm2_gain,
    w_router,
    expert_gate_up,
    expert_down,
    d_out,
):
    rows, width = layer_input.shape
    x_count = lax.axis_size("x")
    ep_count = lax.axis_size("ep")
    seq_len = rows * x_count * 2
    blocks = ep_count * x_count
    topk = routes.shape[1]
    experts_all = w_router.shape[1]
    local = expert_gate_up.shape[0]
    hidden_local = expert_down.shape[1]
    head_dim = q_gain.shape[0]
    qkv_local = w_qkv.shape[2]
    heads = qkv_local // head_dim
    capacity = min(3 * rows * topk // (2 * experts_all), rows)
    my_ep = lax.axis_index("ep")

    gain_one = norm1_gain.astype(F32)
    gain_two = norm2_gain.astype(F32)
    inputs = layer_input.astype(F32)
    grad_out = d_out.astype(F32)
    input_seq = group_gather(layer_input, 8)
    g_flat = gather(d_out, PLANE)
    h_seq = norm_rows(input_seq.astype(F32), gain_one).astype(BF16)
    w_parts = w_qkv.transpose(1, 0, 2)
    raw = [jnp.dot(h_seq, w_parts[part], preferred_element_type=F32) for part in range(3)]
    doc_ids, position = positions(doc_lengths[0], seq_len)
    cosine, sine = rope_tables(position, head_dim)
    tables = (
        q_gain.astype(F32)[None],
        k_gain.astype(F32)[None],
        jnp.concatenate([cosine, cosine], axis=1),
        jnp.concatenate([-sine, sine], axis=1),
        doc_ids[:, None],
        doc_ids[None, :],
    )
    (attn_vals,) = attention_call(
        attend_kernel, heads, head_dim, seq_len, raw, tables, (True,), 4 * seq_len**2 * qkv_local
    )
    attn_part = jnp.dot(attn_vals, w_out, preferred_element_type=F32).astype(BF16)
    attn_out = group_reduce(attn_part, 7)
    middle = inputs + attn_out
    h_two = norm_rows(middle, gain_two).astype(BF16)

    g_plane = g_flat.reshape(blocks, rows, width)
    mask_own = route_mask(routes, experts_all)
    probs_own = masked_softmax(jnp.dot(h_two, w_router, preferred_element_type=F32), mask_own)
    shared = spread(jnp.where(mask_own, probs_own, -1.0).T, PLANE, 1)
    h_flat = gather(h_two, PLANE)
    pair_other = swap_cores(expert_gate_up.reshape(local, width, 2 * hidden_local))
    down_other = swap_cores(expert_down)
    pair_own = expert_gate_up.reshape(local, width, 2 * hidden_local)

    first = my_ep * local
    here = lax.dynamic_slice_in_dim(shared, first, local, axis=1)
    mask_here = here >= 0.0
    before = jnp.triu(jnp.ones((rows, rows), BF16), 1)
    rank = einsum("bet,tu->beu", mask_here.astype(BF16), before).astype(jnp.int32)
    slots = jnp.arange(capacity, dtype=jnp.int32)[None, None, :, None]
    picks = mask_here[:, :, None, :] & (rank[:, :, None, :] == slots)
    pick = picks.astype(BF16)
    pick_rows = pick.reshape(blocks, local * capacity, rows)
    count = blocks * capacity

    g_rows = dispatch(pick_rows, g_plane, local, group=4)
    g_rows = g_rows.reshape(local, count, width)
    back_own = einsum("emd,efd->emf", g_rows, expert_down)
    back_other = einsum("emd,efd->emf", g_rows, down_other)
    prob_rows = jnp.sum(jnp.where(picks, here[:, :, None, :], 0.0), axis=-1)
    prob_rows = prob_rows.transpose(1, 0, 2).reshape(local, count, 1)
    h_flat, back_own, back_other, prob_rows = lax.optimization_barrier(
        (h_flat, back_own, back_other, prob_rows)
    )
    h_rows = dispatch(pick_rows, h_flat.reshape(blocks, rows, width), local, group=4)
    h_rows = h_rows.reshape(local, count, width)
    back_rows, dot_rows, weighted_own, weighted_other, ggu_own, ggu_other = expert(
        h_rows, pair_own, pair_other, back_own, back_other, prob_rows, min(384, count)
    )
    dot_rows = dot_rows.reshape(local, blocks, capacity).transpose(1, 0, 2)
    dots_token = jnp.sum(jnp.where(picks, dot_rows[..., None], 0.0), axis=2)
    grad_probs = spread(dots_token, PLANE, 2, True)
    back_rows, grad_probs = lax.optimization_barrier((back_rows, grad_probs))
    grad_probs = jnp.sum(grad_probs.reshape(ep_count, x_count, local, rows), axis=1)
    grad_probs = grad_probs.reshape(experts_all, rows).T
    back_sum, grad_pair_own, grad_pair_other, grad_down_own, grad_down_other = plane_reduce(
        pick_rows,
        back_rows.reshape(local, blocks, capacity, width),
        3,
        (g_rows, weighted_own, weighted_other, h_rows, ggu_own, ggu_other),
    )
    out_rows = down_rows(
        weighted_own, weighted_other, expert_down, down_other, min(384, count)
    ).reshape(local, blocks, capacity, width)

    grad_pair = grad_pair_own + swap_cores(grad_pair_other).astype(F32)
    grad_down = grad_down_own + swap_cores(grad_down_other).astype(F32)

    inner = jnp.sum(probs_own * grad_probs, axis=-1, keepdims=True)
    grad_logits = probs_own * (grad_probs - inner)
    grad_router = lax.dot_general(
        grad_logits, h_two.astype(F32), (((0,), (0,)), ((), ())), precision=HIGH
    )
    grad_h_two = back_sum + jnp.dot(
        grad_logits, w_router.astype(F32).T, precision=HIGH
    )
    grad_mid_norm, grad_gain_two = norm_back(middle, gain_two, grad_h_two)
    grad_mid = grad_out + grad_mid_norm

    ga_seq = gather(grad_mid.astype(BF16), GROUP)
    ga_seq, out_rows, grad_down, grad_pair = lax.optimization_barrier(
        (ga_seq, out_rows, grad_down, grad_pair)
    )
    grad_gate_up = grad_pair.reshape(local, width, 2, hidden_local)
    grad_wout = lax.dot_general(
        attn_vals, ga_seq, (((0,), (0,)), ((), ())), preferred_element_type=F32
    )
    grad_vals = lax.dot_general(
        ga_seq, w_out, (((1,), (1,)), ((), ())), preferred_element_type=F32
    )
    *grad_proj, grad_q_gain, grad_k_gain = attention_call(
        attend_back_kernel,
        heads,
        head_dim,
        seq_len,
        (*raw, grad_vals.astype(BF16)),
        tables,
        (True, True, True, False, False),
        10 * seq_len**2 * qkv_local,
    )
    grad_h_part = sum(
        lax.dot_general(grad, w, (((1,), (1,)), ((), ())), preferred_element_type=F32)
        for grad, w in zip(grad_proj, w_parts)
    )
    grad_h_one = scatter(grad_h_part.astype(BF16), GROUP).astype(F32)
    grad_wqkv = jnp.stack(
        [
            lax.dot_general(
                h_seq, grad, (((0,), (0,)), ((), ())), preferred_element_type=F32
            ).astype(BF16)
            for grad in grad_proj
        ],
    )
    grad_in_norm, grad_gain_one = norm_back(inputs, gain_one, grad_h_one)
    grad_input = grad_mid + grad_in_norm
    dense_qkv = scatter(grad_wqkv, "ep", 1).astype(F32)
    dense_out = scatter(grad_wout.astype(BF16), "ep", 1).astype(F32)
    devices = blocks * 2
    small = jnp.concatenate(
        [grad_router.reshape(-1), grad_gain_one, grad_gain_two, grad_q_gain[0], grad_k_gain[0]]
    )
    length = small.shape[0]
    padded = -(-length // (devices * 1024)) * devices * 1024
    small = jnp.pad(small, (0, padded - length)).reshape(devices, -1, 128)
    small = jnp.sum(spread(small, ALL, 5, True), axis=0)
    small = spread(small, ALL, 6).reshape(-1)
    out_rows, small = lax.optimization_barrier((out_rows, small))
    output = (middle + plane_reduce(pick_rows, out_rows, 4, sides=1)).astype(BF16)
    cuts = (experts_all * width, width, width, head_dim, head_dim)
    starts = [sum(cuts[:index]) for index in range(5)]
    router_sum, *gains = (small[at : at + cut] for at, cut in zip(starts, cuts))
    grad_router = router_sum.reshape(experts_all, width).T
    return (
        output,
        grad_input,
        gains[0],
        dense_qkv.transpose(1, 0, 2),
        gains[2],
        gains[3],
        dense_out,
        gains[1],
        grad_router,
        grad_gate_up,
        grad_down,
    )


def solution(mesh):
    ep_count, tp_count = mesh.shape["ep"], mesh.shape["tp"]
    fine = Mesh(mesh.devices.reshape(ep_count, tp_count // 2, 2), ALL)
    in_specs = (
        P(ALL, None),
        P(ALL, None),
        P("ep", None),
        P(),
        P(None, None, GROUP),
        P(),
        P(),
        P(GROUP, None),
        P(),
        P(),
        P("ep", None, None, GROUP),
        P("ep", GROUP, None),
        P(ALL, None),
    )
    out_specs = (
        P(ALL, None),
        P(ALL, None),
        P(),
        P("ep", None, GROUP),
        P(),
        P(),
        P(GROUP, "ep"),
        P(),
        P(),
        P("ep", None, None, GROUP),
        P("ep", GROUP, None),
    )

    return jax.shard_map(
        per_device, mesh=fine, in_specs=in_specs, out_specs=out_specs, check_vma=False
    )
```
